16 devices in a mesh: layer: 2 (over y, z), tensor: 8 (over x, core).
Axes of the slice: x: 4, y: 2, z: 1, core: 2. Of those that a mesh axis runs over, the one named last changes fastest.
The devices are a block of a 4x4x8 slice.
Arguments:
- gradient: bfloat16 [1024, 8192], P('layer', 'tensor'), parts along dimension 0
- left_stat: float32 [1024, 512], P(('layer', 'tensor')), parts along dimension 0
- right_stat: float32 [16384, 8192], P(('layer', 'tensor')), parts along dimension 0
- left_root: bfloat16 [1024, 512], P(('layer', 'tensor')), parts along dimension 0
- right_root: bfloat16 [16384, 8192], P(('layer', 'tensor')), parts along dimension 0
Outputs:
- output 1: float32 [1024, 512], P(('layer', 'tensor')), parts along dimension 0
- output 2: float32 [16384, 8192], P(('layer', 'tensor')), parts along dimension 0
- output 3: float32 [1024, 8192], P('layer', 'tensor'), parts along dimension 0
There are 2 independent parts. The reference program is written for one: setup_inputs(seed, part) draws one part's arguments, and reference() takes and returns one part's arrays. A program takes and returns all parts, laid end to end along the dimension named above; each array names one.
All inputs are finite; a program needn't handle non-finite values.
Results may differ from the reference program's by a relative error of at most 0.001.
Values are sent between devices in bfloat16 or wider.
A program may use at most 768 MiB of HBM per device.

```python
import jax
import jax.numpy as jnp

ROW_COUNT = 512
COL_COUNT = 8192
EMA_DECAY = 0.9


def setup_inputs(seed: int = 0, part: int = 0) -> dict:
    base_key = jax.random.fold_in(jax.random.key(seed), part)
    keys = jax.random.split(base_key, 5)
    grad_scale = (ROW_COUNT * COL_COUNT) ** -0.25
    root_scale = (ROW_COUNT * COL_COUNT) ** 0.125
    gradient = grad_scale * jax.random.normal(keys[0], (ROW_COUNT, COL_COUNT), jnp.float32)
    left_hist = jax.random.normal(keys[1], (ROW_COUNT, COL_COUNT // 8), jnp.float32)
    left_stat = (0.8 * grad_scale ** 2) * jnp.dot(left_hist, left_hist.T)
    right_hist = jax.random.normal(keys[2], (COL_COUNT, ROW_COUNT // 8), jnp.float32)
    right_stat = (0.8 * grad_scale ** 2) * jnp.dot(right_hist, right_hist.T)
    left_basis = jax.random.normal(keys[3], (ROW_COUNT, ROW_COUNT // 8), jnp.float32)
    left_root = root_scale * (0.5 * jnp.eye(ROW_COUNT, dtype=jnp.float32) + jnp.dot(left_basis, left_basis.T) / ROW_COUNT)
    right_basis = jax.random.normal(keys[4], (COL_COUNT, COL_COUNT // 8), jnp.float32)
    right_prod = jnp.dot(right_basis, right_basis.T) / COL_COUNT
    right_root = root_scale * (0.5 * jnp.eye(COL_COUNT, dtype=jnp.float32) + 0.5 * (right_prod + right_prod.T))
    return {"gradient": gradient.astype(jnp.bfloat16), "left_stat": left_stat, "right_stat": right_stat, "left_root": left_root.astype(jnp.bfloat16), "right_root": right_root.astype(jnp.bfloat16)}


def reference(gradient, left_stat, right_stat, left_root, right_root):
    left_new = EMA_DECAY * left_stat + (1.0 - EMA_DECAY) * jnp.dot(gradient, gradient.T, preferred_element_type=jnp.float32)
    right_new = EMA_DECAY * right_stat + (1.0 - EMA_DECAY) * jnp.dot(gradient.T, gradient, preferred_element_type=jnp.float32)
    precond = jnp.dot(gradient, right_root, preferred_element_type=jnp.float32).astype(jnp.bfloat16)
    direction = jnp.dot(left_root, precond, preferred_element_type=jnp.float32)
    return (left_new, right_new, direction)
```

```python
import functools

import jax
import jax.numpy as jnp
from jax import lax
from jax.experimental import pallas as pl
from jax.experimental.pallas import tpu as pltpu
from jax.sharding import PartitionSpec as P

EMA_DECAY = 0.9


def _nt(a, b):
    return lax.dot_general(a, b, (((1,), (1,)), ((), ())), preferred_element_type=jnp.float32)


def _step_kernel(m, first, last, rows, sub, idx, *refs):
    refs = list(refs)
    if not first:
        refs.pop(0)
    gt = refs.pop(0)
    chunks = [refs.pop(0) for _ in range(m)]
    right, root = refs.pop(0), refs.pop(0)
    x_in = l_in = None
    if not first:
        x_in, l_in = refs.pop(0), refs.pop(0)
    if last:
        lroot, left = refs.pop(0), refs.pop(0)
        right_out, l_out, d_out, x_acc = refs
        l_acc = l_out
    else:
        right_out, x_acc, l_acc = refs
    i = pl.program_id(0)
    per = chunks[0].shape[1] // sub

    @pl.when(i == 0)
    def _():
        if first:
            x_acc[...] = jnp.zeros_like(x_acc)
            l_acc[...] = jnp.zeros_like(l_acc)
        else:
            x_acc[...] = x_in[...]
            l_acc[...] = l_in[...]

    for q in range(m):
        @pl.when(i // per == q)
        def _(q=q):
            col = pl.multiple_of((i % per) * sub, sub)
            h = chunks[q][0:rows, pl.ds(col, sub)]
            right_out[...] = EMA_DECAY * right[...] + (1.0 - EMA_DECAY) * jnp.dot(
                gt[...], h, preferred_element_type=jnp.float32)
            x_acc[...] += _nt(h, root[...])
            nl = l_acc.shape[0]
            r0 = pl.multiple_of(idx[m] * nl, nl)
            l_acc[...] += _nt(chunks[q][pl.ds(r0, nl), pl.ds(col, sub)], h)

    if last:
        @pl.when(i == pl.num_programs(0) - 1)
        def _():
            d_out[...] = jnp.dot(lroot[...], x_acc[...].astype(jnp.bfloat16), preferred_element_type=jnp.float32)
            l_out[...] = EMA_DECAY * left[...] + (1.0 - EMA_DECAY) * l_acc[...]


def _step(idx, me, prev, gt, chunks, right, root, acc, tail, sub=256):
    first, last = prev is None, tail is not None
    m = len(chunks)
    cols, rows = gt.shape
    nl = rows // (right.shape[1] // cols)
    per = chunks[0].shape[1] // sub
    idx = jnp.stack([*idx, me]).astype(jnp.int32)
    blk = lambda i, idx: (0, idx[i // per] * per + i % per)
    full = lambda a: pl.BlockSpec(a.shape, lambda i, idx: (0, 0))
    args, specs = [], []
    if not first:
        args.append(prev)
        specs.append(pl.BlockSpec(memory_space=pl.ANY))
    args += [gt, *chunks, right, root]
    specs += [full(gt)] + [full(c) for c in chunks] + [pl.BlockSpec((cols, sub), blk)] * 2
    if not first:
        args += list(acc)
        specs += [full(a) for a in acc]
    f32 = jnp.float32
    x_shape = jax.ShapeDtypeStruct((rows, cols), f32)
    l_shape = jax.ShapeDtypeStruct((nl, rows), f32)
    r_shape = jax.ShapeDtypeStruct(right.shape, f32)
    if last:
        args += list(tail)
        specs += [full(a) for a in tail]
        out_shape = (r_shape, l_shape, x_shape)
        scratch = [pltpu.VMEM((rows, cols), f32)]
    else:
        out_shape = (r_shape, x_shape, l_shape)
        scratch = []
    out_specs = (pl.BlockSpec((cols, sub), blk), full(out_shape[1]), full(out_shape[2]))
    flops = 4 * rows * cols * m * chunks[0].shape[1]
    return pl.pallas_call(
        functools.partial(_step_kernel, m, first, last, rows, sub),
        out_shape=out_shape,
        grid_spec=pltpu.PrefetchScalarGridSpec(
            num_scalar_prefetch=1, grid=(m * per,), in_specs=specs, out_specs=out_specs, scratch_shapes=scratch),
        input_output_aliases={} if first else {1: 0},
        compiler_params=pltpu.CompilerParams(vmem_limit_bytes=40 << 20),
        cost_estimate=pl.CostEstimate(flops=flops, bytes_accessed=m * chunks[0].shape[1] * cols * 10, transcendentals=0),
    )(idx, *args)


def solution(mesh):
    row_spec = P(("layer", "tensor"), None)
    col_spec = P("layer", "tensor")
    n = mesh.shape["tensor"]

    def shift(v, k):
        return lax.ppermute(v, "tensor", [(j, (j + k) % n) for j in range(n)])

    def swap(v):
        return lax.ppermute(v, "tensor", [(j, j ^ 1) for j in range(n)])

    def local_step(grad, left, right, lroot, rroot):
        me = lax.axis_index("tensor")
        mate = me ^ 1
        rows, cols = grad.shape
        half = cols // 2
        nl = lroot.shape[0]
        gt = grad.T
        p0 = jnp.concatenate([grad[:, :half], lroot], axis=0)
        p1 = grad[:, half:]
        a0, b0 = shift(p0, 2), shift(p1, n - 2)
        q0, q1 = swap(p0), swap(p1)
        a1, b1 = shift(p1, 2), shift(p0, n - 2)
        a2, b2 = shift(a0, 2), shift(b0, n - 2)
        ax = [swap(v) for v in (a0, a1, a2)]
        bx = [swap(v) for v in (b0, b1, b2)]

        def at(dev, k, h):
            return 2 * ((dev + k) % n) + h

        r, x, l = _step([at(me, 0, 0), at(me, 0, 1)], me, None, gt, [p0, p1], right, rroot, None, None)
        r, x, l = _step([at(mate, 0, 0), at(mate, 0, 1)], me, r, gt, [q0, q1], right, rroot, (x, l), None)
        r, x, l = _step([at(me, n - 2, 0), at(me, 2, 1), at(mate, n - 2, 0), at(mate, 2, 1)], me, r, gt,
                        [a0, b0, ax[0], bx[0]], right, rroot, (x, l), None)
        r, x, l = _step([at(me, n - 2, 1), at(me, 2, 0), at(mate, n - 2, 1), at(mate, 2, 0)], me, r, gt,
                        [a1, b1, ax[1], bx[1]], right, rroot, (x, l), None)
        pieces = [(me, p0), (mate, q0), ((me + n - 2) % n, a0), ((mate + n - 2) % n, ax[0]),
                  ((me + 2) % n, b1), ((mate + 2) % n, bx[1]), ((me + n - 4) % n, a2), ((mate + n - 4) % n, ax[2])]
        lfull = jnp.zeros((rows, rows), lroot.dtype)
        for k, v in pieces:
            lfull = lax.dynamic_update_slice(lfull, v[rows:, :], (k * nl, 0))
        r, l, d = _step([at(me, n - 4, 0), at(me, 4, 1), at(mate, n - 4, 0), at(mate, 4, 1)], me, r, gt,
                        [a2, b2, ax[2], bx[2]], right, rroot, (x, l), (lfull, left))
        return l, r, d

    return jax.shard_map(local_step, mesh=mesh, in_specs=(col_spec, row_spec, row_spec, row_spec, row_spec), out_specs=(row_spec, row_spec, col_spec), check_vma=False)
```

```python
import functools

import jax
import jax.numpy as jnp
from jax import lax
from jax.experimental import pallas as pl
from jax.experimental.pallas import tpu as pltpu
from jax.sharding import PartitionSpec as P

EMA_DECAY = 0.9
SPLIT = 4
AHEAD = 4

MESH = pl.DeviceIdType.MESH
ANY = pl.BlockSpec(memory_space=pl.ANY)
VMEM = pl.BlockSpec(memory_space=pltpu.VMEM)


def _nt(a, b):
    return lax.dot_general(a, b, (((1,), (1,)), ((), ())), preferred_element_type=jnp.float32)


def _gather_kernel(n, grad, lroot, right, rroot, rbuf, xacc, lbuf, gbuf, gt, rr,
                   own_sem, r_sem, rr_sem, recv, send_p, send_m, send_d,
                   l_own, l_recv, l_send):
    me = lax.axis_index("tensor")
    mate = me + 1 - 2 * (me % 2)
    rows, width = gbuf.shape[1], gbuf.shape[2]
    cols = gt.shape[0]
    nl = lroot.shape[0]
    hl = nl // 2
    steps = 6
    ring = lambda d: lax.rem(d + n, n)
    plus, minus = ring(me + 2), ring(me - 2)

    def slot(t, u, i):
        base = jnp.where(u == 0, me, mate)
        s = t - 2
        far = 2 + 2 * (s // SPLIT)
        owner = jnp.where(i == 0, base - far, base + far)
        part = (s + 2 * i) % SPLIT
        owner = jnp.where(t == 0, me, jnp.where(t == 1, mate, owner))
        part = jnp.where(t < 2, 2 * u + i, part)
        return lax.rem(owner + n, n) * SPLIT + part

    def span(sl):
        return pl.ds(pl.multiple_of(sl * width, width), width)

    def r_copy(sl):
        return pltpu.make_async_copy(right.at[:, span(sl)], rbuf.at[:, span(sl)], r_sem.at[sl])

    def rr_copy(sl, k):
        return pltpu.make_async_copy(rroot.at[:, span(sl)], rr.at[k, pl.ds(0, cols)], rr_sem.at[k])

    def own_copy(q):
        return pltpu.make_async_copy(grad.at[:, pl.ds(q * width, width)], gbuf.at[me * SPLIT + q], own_sem.at[q])

    def piece(sl, sem, dev):
        return pltpu.make_async_remote_copy(
            src_ref=gbuf.at[sl], dst_ref=gbuf.at[sl], send_sem=sem, recv_sem=recv.at[sl],
            device_id={"tensor": dev}, device_id_type=MESH)

    def lpart(owner, first, count, s_idx, r_idx, dev):
        at = pl.ds(pl.multiple_of(owner * nl + first, hl), count)
        return pltpu.make_async_remote_copy(
            src_ref=lbuf.at[at], dst_ref=lbuf.at[at], send_sem=l_send.at[s_idx], recv_sem=l_recv.at[r_idx],
            device_id={"tensor": dev}, device_id_type=MESH)

    own = [own_copy(q) for q in range(SPLIT)]
    for c in own:
        c.start()
    lown = pltpu.make_async_copy(lroot, lbuf.at[pl.ds(pl.multiple_of(me * nl, nl), nl)], l_own)
    lown.start()

    def loads(t, k0):
        for u in range(2):
            for i in range(2):
                sl = slot(t, u, i)
                r_copy(sl).start()
                rr_copy(sl, k0 + 2 * u + i).start()

    barrier = pltpu.get_barrier_semaphore()
    for dev in (plus, minus, mate):
        pl.semaphore_signal(barrier, inc=1, device_id={"tensor": dev}, device_id_type=MESH)
    pl.semaphore_wait(barrier, 3)

    for c in own:
        c.wait()
    lown.wait()
    sent = []
    for s in range(SPLIT):
        sent.append(piece(me * SPLIT + s, send_p.at[s], plus))
        sent.append(piece(me * SPLIT + (s + 2) % SPLIT, send_m.at[s], minus))
        sent.append(piece(me * SPLIT + s, send_d.at[s], mate))
        if s == 0:
            sent.append(lpart(me, 0, nl, 0, 0, plus))
            sent.append(lpart(me, 0, nl, 1, 1, minus))
            sent.append(lpart(me, 0, nl, 2, 4, mate))
    for c in sent:
        c.start()
    for t in range(AHEAD):
        loads(t, 4 * t)
    for q in range(SPLIT):
        gt[pl.ds(q * width, width), :] = gbuf[me * SPLIT + q].T
    xacc[...] = jnp.zeros_like(xacc)

    def unit(t, u, k0):
        sls = [slot(t, u, i) for i in range(2)]
        for sl in sls:
            r_copy(sl).wait()
            rbuf[:, span(sl)] = EMA_DECAY * rbuf[:, span(sl)] + (1.0 - EMA_DECAY) * jnp.dot(
                gt[...], gbuf[sl], preferred_element_type=jnp.float32)
        lrow = pl.ds(pl.multiple_of(me * nl, nl), nl)
        for i, sl in enumerate(sls):
            rr_copy(sl, k0 + i).wait()
            rr[k0 + i, pl.ds(cols, nl), :] = gbuf[sl, lrow, :]
        xacc[...] += _nt(rr[k0], gbuf[sls[0]]) + _nt(rr[k0 + 1], gbuf[sls[1]])

    def arrived(sl):
        piece(sl, send_d.at[0], mate).wait_recv()

    def step(t, carry):
        k0 = 4 * lax.rem(t, AHEAD)
        s = t - 2

        @pl.when(t == 1)
        def _():
            for q in range(SPLIT):
                arrived(mate * SPLIT + q)

        @pl.when(t >= 2)
        def _():
            a, b = slot(t, 0, 0), slot(t, 0, 1)
            arrived(a)
            arrived(b)

            @pl.when(s < 2)
            def _():
                piece(a, send_p.at[SPLIT + s], plus).start()
                piece(b, send_m.at[SPLIT + s], minus).start()
            piece(a, send_d.at[SPLIT + 2 * s], mate).start()
            piece(b, send_d.at[SPLIT + 2 * s + 1], mate).start()

            @pl.when(s == 1)
            def _():
                lpart(minus, 0, nl, 0, 0, plus).wait_recv()
                lpart(plus, 0, nl, 1, 1, minus).wait_recv()
                lpart(minus, 0, hl, 3, 2, plus).start()
                lpart(plus, hl, hl, 4, 3, minus).start()
                lpart(minus, 0, nl, 5, 5, mate).start()
                lpart(plus, 0, nl, 6, 6, mate).start()

            @pl.when(s == steps - 1)
            def _():
                far = ring(me + 4)
                lpart(far, 0, hl, 3, 2, plus).wait_recv()
                lpart(far, hl, hl, 4, 3, minus).wait_recv()
                lpart(far, 0, nl, 7, 7, mate).start()

        unit(t, 0, k0)

        @pl.when(t >= 2)
        def _():
            arrived(slot(t, 1, 0))
            arrived(slot(t, 1, 1))
        unit(t, 1, k0 + 2)

        @pl.when(t + AHEAD < steps + 2)
        def _():
            loads(t + AHEAD, k0)
        return carry

    lax.fori_loop(0, steps + 2, step, 0)

    for r_idx in (4, 5, 6, 7):
        lpart(me, 0, nl, 2, r_idx, mate).wait_recv()
    for s in range(steps):
        piece(me * SPLIT, send_p.at[s], plus).wait_send()
        piece(me * SPLIT, send_m.at[s], minus).wait_send()
    for s in range(SPLIT + 2 * steps):
        piece(me * SPLIT, send_d.at[s], mate).wait_send()
    for k in range(8):
        lpart(me, 0, hl if k in (3, 4) else nl, k, 0, mate).wait_send()


def _finish_kernel(xacc, lbuf, left, l_out, d_out):
    cols = d_out.shape[1]
    l_out[...] = EMA_DECAY * left[...] + (1.0 - EMA_DECAY) * xacc[pl.ds(cols, left.shape[0]), :]
    d_out[...] = _nt(lbuf[...], xacc[pl.ds(0, cols), :].astype(jnp.bfloat16))


def solution(mesh):
    row_spec = P(("layer", "tensor"), None)
    col_spec = P("layer", "tensor")
    n = mesh.shape["tensor"]

    def local_step(grad, left, right, lroot, rroot):
        rows, cols = grad.shape
        nl = lroot.shape[0]
        width = cols // SPLIT
        f32, bf16 = jnp.float32, jnp.bfloat16
        dma = pltpu.SemaphoreType.DMA
        rbuf, xacc, lbuf = pl.pallas_call(
            functools.partial(_gather_kernel, n),
            out_shape=(pltpu.VMEM(right.shape, f32), pltpu.VMEM((cols + nl, rows), f32), pltpu.VMEM((rows, rows), bf16)),
            in_specs=[ANY] * 4,
            out_specs=(VMEM,) * 3,
            scratch_shapes=[
                pltpu.VMEM((n * SPLIT, rows, width), bf16),
                pltpu.VMEM((cols, rows), bf16),
                pltpu.VMEM((4 * AHEAD, cols + nl, width), bf16),
                dma((SPLIT,)), dma((n * SPLIT,)), dma((4 * AHEAD,)), dma((n * SPLIT,)),
                dma((6,)), dma((6,)), dma((16,)),
                dma(()), dma((8,)), dma((8,)),
            ],
            compiler_params=pltpu.CompilerParams(collective_id=0, has_side_effects=True, vmem_limit_bytes=24 << 20),
        )(grad, lroot, right, rroot)
        l, d = pl.pallas_call(
            _finish_kernel,
            out_shape=(jax.ShapeDtypeStruct((nl, rows), f32), jax.ShapeDtypeStruct((rows, cols), f32)),
            in_specs=[VMEM] * 3,
            out_specs=(VMEM,) * 2,
            compiler_params=pltpu.CompilerParams(vmem_limit_bytes=8 << 20),
        )(xacc, lbuf, left)
        return l, rbuf, d

    return jax.shard_map(local_step, mesh=mesh, in_specs=(col_spec, row_spec, row_spec, row_spec, row_spec), out_specs=(row_spec, row_spec, col_spec), check_vma=False)
```

```python
import functools

import jax
import jax.numpy as jnp
from jax import lax
from jax.experimental import pallas as pl
from jax.experimental.pallas import tpu as pltpu
from jax.sharding import PartitionSpec as P

EMA_DECAY = 0.9
SPLIT = 4
AHEAD = 3
GRANT = 12 << 20

MESH = pl.DeviceIdType.MESH
ANY = pl.BlockSpec(memory_space=pl.ANY)
VMEM = pl.BlockSpec(memory_space=pltpu.VMEM)


def _nt(a, b):
    return lax.dot_general(a, b, (((1,), (1,)), ((), ())), preferred_element_type=jnp.float32)


def _slot(n, me, t, u, i):
    mate = me + 1 - 2 * (me % 2)
    base = jnp.where(u == 0, me, mate)
    s = t - 2
    far = 2 + 2 * (s // SPLIT)
    owner = jnp.where(i == 0, base - far, base + far)
    part = (s + 2 * i) % SPLIT
    owner = jnp.where(t == 0, me, jnp.where(t == 1, mate, owner))
    part = jnp.where(t < 2, 2 * u + i, part)
    return lax.rem(owner + n, n) * SPLIT + part


def _gather_kernel(n, grad, lroot, right, rroot, rbuf, xacc, lbuf, gbuf, gt, rr,
                   own_sem, r_sem, rr_sem, recv, send_p, send_m, send_d,
                   l_own, l_recv, l_send):
    me = lax.axis_index("tensor")
    mate = me + 1 - 2 * (me % 2)
    rows, width = gbuf.shape[1], gbuf.shape[2]
    cols = gt.shape[0]
    nl = lroot.shape[0]
    hl = nl // 2
    steps = 6
    ring = lambda d: lax.rem(d + n, n)
    plus, minus = ring(me + 2), ring(me - 2)

    slot = functools.partial(_slot, n, me)

    def span(sl):
        return pl.ds(pl.multiple_of(sl * width, width), width)

    def r_copy(sl):
        return pltpu.make_async_copy(right.at[:, span(sl)], rbuf.at[:, span(sl)], r_sem.at[sl])

    def rr_copy(sl, k):
        return pltpu.make_async_copy(rroot.at[:, span(sl)], rr.at[k, pl.ds(0, cols)], rr_sem.at[k])

    def own_copy(q):
        return pltpu.make_async_copy(grad.at[:, pl.ds(q * width, width)], gbuf.at[me * SPLIT + q], own_sem.at[q])

    def piece(sl, sem, dev):
        return pltpu.make_async_remote_copy(
            src_ref=gbuf.at[sl], dst_ref=gbuf.at[sl], send_sem=sem, recv_sem=recv.at[sl],
            device_id={"tensor": dev}, device_id_type=MESH)

    def lpart(owner, first, count, s_idx, r_idx, dev):
        at = pl.ds(pl.multiple_of(owner * nl + first, hl), count)
        return pltpu.make_async_remote_copy(
            src_ref=lbuf.at[at], dst_ref=lbuf.at[at], send_sem=l_send.at[s_idx], recv_sem=l_recv.at[r_idx],
            device_id={"tensor": dev}, device_id_type=MESH)

    own = [own_copy(q) for q in range(SPLIT)]
    for c in own:
        c.start()
    lown = pltpu.make_async_copy(lroot, lbuf.at[pl.ds(pl.multiple_of(me * nl, nl), nl)], l_own)
    lown.start()

    def loads(t, k0):
        for u in range(2):
            for i in range(2):
                sl = slot(t, u, i)
                r_copy(sl).start()
                rr_copy(sl, k0 + 2 * u + i).start()

    barrier = pltpu.get_barrier_semaphore()
    for dev in (plus, minus, mate):
        pl.semaphore_signal(barrier, inc=1, device_id={"tensor": dev}, device_id_type=MESH)
    pl.semaphore_wait(barrier, 3)

    for c in own:
        c.wait()
    lown.wait()
    sent = []
    for s in range(SPLIT):
        sent.append(piece(me * SPLIT + s, send_p.at[s], plus))
        sent.append(piece(me * SPLIT + (s + 2) % SPLIT, send_m.at[s], minus))
        sent.append(piece(me * SPLIT + s, send_d.at[s], mate))
        if s == 0:
            sent.append(lpart(me, 0, nl, 0, 0, plus))
            sent.append(lpart(me, 0, nl, 1, 1, minus))
            sent.append(lpart(me, 0, nl, 2, 4, mate))
    for c in sent:
        c.start()
    for t in range(AHEAD):
        loads(t, 4 * t)
    for q in range(SPLIT):
        gt[pl.ds(q * width, width), :] = gbuf[me * SPLIT + q].T
    xacc[...] = jnp.zeros_like(xacc)

    lrow = pl.ds(pl.multiple_of(me * nl, nl), nl)

    def ready(t, u, k0):
        for i in range(2):
            sl = slot(t, u, i)
            r_copy(sl).wait()
            rr_copy(sl, k0 + i).wait()
            rr[k0 + i, pl.ds(cols, nl), :] = gbuf[sl, lrow, :]

    def unit(t, u, k0):
        ready(t, u, k0)
        sls = [slot(t, u, i) for i in range(2)]
        for sl in sls:
            rbuf[:, span(sl)] = EMA_DECAY * rbuf[:, span(sl)] + (1.0 - EMA_DECAY) * jnp.dot(
                gt[...], gbuf[sl], preferred_element_type=jnp.float32)
        xacc[...] += _nt(rr[k0], gbuf[sls[0]]) + _nt(rr[k0 + 1], gbuf[sls[1]])

    def arrived(sl):
        piece(sl, send_d.at[0], mate).wait_recv()

    def take(t):
        s = t - 2

        @pl.when(t == 1)
        def _():
            for q in range(SPLIT):
                arrived(mate * SPLIT + q)

        @pl.when(t >= 2)
        def _():
            a, b = slot(t, 0, 0), slot(t, 0, 1)
            arrived(a)
            arrived(b)

            @pl.when(s < 2)
            def _():
                piece(a, send_p.at[SPLIT + s], plus).start()
                piece(b, send_m.at[SPLIT + s], minus).start()
            piece(a, send_d.at[SPLIT + 2 * s], mate).start()
            piece(b, send_d.at[SPLIT + 2 * s + 1], mate).start()

            @pl.when(s == 1)
            def _():
                lpart(minus, 0, nl, 0, 0, plus).wait_recv()
                lpart(plus, 0, nl, 1, 1, minus).wait_recv()
                lpart(minus, 0, hl, 3, 2, plus).start()
                lpart(plus, hl, hl, 4, 3, minus).start()
                lpart(minus, 0, nl, 5, 5, mate).start()
                lpart(plus, 0, nl, 6, 6, mate).start()

            @pl.when(s == steps - 1)
            def _():
                far = ring(me + 4)
                lpart(far, 0, hl, 3, 2, plus).wait_recv()
                lpart(far, hl, hl, 4, 3, minus).wait_recv()
                lpart(far, 0, nl, 7, 7, mate).start()

    def take_mate(t):
        @pl.when(t >= 2)
        def _():
            arrived(slot(t, 1, 0))
            arrived(slot(t, 1, 1))

    def step(t, carry):
        k0 = 4 * lax.rem(t, AHEAD)
        take(t)
        unit(t, 0, k0)
        take_mate(t)
        unit(t, 1, k0 + 2)

        @pl.when(t + AHEAD < steps + 2)
        def _():
            loads(t + AHEAD, k0)
        return carry

    lax.fori_loop(0, steps + 1, step, 0)
    last = steps + 1
    k0 = 4 * (last % AHEAD)
    take(last)
    ready(last, 0, k0)
    take_mate(last)
    ready(last, 1, k0 + 2)

    for r_idx in (4, 5, 6, 7):
        lpart(me, 0, nl, 2, r_idx, mate).wait_recv()
    for s in range(steps):
        piece(me * SPLIT, send_p.at[s], plus).wait_send()
        piece(me * SPLIT, send_m.at[s], minus).wait_send()
    for s in range(SPLIT + 2 * steps):
        piece(me * SPLIT, send_d.at[s], mate).wait_send()
    for k in range(8):
        lpart(me, 0, hl if k in (3, 4) else nl, k, 0, mate).wait_send()


def _write_kernel(n, rbuf, xacc, lbuf, gbuf, gt, rr, left, r_out, l_out, d_out,
                  tail, xs, d_buf, l_buf, r_sem, sem):
    me = lax.axis_index("tensor")
    mate = me + 1 - 2 * (me % 2)
    width = gbuf.shape[2]
    cols, nl = d_buf.shape[1], left.shape[0]
    last = 7
    k0 = 4 * (last % AHEAD)

    def span(sl):
        return pl.ds(pl.multiple_of(sl * width, width), width)

    tails = [_slot(n, me, last, u, i) for u in range(2) for i in range(2)]
    copies = []
    for t in range(last):
        for u in range(2):
            for i in range(2):
                at = span(_slot(n, me, t, u, i))
                copies.append(pltpu.make_async_copy(rbuf.at[:, at], r_out.at[:, at], r_sem.at[len(copies)]))
                copies[-1].start()
    for k, sl in enumerate(tails):
        tail[k] = EMA_DECAY * rbuf[:, span(sl)] + (1.0 - EMA_DECAY) * jnp.dot(
            gt[...], gbuf[sl], preferred_element_type=jnp.float32)
        copies.append(pltpu.make_async_copy(tail.at[k], r_out.at[:, span(sl)], r_sem.at[len(copies)]))
        copies[-1].start()
    xs[...] = xacc[...] + _nt(rr[k0], gbuf[tails[0]]) + _nt(rr[k0 + 1], gbuf[tails[1]])
    xs[...] += _nt(rr[k0 + 2], gbuf[tails[2]]) + _nt(rr[k0 + 3], gbuf[tails[3]])
    l_buf[...] = EMA_DECAY * left[...] + (1.0 - EMA_DECAY) * xs[pl.ds(cols, nl), :]
    d_buf[...] = _nt(lbuf[...], xs[pl.ds(0, cols), :].astype(jnp.bfloat16))
    copies.append(pltpu.make_async_copy(l_buf, l_out, sem.at[0]))
    copies[-1].start()
    copies.append(pltpu.make_async_copy(d_buf, d_out, sem.at[1]))
    copies[-1].start()
    for c in copies:
        c.wait()


def solution(mesh):
    row_spec = P(("layer", "tensor"), None)
    col_spec = P("layer", "tensor")
    n = mesh.shape["tensor"]

    def local_step(grad, left, right, lroot, rroot):
        rows, cols = grad.shape
        nl = lroot.shape[0]
        width = cols // SPLIT
        f32, bf16 = jnp.float32, jnp.bfloat16
        dma = pltpu.SemaphoreType.DMA
        held = pl.pallas_call(
            functools.partial(_gather_kernel, n),
            out_shape=(pltpu.VMEM(right.shape, f32), pltpu.VMEM((cols + nl, rows), f32), pltpu.VMEM((rows, rows), bf16),
                       pltpu.VMEM((n * SPLIT, rows, width), bf16), pltpu.VMEM((cols, rows), bf16),
                       pltpu.VMEM((4 * AHEAD, cols + nl, width), bf16)),
            in_specs=[ANY] * 4,
            out_specs=(VMEM,) * 6,
            scratch_shapes=[
                dma((SPLIT,)), dma((n * SPLIT,)), dma((4 * AHEAD,)), dma((n * SPLIT,)),
                dma((6,)), dma((6,)), dma((16,)),
                dma(()), dma((8,)), dma((8,)),
            ],
            compiler_params=pltpu.CompilerParams(collective_id=0, has_side_effects=True, vmem_limit_bytes=GRANT),
        )(grad, lroot, right, rroot)
        r, l, d = pl.pallas_call(
            functools.partial(_write_kernel, n),
            out_shape=(jax.ShapeDtypeStruct(right.shape, f32), jax.ShapeDtypeStruct((nl, rows), f32),
                       jax.ShapeDtypeStruct((rows, cols), f32)),
            in_specs=[VMEM] * 7,
            out_specs=(ANY,) * 3,
            scratch_shapes=[pltpu.VMEM((4, cols, width), f32), pltpu.VMEM((cols + nl, rows), f32),
                            pltpu.VMEM((rows, cols), f32), pltpu.VMEM((nl, rows), f32), dma((n * SPLIT,)), dma((2,))],
            compiler_params=pltpu.CompilerParams(vmem_limit_bytes=GRANT),
        )(*[pltpu.with_memory_space_constraint(v, pltpu.VMEM) for v in held], left)
        return l, r, d

    return jax.shard_map(local_step, mesh=mesh, in_specs=(col_spec, row_spec, row_spec, row_spec, row_spec), out_specs=(row_spec, row_spec, col_spec), check_vma=False)
```

```python
import functools

import jax
import jax.numpy as jnp
from jax import lax
from jax.experimental import pallas as pl
from jax.experimental.pallas import tpu as pltpu
from jax.sharding import PartitionSpec as P

EMA_DECAY = 0.9
SPLIT = 4
AHEAD = 3
GRANT = 12 << 20

MESH = pl.DeviceIdType.MESH
ANY = pl.BlockSpec(memory_space=pl.ANY)
VMEM = pl.BlockSpec(memory_space=pltpu.VMEM)


def _nt(a, b):
    return lax.dot_general(a, b, (((1,), (1,)), ((), ())), preferred_element_type=jnp.float32)


def _slot(n, me, t, u, i):
    mate = me + 1 - 2 * (me % 2)
    base = jnp.where(u == 0, me, mate)
    s = t - 2
    far = 2 + 2 * (s // SPLIT)
    owner = jnp.where(i == 0, base - far, base + far)
    part = (s + 2 * i) % SPLIT
    owner = jnp.where(t == 0, me, jnp.where(t == 1, mate, owner))
    part = jnp.where(t < 2, 2 * u + i, part)
    return lax.rem(owner + n, n) * SPLIT + part


def _gather_kernel(n, grad, lroot, right, rroot, rbuf, xacc, lbuf, gbuf, gt, rr,
                   own_sem, r_sem, rr_sem, recv, send_p, send_m, send_d,
                   l_own, l_recv, l_send):
    me = lax.axis_index("tensor")
    mate = me + 1 - 2 * (me % 2)
    rows, width = gbuf.shape[1], gbuf.shape[2]
    cols = gt.shape[0]
    nl = lroot.shape[0]
    hl = nl // 2
    steps = 6
    ring = lambda d: lax.rem(d + n, n)
    plus, minus = ring(me + 2), ring(me - 2)

    slot = functools.partial(_slot, n, me)

    def span(sl):
        return pl.ds(pl.multiple_of(sl * width, width), width)

    def r_copy(sl):
        return pltpu.make_async_copy(right.at[:, span(sl)], rbuf.at[:, span(sl)], r_sem.at[sl])

    def rr_copy(sl, k):
        return pltpu.make_async_copy(rroot.at[:, span(sl)], rr.at[k, pl.ds(0, cols)], rr_sem.at[k])

    def own_copy(q):
        return pltpu.make_async_copy(grad.at[:, pl.ds(q * width, width)], gbuf.at[me * SPLIT + q], own_sem.at[q])

    def piece(sl, sem, dev):
        return pltpu.make_async_remote_copy(
            src_ref=gbuf.at[sl], dst_ref=gbuf.at[sl], send_sem=sem, recv_sem=recv.at[sl],
            device_id={"tensor": dev}, device_id_type=MESH)

    def lpart(owner, first, count, s_idx, r_idx, dev):
        at = pl.ds(pl.multiple_of(owner * nl + first, hl), count)
        return pltpu.make_async_remote_copy(
            src_ref=lbuf.at[at], dst_ref=lbuf.at[at], send_sem=l_send.at[s_idx], recv_sem=l_recv.at[r_idx],
            device_id={"tensor": dev}, device_id_type=MESH)

    own = [own_copy(q) for q in range(SPLIT)]
    for c in own:
        c.start()
    lown = pltpu.make_async_copy(lroot, lbuf.at[pl.ds(pl.multiple_of(me * nl, nl), nl)], l_own)
    lown.start()

    def loads(t, k0):
        for u in range(2):
            for i in range(2):
                sl = slot(t, u, i)
                r_copy(sl).start()
                rr_copy(sl, k0 + 2 * u + i).start()

    barrier = pltpu.get_barrier_semaphore()
    for dev in (plus, minus, mate):
        pl.semaphore_signal(barrier, inc=1, device_id={"tensor": dev}, device_id_type=MESH)
    pl.semaphore_wait(barrier, 3)

    for c in own:
        c.wait()
    lown.wait()
    sent = []
    for s in range(SPLIT):
        sent.append(piece(me * SPLIT + s, send_p.at[s], plus))
        sent.append(piece(me * SPLIT + (s + 2) % SPLIT, send_m.at[s], minus))
        sent.append(piece(me * SPLIT + s, send_d.at[s], mate))
        if s == 0:
            sent.append(lpart(me, 0, nl, 0, 0, plus))
            sent.append(lpart(me, 0, nl, 1, 1, minus))
            sent.append(lpart(me, 0, nl, 2, 4, mate))
    for c in sent:
        c.start()
    for t in range(AHEAD):
        loads(t, 4 * t)
    for q in range(SPLIT):
        gt[pl.ds(q * width, width), :] = gbuf[me * SPLIT + q].T
    xacc[...] = jnp.zeros_like(xacc)

    lrow = pl.ds(pl.multiple_of(me * nl, nl), nl)

    def ready(t, u, k0):
        for i in range(2):
            sl = slot(t, u, i)
            r_copy(sl).wait()
            rr_copy(sl, k0 + i).wait()
            rr[k0 + i, pl.ds(cols, nl), :] = gbuf[sl, lrow, :]

    def unit(t, u, k0):
        ready(t, u, k0)
        sls = [slot(t, u, i) for i in range(2)]
        for sl in sls:
            rbuf[:, span(sl)] = EMA_DECAY * rbuf[:, span(sl)] + (1.0 - EMA_DECAY) * jnp.dot(
                gt[...], gbuf[sl], preferred_element_type=jnp.float32)
        xacc[...] += _nt(rr[k0], gbuf[sls[0]]) + _nt(rr[k0 + 1], gbuf[sls[1]])

    def arrived(sl):
        piece(sl, send_d.at[0], mate).wait_recv()

    def take(t):
        s = t - 2

        @pl.when(t == 1)
        def _():
            for q in range(SPLIT):
                arrived(mate * SPLIT + q)

        @pl.when(t >= 2)
        def _():
            a, b = slot(t, 0, 0), slot(t, 0, 1)
            arrived(a)
            arrived(b)

            @pl.when(s < 2)
            def _():
                piece(a, send_p.at[SPLIT + s], plus).start()
                piece(b, send_m.at[SPLIT + s], minus).start()
            piece(a, send_d.at[SPLIT + 2 * s], mate).start()
            piece(b, send_d.at[SPLIT + 2 * s + 1], mate).start()

            @pl.when(s == 1)
            def _():
                lpart(minus, 0, nl, 0, 0, plus).wait_recv()
                lpart(plus, 0, nl, 1, 1, minus).wait_recv()
                lpart(minus, 0, hl, 3, 2, plus).start()
                lpart(plus, hl, hl, 4, 3, minus).start()
                lpart(minus, 0, nl, 5, 5, mate).start()
                lpart(plus, 0, nl, 6, 6, mate).start()

            @pl.when(s == steps - 1)
            def _():
                far = ring(me + 4)
                lpart(far, 0, hl, 3, 2, plus).wait_recv()
                lpart(far, hl, hl, 4, 3, minus).wait_recv()
                lpart(far, 0, nl, 7, 7, mate).start()

    def take_mate(t):
        @pl.when(t >= 2)
        def _():
            arrived(slot(t, 1, 0))
            arrived(slot(t, 1, 1))

    def step(t, carry):
        k0 = 4 * lax.rem(t, AHEAD)
        take(t)
        unit(t, 0, k0)
        take_mate(t)
        unit(t, 1, k0 + 2)

        @pl.when(t + AHEAD < steps + 2)
        def _():
            loads(t + AHEAD, k0)
        return carry

    lax.fori_loop(0, steps + 1, step, 0)
    last = steps + 1
    k0 = 4 * (last % AHEAD)
    take(last)
    ready(last, 0, k0)
    take_mate(last)
    ready(last, 1, k0 + 2)

    for r_idx in (4, 5, 6, 7):
        lpart(me, 0, nl, 2, r_idx, mate).wait_recv()
    for s in range(steps):
        piece(me * SPLIT, send_p.at[s], plus).wait_send()
        piece(me * SPLIT, send_m.at[s], minus).wait_send()
    for s in range(SPLIT + 2 * steps):
        piece(me * SPLIT, send_d.at[s], mate).wait_send()
    for k in range(8):
        lpart(me, 0, hl if k in (3, 4) else nl, k, 0, mate).wait_send()


def _write_kernel(n, rbuf, xacc, lbuf, gbuf, gt, rr, left, r_out, l_out, d_out,
                  tail, xs, d_buf, l_buf, r_sem, sem):
    me = lax.axis_index("tensor")
    mate = me + 1 - 2 * (me % 2)
    width = gbuf.shape[2]
    cols, nl = d_buf.shape[1], left.shape[0]
    last = 7
    k0 = 4 * (last % AHEAD)

    def span(sl):
        return pl.ds(pl.multiple_of(sl * width, width), width)

    tails = [_slot(n, me, last, u, i) for u in range(2) for i in range(2)]
    copies = []
    for t in range(last):
        for u in range(2):
            for i in range(2):
                at = span(_slot(n, me, t, u, i))
                copies.append(pltpu.make_async_copy(rbuf.at[:, at], r_out.at[:, at], r_sem.at[len(copies)]))
                copies[-1].start(priority=len(copies) % 2)
    for k, sl in enumerate(tails):
        tail[k] = EMA_DECAY * rbuf[:, span(sl)] + (1.0 - EMA_DECAY) * jnp.dot(
            gt[...], gbuf[sl], preferred_element_type=jnp.float32)
        copies.append(pltpu.make_async_copy(tail.at[k], r_out.at[:, span(sl)], r_sem.at[len(copies)]))
        copies[-1].start(priority=len(copies) % 2)
    xs[...] = xacc[...] + _nt(rr[k0], gbuf[tails[0]]) + _nt(rr[k0 + 1], gbuf[tails[1]])
    xs[...] += _nt(rr[k0 + 2], gbuf[tails[2]]) + _nt(rr[k0 + 3], gbuf[tails[3]])
    l_buf[...] = EMA_DECAY * left[...] + (1.0 - EMA_DECAY) * xs[pl.ds(cols, nl), :]
    d_buf[...] = _nt(lbuf[...], xs[pl.ds(0, cols), :].astype(jnp.bfloat16))
    copies.append(pltpu.make_async_copy(l_buf, l_out, sem.at[0]))
    copies[-1].start(priority=len(copies) % 2)
    copies.append(pltpu.make_async_copy(d_buf, d_out, sem.at[1]))
    copies[-1].start(priority=len(copies) % 2)
    for c in copies:
        c.wait()


def solution(mesh):
    row_spec = P(("layer", "tensor"), None)
    col_spec = P("layer", "tensor")
    n = mesh.shape["tensor"]

    def local_step(grad, left, right, lroot, rroot):
        rows, cols = grad.shape
        nl = lroot.shape[0]
        width = cols // SPLIT
        f32, bf16 = jnp.float32, jnp.bfloat16
        dma = pltpu.SemaphoreType.DMA
        held = pl.pallas_call(
            functools.partial(_gather_kernel, n),
            out_shape=(pltpu.VMEM(right.shape, f32), pltpu.VMEM((cols + nl, rows), f32), pltpu.VMEM((rows, rows), bf16),
                       pltpu.VMEM((n * SPLIT, rows, width), bf16), pltpu.VMEM((cols, rows), bf16),
                       pltpu.VMEM((4 * AHEAD, cols + nl, width), bf16)),
            in_specs=[ANY] * 4,
            out_specs=(VMEM,) * 6,
            scratch_shapes=[
                dma((SPLIT,)), dma((n * SPLIT,)), dma((4 * AHEAD,)), dma((n * SPLIT,)),
                dma((6,)), dma((6,)), dma((16,)),
                dma(()), dma((8,)), dma((8,)),
            ],
            compiler_params=pltpu.CompilerParams(collective_id=0, has_side_effects=True, vmem_limit_bytes=GRANT),
        )(grad, lroot, right, rroot)
        r, l, d = pl.pallas_call(
            functools.partial(_write_kernel, n),
            out_shape=(jax.ShapeDtypeStruct(right.shape, f32), jax.ShapeDtypeStruct((nl, rows), f32),
                       jax.ShapeDtypeStruct((rows, cols), f32)),
            in_specs=[VMEM] * 7,
            out_specs=(ANY,) * 3,
            scratch_shapes=[pltpu.VMEM((4, cols, width), f32), pltpu.VMEM((cols + nl, rows), f32),
                            pltpu.VMEM((rows, cols), f32), pltpu.VMEM((nl, rows), f32), dma((n * SPLIT,)), dma((2,))],
            compiler_params=pltpu.CompilerParams(vmem_limit_bytes=GRANT),
        )(*[pltpu.with_memory_space_constraint(v, pltpu.VMEM) for v in held], left)
        return l, r, d

    return jax.shard_map(local_step, mesh=mesh, in_specs=(col_spec, row_spec, row_spec, row_spec, row_spec), out_specs=(row_spec, row_spec, col_spec), check_vma=False)
```

```python
import jax
import jax.numpy as jnp
from jax import lax
from jax.experimental import pallas as pl
from jax.experimental.pallas import tpu as pltpu
from jax.sharding import PartitionSpec as P


EMA_DECAY = 0.9
WIDTH = 256
GRANT = 14 << 20


ANY = pl.BlockSpec(memory_space=pl.ANY)
VMEM = pl.BlockSpec(memory_space=pltpu.VMEM)


def _nt(a, b):
    return lax.dot_general(a, b, (((1,), (1,)), ((), ())), preferred_element_type=jnp.float32)


def _places(n, me, where, cols, span):
    mate = me + 1 - 2 * (me % 2)
    owners = [lax.rem((mate if swapped else me) + shift, n) for swapped, shift, _ in where]
    return owners, [owner * cols + half * span for owner, (_, _, half) in zip(owners, where)]


def _unit_kernel(n, where, nxt, *refs):
    refs = list(refs)
    m = len(where)
    first, last = refs.pop(0), refs.pop(0)
    take = lambda k: [refs.pop(0) for _ in range(k)]
    if not first:
        take(1)
    right, rroot, gt = take(3)
    chunks = take(m)
    if not first:
        r_in, rr_in, x_prev, l_prev = take(4)
    if last:
        left, r_out, l_out, d_out = take(4)
    else:
        r_out, r_next, rr_next, xs, lbuf = take(5)
    stage, w_sem, r_sem, rr_sem = take(4)
    if first:
        r_in, rr_in = take(2)
    if last:
        xs, lbuf, d_buf, l_buf, sem = take(5)
    me = lax.axis_index("tensor")
    cols, rows = gt.shape
    span = chunks[0].shape[1]
    nl = rows // n
    lrow = pl.ds(pl.multiple_of(me * nl, nl), nl)
    per = span // WIDTH

    def loads(places, r_to, rr_to, base):
        out = []
        for k, c0 in enumerate(places):
            for i in range(per):
                at = pl.ds(pl.multiple_of(c0 + i * WIDTH, WIDTH), WIDTH)
                s = k * per + i
                out.append(pltpu.make_async_copy(right.at[:, at], r_to.at[s], r_sem.at[base + s]))
            at = pl.ds(pl.multiple_of(c0, span), span)
            out.append(pltpu.make_async_copy(rroot.at[:, at], rr_to.at[k, pl.ds(0, cols)], rr_sem.at[base // per + k]))
        for c in out:
            c.start()
        return out

    owners, places = _places(n, me, where, cols, span)
    if first:
        mine = loads(places, r_in, rr_in, m * per)
    ahead = [] if last else loads(_places(n, me, nxt, cols, span)[1], r_next, rr_next, 0)
    if first:
        for c in mine:
            c.wait()
    if not first:
        lbuf[...] = l_prev[...]
    writes = []
    for k in range(m):
        for i in range(per):
            at = pl.ds(pl.multiple_of(places[k] + i * WIDTH, WIDTH), WIDTH)
            s = k * per + i
            stage[s] = EMA_DECAY * r_in[s] + (1.0 - EMA_DECAY) * jnp.dot(
                gt[...], chunks[k][pl.ds(0, rows), pl.ds(i * WIDTH, WIDTH)], preferred_element_type=jnp.float32)
            writes.append(pltpu.make_async_copy(stage.at[s], r_out.at[:, at], w_sem.at[s]))
            writes[-1].start()
    for k in range(m):
        if chunks[k].shape[0] > rows:
            lbuf[pl.ds(pl.multiple_of(owners[k] * nl, nl), nl), :] = chunks[k][pl.ds(rows, nl), :]
        h = chunks[k][pl.ds(0, rows), :]
        x_term, l_term = _nt(rr_in[k, pl.ds(0, cols)], h), _nt(chunks[k][lrow, :], h)
        top, low = pl.ds(0, cols), pl.ds(cols, nl)
        if k == 0 and first:
            xs[top, :], xs[low, :] = x_term, l_term
        else:
            old = xs if k else x_prev
            xs[top, :] = old[top, :] + x_term
            xs[low, :] = old[low, :] + l_term
    if last:
        d_buf[...] = _nt(lbuf[...], xs[pl.ds(0, cols), :].astype(jnp.bfloat16))
        writes.append(pltpu.make_async_copy(d_buf, d_out, sem.at[0]))
        writes[-1].start()
        l_buf[...] = EMA_DECAY * left[...] + (1.0 - EMA_DECAY) * xs[pl.ds(cols, nl), :]
        writes.append(pltpu.make_async_copy(l_buf, l_out, sem.at[1]))
        writes[-1].start()
    for w in writes + ahead:
        w.wait()


def _on_chip(v):
    return pltpu.with_memory_space_constraint(v, pltpu.VMEM)


def _unit(n, where, nxt, state, right, rroot, gt, chunks, left=None):
    first, last = state is None, left is not None
    m = len(where)
    cols, rows = gt.shape
    span = chunks[0].shape[1]
    nl = rows // n
    f32, bf16 = jnp.float32, gt.dtype
    dma = pltpu.SemaphoreType.DMA
    slabs = m * span // WIDTH
    args, specs = ([], []) if first else ([state[0]], [ANY])
    args += [right, rroot, gt, *[_on_chip(c) for c in chunks]]
    specs += [ANY, ANY, VMEM] + [VMEM] * m
    alias = {} if first else {0: 0}
    r_shape = jax.ShapeDtypeStruct(rroot.shape, f32)
    held = ((slabs, cols, WIDTH), f32), ((m, cols, span), bf16), ((cols + nl, rows), f32), ((rows, rows), bf16)
    scratch = [pltpu.VMEM((slabs, cols, WIDTH), f32), dma((slabs,)), dma((2 * slabs,)), dma((2 * m,))]
    if first:
        scratch += [pltpu.VMEM(*held[0]), pltpu.VMEM(*held[1])]
    else:
        if not last:
            alias.update({len(args) + 2: 3, len(args) + 3: 4})
        args += [_on_chip(v) for v in state[1:]]
        specs += [VMEM] * 4
    if last:
        args.append(left)
        specs.append(VMEM)
        out_shape = (r_shape, jax.ShapeDtypeStruct((nl, rows), f32), jax.ShapeDtypeStruct((rows, cols), f32))
        out_specs = (ANY,) * 3
        scratch += [pltpu.VMEM(*held[2]), pltpu.VMEM(*held[3]), pltpu.VMEM((rows, cols), f32),
                    pltpu.VMEM((nl, rows), f32), dma((2,))]
    else:
        out_shape = (r_shape, *[pltpu.VMEM(*h) for h in held])
        out_specs = (ANY,) + (VMEM,) * 4
    flops = 4 * rows * cols * m * span
    return pl.pallas_call(
        lambda *refs: _unit_kernel(n, where, nxt, first, last, *refs),
        out_shape=out_shape, in_specs=specs, out_specs=out_specs, scratch_shapes=scratch, input_output_aliases=alias,
        compiler_params=pltpu.CompilerParams(vmem_limit_bytes=GRANT),
        cost_estimate=pl.CostEstimate(flops=flops, bytes_accessed=m * span * cols * 10, transcendentals=0),
    )(*args)


def solution(mesh):
    row_spec = P(("layer", "tensor"), None)
    col_spec = P("layer", "tensor")
    n = mesh.shape["tensor"]

    def shift(v, k):
        return lax.ppermute(v, "tensor", [(j, (j + k) % n) for j in range(n)])

    def swap(v):
        return lax.ppermute(v, "tensor", [(j, j ^ 1) for j in range(n)])

    def after(vals, state):
        out = lax.optimization_barrier((*vals, state[3], state[4]))
        return out[:-2], (*state[:3], *out[-2:])

    def both(swapped, da, ha, db, hb):
        return [(swapped, da % n, ha), (swapped, db % n, hb)]

    def group_step(grad, left, right, lroot, rroot):
        _, cols = grad.shape
        half = cols // 2
        p0, p1 = grad[:, :half], grad[:, half:]
        u0 = jnp.concatenate([p0, lroot], axis=0)
        u1 = jnp.concatenate([p1, lroot], axis=0)
        a0, b0 = shift(u0, 2), shift(u1, n - 2)
        a1, b1 = shift(p1, 2), shift(p0, n - 2)
        s = swap(u0), swap(u1)
        gt = _on_chip(grad.T)
        right, rroot = (pltpu.with_memory_space_constraint(v, pltpu.HBM) for v in (right, rroot))
        plan = [[(False, 0, 0), (False, 0, 1)], [(True, 0, 0), (True, 0, 1)]]
        for args in ((-2, 0, 2, 1), (-2, 1, 2, 0), (-4, 0, 4, 1)):
            plan += [both(False, *args), both(True, *args)]
        plan.append(None)

        def unit(k, state, chunks, *tail):
            return _unit(n, plan[k], plan[k + 1], state, right, rroot, gt, chunks, *tail)

        st = unit(0, None, [u0, u1])
        s, st = after(s, st)
        st = unit(1, st, s)
        (a0, b0), st = after((a0, b0), st)
        f = shift(a0, 2), shift(b0, n - 2)
        for k, got in ((2, (a0, b0)), (4, (a1, b1)), (6, f)):
            if k > 2:
                got, st = after(got, st)
            s = swap(got[0]), swap(got[1])
            st = unit(k, st, got)
            s, st = after(s, st)
            st = unit(k + 1, st, s, *([left] if k == 6 else []))
        r, l, d = st
        return l, r, d

    return jax.shard_map(group_step, mesh=mesh, in_specs=(col_spec, row_spec, row_spec, row_spec, row_spec), out_specs=(row_spec, row_spec, col_spec), check_vma=False)
```

```python
import functools

import jax
import jax.numpy as jnp
from jax import lax
from jax.experimental import pallas as pl
from jax.experimental.pallas import tpu as pltpu
from jax.sharding import PartitionSpec as P

EMA_DECAY = 0.9
SPLIT = 4
SUB = 4
AHEAD = 3
GRANT = 12 << 20

MESH = pl.DeviceIdType.MESH
ANY = pl.BlockSpec(memory_space=pl.ANY)
VMEM = pl.BlockSpec(memory_space=pltpu.VMEM)


def _nt(a, b):
    return lax.dot_general(a, b, (((1,), (1,)), ((), ())), preferred_element_type=jnp.float32)


def _slot(n, me, t, u, i):
    mate = me + 1 - 2 * (me % 2)
    base = jnp.where(u == 0, me, mate)
    s = t - 2
    far = 2 + 2 * (s // SPLIT)
    owner = jnp.where(i == 0, base - far, base + far)
    part = (s + 2 * i) % SPLIT
    owner = jnp.where(t == 0, me, jnp.where(t == 1, mate, owner))
    part = jnp.where(t < 2, 2 * u + i, part)
    return lax.rem(owner + n, n) * SPLIT + part


def _gather_kernel(n, grad, lroot, right, rroot, rbuf, xacc, lbuf, gbuf, gt, rr,
                   own_sem, r_sem, rr_sem, recv, recv_sub, send_p, send_m, send_d,
                   l_own, l_recv, l_send):
    me = lax.axis_index("tensor")
    mate = me + 1 - 2 * (me % 2)
    rows, width = gbuf.shape[1], gbuf.shape[2]
    cols = gt.shape[0]
    nl = lroot.shape[0]
    hl = nl // 2
    steps = 6
    ring = lambda d: lax.rem(d + n, n)
    plus, minus = ring(me + 2), ring(me - 2)

    slot = functools.partial(_slot, n, me)

    def span(sl):
        return pl.ds(pl.multiple_of(sl * width, width), width)

    def r_copy(sl):
        return pltpu.make_async_copy(right.at[:, span(sl)], rbuf.at[:, span(sl)], r_sem.at[sl])

    def rr_copy(sl, k):
        return pltpu.make_async_copy(rroot.at[:, span(sl)], rr.at[k, pl.ds(0, cols)], rr_sem.at[k])

    def own_copy(q):
        return pltpu.make_async_copy(grad.at[:, pl.ds(q * width, width)], gbuf.at[me * SPLIT + q], own_sem.at[q])

    def piece(sl, sem, dev):
        return pltpu.make_async_remote_copy(
            src_ref=gbuf.at[sl], dst_ref=gbuf.at[sl], send_sem=sem, recv_sem=recv.at[sl],
            device_id={"tensor": dev}, device_id_type=MESH)

    def part(sl, r, sem, group, dev):
        at = gbuf.at[sl, pl.ds(r * (rows // SUB), rows // SUB)]
        return pltpu.make_async_remote_copy(
            src_ref=at, dst_ref=at, send_sem=sem, recv_sem=recv_sub.at[group, r],
            device_id={"tensor": dev}, device_id_type=MESH)

    def lpart(owner, first, count, s_idx, r_idx, dev):
        at = pl.ds(pl.multiple_of(owner * nl + first, hl), count)
        return pltpu.make_async_remote_copy(
            src_ref=lbuf.at[at], dst_ref=lbuf.at[at], send_sem=l_send.at[s_idx], recv_sem=l_recv.at[r_idx],
            device_id={"tensor": dev}, device_id_type=MESH)

    own = [own_copy(q) for q in range(SPLIT)]
    for c in own:
        c.start()
    lown = pltpu.make_async_copy(lroot, lbuf.at[pl.ds(pl.multiple_of(me * nl, nl), nl)], l_own)
    lown.start()

    def loads(t, k0):
        for u in range(2):
            for i in range(2):
                sl = slot(t, u, i)
                r_copy(sl).start()
                rr_copy(sl, k0 + 2 * u + i).start()

    barrier = pltpu.get_barrier_semaphore()
    for dev in (plus, minus, mate):
        pl.semaphore_signal(barrier, inc=1, device_id={"tensor": dev}, device_id_type=MESH)
    pl.semaphore_wait(barrier, 3)

    landed = set()
    for s in range(SPLIT):
        for q in (s, (s + 2) % SPLIT):
            if q not in landed:
                own[q].wait()
                landed.add(q)
        piece(me * SPLIT + s, send_p.at[s], plus).start()
        piece(me * SPLIT + (s + 2) % SPLIT, send_m.at[s], minus).start()
        if s == 0:
            lown.wait()
            lpart(me, 0, nl, 0, 0, plus).start()
            lpart(me, 0, nl, 1, 1, minus).start()
    for s in range(SPLIT):
        piece(me * SPLIT + s, send_d.at[s], mate).start()
    lpart(me, 0, nl, 2, 4, mate).start()
    for t in range(AHEAD):
        loads(t, 4 * t)
    for q in range(SPLIT):
        gt[pl.ds(q * width, width), :] = gbuf[me * SPLIT + q].T
    xacc[...] = jnp.zeros_like(xacc)

    lrow = pl.ds(pl.multiple_of(me * nl, nl), nl)

    def ready(t, u, k0):
        for i in range(2):
            sl = slot(t, u, i)
            r_copy(sl).wait()
            rr_copy(sl, k0 + i).wait()
            rr[k0 + i, pl.ds(cols, nl), :] = gbuf[sl, lrow, :]

    def unit(t, u, k0):
        ready(t, u, k0)
        sls = [slot(t, u, i) for i in range(2)]
        for sl in sls:
            rbuf[:, span(sl)] = EMA_DECAY * rbuf[:, span(sl)] + (1.0 - EMA_DECAY) * jnp.dot(
                gt[...], gbuf[sl], preferred_element_type=jnp.float32)
        xacc[...] += _nt(rr[k0], gbuf[sls[0]]) + _nt(rr[k0 + 1], gbuf[sls[1]])

    def arrived(sl):
        piece(sl, send_d.at[0], mate).wait_recv()

    def take(t):
        s = t - 2

        @pl.when(t == 1)
        def _():
            for q in range(SPLIT):
                arrived(mate * SPLIT + q)

        @pl.when(t >= 2)
        def _():
            a, b = slot(t, 0, 0), slot(t, 0, 1)
            arrived(a)
            piece(a, send_d.at[SPLIT + 2 * s], mate).start()

            @pl.when(s == 0)
            def _():
                piece(a, send_p.at[SPLIT], plus).start()
            arrived(b)
            piece(b, send_d.at[SPLIT + 2 * s + 1], mate).start()

            @pl.when(s == 0)
            def _():
                piece(b, send_m.at[SPLIT], minus).start()

            @pl.when(s == 1)
            def _():
                lpart(minus, 0, nl, 0, 0, plus).wait_recv()
                lpart(plus, 0, nl, 1, 1, minus).wait_recv()
                lpart(minus, 0, hl, 3, 2, plus).start()
                lpart(plus, hl, hl, 4, 3, minus).start()
                for r in range(SUB):
                    part(a, r, send_p.at[SPLIT + 1 + r], 0, plus).start()
                    part(b, r, send_m.at[SPLIT + 1 + r], 1, minus).start()
                lpart(minus, 0, nl, 5, 5, mate).start()
                lpart(plus, 0, nl, 6, 6, mate).start()

    def take_last(t):
        far = ring(me + 4)
        lpart(far, 0, hl, 3, 2, plus).wait_recv()
        lpart(far, hl, hl, 4, 3, minus).wait_recv()
        lpart(far, 0, nl, 7, 7, mate).start()
        for r in range(SUB):
            for i in range(2):
                sl = slot(t, 0, i)
                part(sl, r, send_d.at[0], i, mate).wait_recv()
                part(sl, r, send_d.at[SPLIT + 2 * (steps - 1) + i * SUB + r], 2 + i, mate).start()

    def take_mate(t):
        @pl.when(t >= 2)
        def _():
            arrived(slot(t, 1, 0))
            arrived(slot(t, 1, 1))

    def step(t, carry):
        k0 = 4 * lax.rem(t, AHEAD)
        take(t)
        unit(t, 0, k0)
        take_mate(t)
        unit(t, 1, k0 + 2)

        @pl.when(t + AHEAD < steps + 2)
        def _():
            loads(t + AHEAD, k0)
        return carry

    lax.fori_loop(0, steps + 1, step, 0)
    last = steps + 1
    k0 = 4 * (last % AHEAD)
    take_last(last)
    ready(last, 0, k0)
    for r in range(SUB):
        for i in range(2):
            part(slot(last, 1, i), r, send_d.at[0], 2 + i, mate).wait_recv()
    ready(last, 1, k0 + 2)

    for r_idx in (4, 5, 6, 7):
        lpart(me, 0, nl, 2, r_idx, mate).wait_recv()
    for s in range(SPLIT + 1):
        piece(me * SPLIT, send_p.at[s], plus).wait_send()
        piece(me * SPLIT, send_m.at[s], minus).wait_send()
    for r in range(SUB):
        part(me * SPLIT, r, send_p.at[SPLIT + 1 + r], 0, plus).wait_send()
        part(me * SPLIT, r, send_m.at[SPLIT + 1 + r], 1, minus).wait_send()
    whole = SPLIT + 2 * (steps - 1)
    for s in range(whole):
        piece(me * SPLIT, send_d.at[s], mate).wait_send()
    for s in range(2 * SUB):
        part(me * SPLIT, 0, send_d.at[whole + s], 2, mate).wait_send()
    for k in range(8):
        lpart(me, 0, hl if k in (3, 4) else nl, k, 0, mate).wait_send()


def _write_kernel(n, rbuf, xacc, lbuf, gbuf, gt, rr, left, r_out, l_out, d_out,
                  tail, xs, d_buf, l_buf, r_sem, sem):
    me = lax.axis_index("tensor")
    width = gbuf.shape[2]
    cols, nl = d_buf.shape[1], left.shape[0]
    last = 7
    k0 = 4 * (last % AHEAD)

    def span(sl):
        return pl.ds(pl.multiple_of(sl * width, width), width)

    left_copy = pltpu.make_async_copy(left, l_buf, sem.at[0])
    left_copy.start()
    copies = []

    def write(src, dst):
        copies.append(pltpu.make_async_copy(src, dst, r_sem.at[len(copies)]))
        copies[-1].start()

    chips = n // 2
    far = me // 2 + chips // 2
    tall, wide = cols // 4, 2 * cols
    for c in range(1, chips):
        at = pl.ds(pl.multiple_of(lax.rem(far + c, chips) * wide, wide), wide)
        for p in range(4):
            block = (pl.ds(p * tall, tall), at)
            write(rbuf.at[block], r_out.at[block])
    for u in range(2):
        for i in range(2):
            at = span(_slot(n, me, last - 1, u, i))
            write(rbuf.at[:, at], r_out.at[:, at])
    tails = [_slot(n, me, last, u, i) for u in range(2) for i in range(2)]
    for k, sl in enumerate(tails):
        tail[k] = EMA_DECAY * rbuf[:, span(sl)] + (1.0 - EMA_DECAY) * jnp.dot(
            gt[...], gbuf[sl], preferred_element_type=jnp.float32)
        write(tail.at[k], r_out.at[:, span(sl)])
    xs[...] = xacc[...] + _nt(rr[k0], gbuf[tails[0]]) + _nt(rr[k0 + 1], gbuf[tails[1]])
    xs[...] += _nt(rr[k0 + 2], gbuf[tails[2]]) + _nt(rr[k0 + 3], gbuf[tails[3]])
    d_buf[...] = _nt(lbuf[...], xs[pl.ds(0, cols), :].astype(jnp.bfloat16))
    write(d_buf, d_out)
    left_copy.wait()
    l_buf[...] = EMA_DECAY * l_buf[...] + (1.0 - EMA_DECAY) * xs[pl.ds(cols, nl), :]
    write(l_buf, l_out)
    for c in copies:
        c.wait()


def solution(mesh):
    row_spec = P(("layer", "tensor"), None)
    col_spec = P("layer", "tensor")
    n = mesh.shape["tensor"]

    def local_step(grad, left, right, lroot, rroot):
        rows, cols = grad.shape
        nl = lroot.shape[0]
        width = cols // SPLIT
        f32, bf16 = jnp.float32, jnp.bfloat16
        dma = pltpu.SemaphoreType.DMA
        held = pl.pallas_call(
            functools.partial(_gather_kernel, n),
            out_shape=(pltpu.VMEM(right.shape, f32), pltpu.VMEM((cols + nl, rows), f32), pltpu.VMEM((rows, rows), bf16),
                       pltpu.VMEM((n * SPLIT, rows, width), bf16), pltpu.VMEM((cols, rows), bf16),
                       pltpu.VMEM((4 * AHEAD, cols + nl, width), bf16)),
            in_specs=[ANY] * 4,
            out_specs=(VMEM,) * 6,
            scratch_shapes=[
                dma((SPLIT,)), dma((n * SPLIT,)), dma((4 * AHEAD,)), dma((n * SPLIT,)),
                dma((4, SUB)), dma((SPLIT + 1 + SUB,)), dma((SPLIT + 1 + SUB,)), dma((SPLIT + 10 + 2 * SUB,)),
                dma(()), dma((8,)), dma((8,)),
            ],
            compiler_params=pltpu.CompilerParams(collective_id=0, has_side_effects=True, vmem_limit_bytes=GRANT),
        )(grad, lroot, right, rroot)
        r, l, d = pl.pallas_call(
            functools.partial(_write_kernel, n),
            out_shape=(jax.ShapeDtypeStruct(right.shape, f32), jax.ShapeDtypeStruct((nl, rows), f32),
                       jax.ShapeDtypeStruct((rows, cols), f32)),
            in_specs=[VMEM] * 6 + [ANY],
            out_specs=(ANY,) * 3,
            scratch_shapes=[pltpu.VMEM((4, cols, width), f32), pltpu.VMEM((cols + nl, rows), f32),
                            pltpu.VMEM((rows, cols), f32), pltpu.VMEM((nl, rows), f32), dma((22,)), dma((1,))],
            compiler_params=pltpu.CompilerParams(vmem_limit_bytes=GRANT),
        )(*[pltpu.with_memory_space_constraint(v, pltpu.VMEM) for v in held], left)
        return l, r, d

    return jax.shard_map(local_step, mesh=mesh, in_specs=(col_spec, row_spec, row_spec, row_spec, row_spec), out_specs=(row_spec, row_spec, col_spec), check_vma=False)
```

```python
import functools

import jax
import jax.numpy as jnp
from jax import lax
from jax.experimental import pallas as pl
from jax.experimental.pallas import tpu as pltpu
from jax.sharding import PartitionSpec as P

EMA_DECAY = 0.9
SPLIT = 4
SUB = 8
AHEAD = 3
GRANT = 12 << 20

MESH = pl.DeviceIdType.MESH
ANY = pl.BlockSpec(memory_space=pl.ANY)
VMEM = pl.BlockSpec(memory_space=pltpu.VMEM)


def _nt(a, b):
    return lax.dot_general(a, b, (((1,), (1,)), ((), ())), preferred_element_type=jnp.float32)


def _slot(n, me, t, u, i):
    mate = me + 1 - 2 * (me % 2)
    base = jnp.where(u == 0, me, mate)
    s = t - 2
    far = 2 + 2 * (s // SPLIT)
    owner = jnp.where(i == 0, base - far, base + far)
    part = (s + 2 * i) % SPLIT
    owner = jnp.where(t == 0, me, jnp.where(t == 1, mate, owner))
    part = jnp.where(t < 2, 2 * u + i, part)
    return lax.rem(owner + n, n) * SPLIT + part


def _gather_kernel(n, grad, lroot, right, rroot, rbuf, xacc, lbuf, gbuf, gt, rr,
                   own_sem, r_sem, rr_sem, recv, recv_sub, send_p, send_m, send_d,
                   l_own, l_recv, l_send):
    me = lax.axis_index("tensor")
    mate = me + 1 - 2 * (me % 2)
    rows, width = gbuf.shape[1], gbuf.shape[2]
    cols = gt.shape[0]
    nl = lroot.shape[0]
    hl = nl // 2
    steps = 6
    ring = lambda d: lax.rem(d + n, n)
    plus, minus = ring(me + 2), ring(me - 2)

    slot = functools.partial(_slot, n, me)

    def span(sl):
        return pl.ds(pl.multiple_of(sl * width, width), width)

    def r_copy(sl):
        return pltpu.make_async_copy(right.at[:, span(sl)], rbuf.at[:, span(sl)], r_sem.at[sl])

    def rr_copy(sl, k):
        return pltpu.make_async_copy(rroot.at[:, span(sl)], rr.at[k, pl.ds(0, cols)], rr_sem.at[k])

    def own_copy(q):
        return pltpu.make_async_copy(grad.at[:, pl.ds(q * width, width)], gbuf.at[me * SPLIT + q], own_sem.at[q])

    def piece(sl, sem, dev):
        return pltpu.make_async_remote_copy(
            src_ref=gbuf.at[sl], dst_ref=gbuf.at[sl], send_sem=sem, recv_sem=recv.at[sl],
            device_id={"tensor": dev}, device_id_type=MESH)

    def part(sl, r, sem, group, dev):
        at = gbuf.at[sl, pl.ds(r * (rows // SUB), rows // SUB)]
        return pltpu.make_async_remote_copy(
            src_ref=at, dst_ref=at, send_sem=sem, recv_sem=recv_sub.at[group, r],
            device_id={"tensor": dev}, device_id_type=MESH)

    def lpart(owner, first, count, s_idx, r_idx, dev):
        at = pl.ds(pl.multiple_of(owner * nl + first, hl), count)
        return pltpu.make_async_remote_copy(
            src_ref=lbuf.at[at], dst_ref=lbuf.at[at], send_sem=l_send.at[s_idx], recv_sem=l_recv.at[r_idx],
            device_id={"tensor": dev}, device_id_type=MESH)

    own = [own_copy(q) for q in range(SPLIT)]
    lown = pltpu.make_async_copy(lroot, lbuf.at[pl.ds(pl.multiple_of(me * nl, nl), nl)], l_own)
    lown.start()
    for q in (0, 2, 1, 3):
        own[q].start()

    def loads(t, k0):
        for u in range(2):
            for i in range(2):
                sl = slot(t, u, i)
                r_copy(sl).start()
                rr_copy(sl, k0 + 2 * u + i).start()

    barrier = pltpu.get_barrier_semaphore()
    for dev in (plus, minus, mate):
        pl.semaphore_signal(barrier, inc=1, device_id={"tensor": dev}, device_id_type=MESH)
    pl.semaphore_wait(barrier, 3)

    landed = set()
    lown.wait()
    lpart(me, 0, nl, 0, 0, plus).start()
    lpart(me, 0, nl, 1, 1, minus).start()
    for s in range(SPLIT):
        for q in (s, (s + 2) % SPLIT):
            if q not in landed:
                own[q].wait()
                landed.add(q)
        piece(me * SPLIT + s, send_p.at[s], plus).start()
        piece(me * SPLIT + (s + 2) % SPLIT, send_m.at[s], minus).start()
    for s in range(SPLIT):
        piece(me * SPLIT + s, send_d.at[s], mate).start()
    lpart(me, 0, nl, 2, 4, mate).start()
    for t in range(AHEAD):
        loads(t, 4 * t)
    for q in range(SPLIT):
        gt[pl.ds(q * width, width), :] = gbuf[me * SPLIT + q].T
    xacc[...] = jnp.zeros_like(xacc)

    lrow = pl.ds(pl.multiple_of(me * nl, nl), nl)

    def ready(t, u, k0):
        for i in range(2):
            sl = slot(t, u, i)
            r_copy(sl).wait()
            rr_copy(sl, k0 + i).wait()
            rr[k0 + i, pl.ds(cols, nl), :] = gbuf[sl, lrow, :]

    def unit(t, u, k0):
        ready(t, u, k0)
        sls = [slot(t, u, i) for i in range(2)]
        for sl in sls:
            rbuf[:, span(sl)] = EMA_DECAY * rbuf[:, span(sl)] + (1.0 - EMA_DECAY) * jnp.dot(
                gt[...], gbuf[sl], preferred_element_type=jnp.float32)
        xacc[...] += _nt(rr[k0], gbuf[sls[0]]) + _nt(rr[k0 + 1], gbuf[sls[1]])

    def arrived(sl):
        piece(sl, send_d.at[0], mate).wait_recv()

    def take(t):
        s = t - 2

        @pl.when(t == 1)
        def _():
            for q in range(SPLIT):
                arrived(mate * SPLIT + q)

        @pl.when(t >= 2)
        def _():
            a, b = slot(t, 0, 0), slot(t, 0, 1)
            arrived(a)
            piece(a, send_d.at[SPLIT + 2 * s], mate).start()

            @pl.when(s == 0)
            def _():
                piece(a, send_p.at[SPLIT], plus).start()
            arrived(b)
            piece(b, send_d.at[SPLIT + 2 * s + 1], mate).start()

            @pl.when(s == 0)
            def _():
                piece(b, send_m.at[SPLIT], minus).start()

            @pl.when(s == 1)
            def _():
                lpart(minus, 0, nl, 0, 0, plus).wait_recv()
                lpart(plus, 0, nl, 1, 1, minus).wait_recv()
                lpart(minus, 0, hl, 3, 2, plus).start()
                lpart(plus, hl, hl, 4, 3, minus).start()
                for r in range(SUB):
                    part(a, r, send_p.at[SPLIT + 1 + r], 0, plus).start()
                    part(b, r, send_m.at[SPLIT + 1 + r], 1, minus).start()
                lpart(minus, 0, nl, 5, 5, mate).start()
                lpart(plus, 0, nl, 6, 6, mate).start()

    def take_last(t):
        far = ring(me + 4)
        lpart(far, 0, hl, 3, 2, plus).wait_recv()
        lpart(far, hl, hl, 4, 3, minus).wait_recv()
        lpart(far, 0, nl, 7, 7, mate).start()
        for r in range(SUB):
            for i in range(2):
                sl = slot(t, 0, i)
                part(sl, r, send_d.at[0], i, mate).wait_recv()
                part(sl, r, send_d.at[SPLIT + 2 * (steps - 1) + i * SUB + r], 2 + i, mate).start()

    def take_mate(t):
        @pl.when(t >= 2)
        def _():
            arrived(slot(t, 1, 0))
            arrived(slot(t, 1, 1))

    def step(t, carry):
        k0 = 4 * lax.rem(t, AHEAD)
        take(t)
        unit(t, 0, k0)
        take_mate(t)
        unit(t, 1, k0 + 2)

        @pl.when(t + AHEAD < steps + 2)
        def _():
            loads(t + AHEAD, k0)
        return carry

    lax.fori_loop(0, steps + 1, step, 0)
    last = steps + 1
    k0 = 4 * (last % AHEAD)
    take_last(last)
    ready(last, 0, k0)
    for r in range(SUB):
        for i in range(2):
            part(slot(last, 1, i), r, send_d.at[0], 2 + i, mate).wait_recv()
    ready(last, 1, k0 + 2)

    for r_idx in (4, 5, 6, 7):
        lpart(me, 0, nl, 2, r_idx, mate).wait_recv()
    for s in range(SPLIT + 1):
        piece(me * SPLIT, send_p.at[s], plus).wait_send()
        piece(me * SPLIT, send_m.at[s], minus).wait_send()
    for r in range(SUB):
        part(me * SPLIT, r, send_p.at[SPLIT + 1 + r], 0, plus).wait_send()
        part(me * SPLIT, r, send_m.at[SPLIT + 1 + r], 1, minus).wait_send()
    whole = SPLIT + 2 * (steps - 1)
    for s in range(whole):
        piece(me * SPLIT, send_d.at[s], mate).wait_send()
    for s in range(2 * SUB):
        part(me * SPLIT, 0, send_d.at[whole + s], 2, mate).wait_send()
    for k in range(8):
        lpart(me, 0, hl if k in (3, 4) else nl, k, 0, mate).wait_send()


def _write_kernel(n, rbuf, xacc, lbuf, gbuf, gt, rr, left, r_out, l_out, d_out,
                  tail, xs, d_buf, l_buf, r_sem, sem):
    me = lax.axis_index("tensor")
    width = gbuf.shape[2]
    cols, nl = d_buf.shape[1], left.shape[0]
    last = 7
    k0 = 4 * (last % AHEAD)

    def span(sl):
        return pl.ds(pl.multiple_of(sl * width, width), width)

    left_copy = pltpu.make_async_copy(left, l_buf, sem.at[0])
    left_copy.start()
    copies = []

    def write(src, dst):
        copies.append(pltpu.make_async_copy(src, dst, r_sem.at[len(copies)]))
        copies[-1].start()

    chips = n // 2
    far = me // 2 + chips // 2
    tall, wide = cols // 2, 2 * cols
    for c in range(1, chips):
        at = pl.ds(pl.multiple_of(lax.rem(far + c, chips) * wide, wide), wide)
        for p in range(2):
            block = (pl.ds(p * tall, tall), at)
            write(rbuf.at[block], r_out.at[block])
    for u in range(2):
        for i in range(2):
            at = span(_slot(n, me, last - 1, u, i))
            write(rbuf.at[:, at], r_out.at[:, at])
    tails = [_slot(n, me, last, u, i) for u in range(2) for i in range(2)]
    for k, sl in enumerate(tails):
        tail[k] = EMA_DECAY * rbuf[:, span(sl)] + (1.0 - EMA_DECAY) * jnp.dot(
            gt[...], gbuf[sl], preferred_element_type=jnp.float32)
        write(tail.at[k], r_out.at[:, span(sl)])
    xs[...] = xacc[...] + _nt(rr[k0], gbuf[tails[0]]) + _nt(rr[k0 + 1], gbuf[tails[1]])
    xs[...] += _nt(rr[k0 + 2], gbuf[tails[2]]) + _nt(rr[k0 + 3], gbuf[tails[3]])
    d_buf[...] = _nt(lbuf[...], xs[pl.ds(0, cols), :].astype(jnp.bfloat16))
    write(d_buf, d_out)
    left_copy.wait()
    l_buf[...] = EMA_DECAY * l_buf[...] + (1.0 - EMA_DECAY) * xs[pl.ds(cols, nl), :]
    write(l_buf, l_out)
    for c in copies:
        c.wait()


def solution(mesh):
    row_spec = P(("layer", "tensor"), None)
    col_spec = P("layer", "tensor")
    n = mesh.shape["tensor"]

    def local_step(grad, left, right, lroot, rroot):
        rows, cols = grad.shape
        nl = lroot.shape[0]
        width = cols // SPLIT
        f32, bf16 = jnp.float32, jnp.bfloat16
        dma = pltpu.SemaphoreType.DMA
        held = pl.pallas_call(
            functools.partial(_gather_kernel, n),
            out_shape=(pltpu.VMEM(right.shape, f32), pltpu.VMEM((cols + nl, rows), f32), pltpu.VMEM((rows, rows), bf16),
                       pltpu.VMEM((n * SPLIT, rows, width), bf16), pltpu.VMEM((cols, rows), bf16),
                       pltpu.VMEM((4 * AHEAD, cols + nl, width), bf16)),
            in_specs=[ANY] * 4,
            out_specs=(VMEM,) * 6,
            scratch_shapes=[
                dma((SPLIT,)), dma((n * SPLIT,)), dma((4 * AHEAD,)), dma((n * SPLIT,)),
                dma((4, SUB)), dma((SPLIT + 1 + SUB,)), dma((SPLIT + 1 + SUB,)), dma((SPLIT + 10 + 2 * SUB,)),
                dma(()), dma((8,)), dma((8,)),
            ],
            compiler_params=pltpu.CompilerParams(collective_id=0, has_side_effects=True, vmem_limit_bytes=GRANT),
        )(grad, lroot, right, rroot)
        r, l, d = pl.pallas_call(
            functools.partial(_write_kernel, n),
            out_shape=(jax.ShapeDtypeStruct(right.shape, f32), jax.ShapeDtypeStruct((nl, rows), f32),
                       jax.ShapeDtypeStruct((rows, cols), f32)),
            in_specs=[VMEM] * 6 + [ANY],
            out_specs=(ANY,) * 3,
            scratch_shapes=[pltpu.VMEM((4, cols, width), f32), pltpu.VMEM((cols + nl, rows), f32),
                            pltpu.VMEM((rows, cols), f32), pltpu.VMEM((nl, rows), f32), dma((22,)), dma((1,))],
            compiler_params=pltpu.CompilerParams(vmem_limit_bytes=GRANT),
        )(*[pltpu.with_memory_space_constraint(v, pltpu.VMEM) for v in held], left)
        return l, r, d

    return jax.shard_map(local_step, mesh=mesh, in_specs=(col_spec, row_spec, row_spec, row_spec, row_spec), out_specs=(row_spec, row_spec, col_spec), check_vma=False)
```

```python
import functools

import jax
import jax.numpy as jnp
from jax import lax
from jax.experimental import pallas as pl
from jax.experimental.pallas import tpu as pltpu
from jax.sharding import PartitionSpec as P

EMA_DECAY = 0.9
SPLIT = 4
SUB = 2
AHEAD = 3
GRANT = 12 << 20

MESH = pl.DeviceIdType.MESH
ANY = pl.BlockSpec(memory_space=pl.ANY)
VMEM = pl.BlockSpec(memory_space=pltpu.VMEM)


def _nt(a, b):
    return lax.dot_general(a, b, (((1,), (1,)), ((), ())), preferred_element_type=jnp.float32)


def _slot(n, me, t, u, i):
    mate = me + 1 - 2 * (me % 2)
    base = jnp.where(u == 0, me, mate)
    s = t - 2
    far = 2 + 2 * (s // SPLIT)
    owner = jnp.where(i == 0, base - far, base + far)
    part = (s + 2 * i) % SPLIT
    owner = jnp.where(t == 0, me, jnp.where(t == 1, mate, owner))
    part = jnp.where(t < 2, 2 * u + i, part)
    return lax.rem(owner + n, n) * SPLIT + part


def _gather_kernel(n, grad, lroot, right, rroot, rbuf, xacc, lbuf, gbuf, gt, rr,
                   own_sem, r_sem, rr_sem, recv, recv_sub, send_p, send_m, send_d,
                   l_own, l_recv, l_send):
    me = lax.axis_index("tensor")
    mate = me + 1 - 2 * (me % 2)
    rows, width = gbuf.shape[1], gbuf.shape[2]
    cols = gt.shape[0]
    nl = lroot.shape[0]
    hl = nl // 2
    steps = 6
    ring = lambda d: lax.rem(d + n, n)
    plus, minus = ring(me + 2), ring(me - 2)

    slot = functools.partial(_slot, n, me)

    def span(sl):
        return pl.ds(pl.multiple_of(sl * width, width), width)

    def r_copy(sl):
        return pltpu.make_async_copy(right.at[:, span(sl)], rbuf.at[:, span(sl)], r_sem.at[sl])

    def rr_copy(sl, k):
        return pltpu.make_async_copy(rroot.at[:, span(sl)], rr.at[k, pl.ds(0, cols)], rr_sem.at[k])

    def own_copy(q):
        return pltpu.make_async_copy(grad.at[:, pl.ds(q * width, width)], gbuf.at[me * SPLIT + q], own_sem.at[q])

    def piece(sl, sem, dev):
        return pltpu.make_async_remote_copy(
            src_ref=gbuf.at[sl], dst_ref=gbuf.at[sl], send_sem=sem, recv_sem=recv.at[sl],
            device_id={"tensor": dev}, device_id_type=MESH)

    def pair(sl, sem, dev):
        at = gbuf.at[pl.ds(sl, 2)]
        return pltpu.make_async_remote_copy(
            src_ref=at, dst_ref=at, send_sem=sem, recv_sem=recv.at[sl],
            device_id={"tensor": dev}, device_id_type=MESH)

    def part(sl, r, sem, group, dev):
        at = gbuf.at[sl, pl.ds(r * (rows // SUB), rows // SUB)]
        return pltpu.make_async_remote_copy(
            src_ref=at, dst_ref=at, send_sem=sem, recv_sem=recv_sub.at[group, r],
            device_id={"tensor": dev}, device_id_type=MESH)

    def lpart(owner, first, count, s_idx, r_idx, dev):
        at = pl.ds(pl.multiple_of(owner * nl + first, hl), count)
        return pltpu.make_async_remote_copy(
            src_ref=lbuf.at[at], dst_ref=lbuf.at[at], send_sem=l_send.at[s_idx], recv_sem=l_recv.at[r_idx],
            device_id={"tensor": dev}, device_id_type=MESH)

    own = [own_copy(q) for q in range(SPLIT)]
    for c in own:
        c.start()
    lown = pltpu.make_async_copy(lroot, lbuf.at[pl.ds(pl.multiple_of(me * nl, nl), nl)], l_own)
    lown.start()

    def loads(t, k0):
        for u in range(2):
            for i in range(2):
                sl = slot(t, u, i)
                r_copy(sl).start()
                rr_copy(sl, k0 + 2 * u + i).start()

    barrier = pltpu.get_barrier_semaphore()
    for dev in (plus, minus, mate):
        pl.semaphore_signal(barrier, inc=1, device_id={"tensor": dev}, device_id_type=MESH)
    pl.semaphore_wait(barrier, 3)

    base = me * SPLIT
    for q in (0, 1):
        own[q].wait()
    pair(base, send_p.at[0], plus).start()
    for q in (2, 3):
        own[q].wait()
    pair(base + 2, send_m.at[0], minus).start()
    lown.wait()
    lpart(me, 0, nl, 0, 0, plus).start()
    lpart(me, 0, nl, 1, 1, minus).start()
    pair(base + 2, send_p.at[1], plus).start()
    pair(base, send_m.at[1], minus).start()
    pair(base, send_d.at[0], mate).start()
    pair(base + 2, send_d.at[1], mate).start()
    lpart(me, 0, nl, 2, 4, mate).start()
    for t in range(AHEAD):
        loads(t, 4 * t)
    for q in range(SPLIT):
        gt[pl.ds(q * width, width), :] = gbuf[me * SPLIT + q].T
    xacc[...] = jnp.zeros_like(xacc)

    lrow = pl.ds(pl.multiple_of(me * nl, nl), nl)

    def ready(t, u, k0):
        for i in range(2):
            sl = slot(t, u, i)
            r_copy(sl).wait()
            rr_copy(sl, k0 + i).wait()
            rr[k0 + i, pl.ds(cols, nl), :] = gbuf[sl, lrow, :]

    def unit(t, u, k0):
        ready(t, u, k0)
        sls = [slot(t, u, i) for i in range(2)]
        for sl in sls:
            rbuf[:, span(sl)] = EMA_DECAY * rbuf[:, span(sl)] + (1.0 - EMA_DECAY) * jnp.dot(
                gt[...], gbuf[sl], preferred_element_type=jnp.float32)
        xacc[...] += _nt(rr[k0], gbuf[sls[0]]) + _nt(rr[k0 + 1], gbuf[sls[1]])

    def arrived(sl):
        piece(sl, send_d.at[0], mate).wait_recv()

    def pair_arrived(sl):
        pair(sl, send_d.at[0], mate).wait_recv()

    def take(t):
        s = t - 2

        @pl.when(t == 1)
        def _():
            for q in (0, 2):
                pair_arrived(mate * SPLIT + q)

        @pl.when(t >= 2)
        def _():
            a, b = slot(t, 0, 0), slot(t, 0, 1)

            @pl.when((s == 0) | (s == 2))
            def _():
                pair_arrived(a)
                pair(a, send_d.at[2 + s], mate).start()
                pair_arrived(b)
                pair(b, send_d.at[3 + s], mate).start()

            @pl.when(s == 4)
            def _():
                arrived(a)
                piece(a, send_d.at[6], mate).start()
                arrived(b)
                piece(b, send_d.at[7], mate).start()

            @pl.when(s == 1)
            def _():
                lpart(minus, 0, nl, 0, 0, plus).wait_recv()
                lpart(plus, 0, nl, 1, 1, minus).wait_recv()
                lpart(minus, 0, hl, 3, 2, plus).start()
                lpart(plus, hl, hl, 4, 3, minus).start()
                piece(a - 1, send_p.at[2], plus).start()
                piece(b - 1, send_m.at[2], minus).start()
                for r in range(SUB):
                    part(a, r, send_p.at[3 + r], 0, plus).start()
                    part(b, r, send_m.at[3 + r], 1, minus).start()
                lpart(minus, 0, nl, 5, 5, mate).start()
                lpart(plus, 0, nl, 6, 6, mate).start()

    def take_last(t):
        far = ring(me + 4)
        lpart(far, 0, hl, 3, 2, plus).wait_recv()
        lpart(far, hl, hl, 4, 3, minus).wait_recv()
        lpart(far, 0, nl, 7, 7, mate).start()
        for r in range(SUB):
            for i in range(2):
                sl = slot(t, 0, i)
                part(sl, r, send_d.at[0], i, mate).wait_recv()
                part(sl, r, send_d.at[8 + i * SUB + r], 2 + i, mate).start()

    def take_mate(t):
        s = t - 2

        @pl.when((s == 0) | (s == 2))
        def _():
            pair_arrived(slot(t, 1, 0))
            pair_arrived(slot(t, 1, 1))

        @pl.when(s == 4)
        def _():
            arrived(slot(t, 1, 0))
            arrived(slot(t, 1, 1))

    def step(t, carry):
        k0 = 4 * lax.rem(t, AHEAD)
        take(t)
        unit(t, 0, k0)
        take_mate(t)
        unit(t, 1, k0 + 2)

        @pl.when(t + AHEAD < steps + 2)
        def _():
            loads(t + AHEAD, k0)
        return carry

    lax.fori_loop(0, steps + 1, step, 0)
    last = steps + 1
    k0 = 4 * (last % AHEAD)
    take_last(last)
    ready(last, 0, k0)
    for r in range(SUB):
        for i in range(2):
            part(slot(last, 1, i), r, send_d.at[0], 2 + i, mate).wait_recv()
    ready(last, 1, k0 + 2)

    for r_idx in (4, 5, 6, 7):
        lpart(me, 0, nl, 2, r_idx, mate).wait_recv()
    for s in range(2):
        pair(base, send_p.at[s], plus).wait_send()
        pair(base, send_m.at[s], minus).wait_send()
    piece(base, send_p.at[2], plus).wait_send()
    piece(base, send_m.at[2], minus).wait_send()
    for r in range(SUB):
        part(base, r, send_p.at[3 + r], 0, plus).wait_send()
        part(base, r, send_m.at[3 + r], 1, minus).wait_send()
    for s in range(6):
        pair(base, send_d.at[s], mate).wait_send()
    for s in (6, 7):
        piece(base, send_d.at[s], mate).wait_send()
    for s in range(2 * SUB):
        part(base, 0, send_d.at[8 + s], 2, mate).wait_send()
    for k in range(8):
        lpart(me, 0, hl if k in (3, 4) else nl, k, 0, mate).wait_send()


def _write_kernel(n, rbuf, xacc, lbuf, gbuf, gt, rr, left, r_out, l_out, d_out,
                  tail, xs, d_buf, l_buf, r_sem, sem):
    me = lax.axis_index("tensor")
    width = gbuf.shape[2]
    cols, nl = d_buf.shape[1], left.shape[0]
    last = 7
    k0 = 4 * (last % AHEAD)

    def span(sl):
        return pl.ds(pl.multiple_of(sl * width, width), width)

    left_copy = pltpu.make_async_copy(left, l_buf, sem.at[0])
    left_copy.start()
    copies = []

    def write(src, dst):
        copies.append(pltpu.make_async_copy(src, dst, r_sem.at[len(copies)]))
        copies[-1].start()

    chips = n // 2
    far = me // 2 + chips // 2
    tall, wide = cols // 4, 2 * cols
    for c in range(1, chips):
        at = pl.ds(pl.multiple_of(lax.rem(far + c, chips) * wide, wide), wide)
        for p in range(4):
            block = (pl.ds(p * tall, tall), at)
            write(rbuf.at[block], r_out.at[block])
    for u in range(2):
        for i in range(2):
            at = span(_slot(n, me, last - 1, u, i))
            write(rbuf.at[:, at], r_out.at[:, at])
    tails = [_slot(n, me, last, u, i) for u in range(2) for i in range(2)]
    for k, sl in enumerate(tails):
        tail[k] = EMA_DECAY * rbuf[:, span(sl)] + (1.0 - EMA_DECAY) * jnp.dot(
            gt[...], gbuf[sl], preferred_element_type=jnp.float32)
        write(tail.at[k], r_out.at[:, span(sl)])
    xs[...] = xacc[...] + _nt(rr[k0], gbuf[tails[0]]) + _nt(rr[k0 + 1], gbuf[tails[1]])
    xs[...] += _nt(rr[k0 + 2], gbuf[tails[2]]) + _nt(rr[k0 + 3], gbuf[tails[3]])
    d_buf[...] = _nt(lbuf[...], xs[pl.ds(0, cols), :].astype(jnp.bfloat16))
    write(d_buf, d_out)
    left_copy.wait()
    l_buf[...] = EMA_DECAY * l_buf[...] + (1.0 - EMA_DECAY) * xs[pl.ds(cols, nl), :]
    write(l_buf, l_out)
    for c in copies:
        c.wait()


def solution(mesh):
    row_spec = P(("layer", "tensor"), None)
    col_spec = P("layer", "tensor")
    n = mesh.shape["tensor"]

    def local_step(grad, left, right, lroot, rroot):
        rows, cols = grad.shape
        nl = lroot.shape[0]
        width = cols // SPLIT
        f32, bf16 = jnp.float32, jnp.bfloat16
        dma = pltpu.SemaphoreType.DMA
        held = pl.pallas_call(
            functools.partial(_gather_kernel, n),
            out_shape=(pltpu.VMEM(right.shape, f32), pltpu.VMEM((cols + nl, rows), f32), pltpu.VMEM((rows, rows), bf16),
                       pltpu.VMEM((n * SPLIT, rows, width), bf16), pltpu.VMEM((cols, rows), bf16),
                       pltpu.VMEM((4 * AHEAD, cols + nl, width), bf16)),
            in_specs=[ANY] * 4,
            out_specs=(VMEM,) * 6,
            scratch_shapes=[
                dma((SPLIT,)), dma((n * SPLIT,)), dma((4 * AHEAD,)), dma((n * SPLIT,)),
                dma((4, SUB)), dma((3 + SUB,)), dma((3 + SUB,)), dma((8 + 2 * SUB,)),
                dma(()), dma((8,)), dma((8,)),
            ],
            compiler_params=pltpu.CompilerParams(collective_id=0, has_side_effects=True, vmem_limit_bytes=GRANT),
        )(grad, lroot, right, rroot)
        r, l, d = pl.pallas_call(
            functools.partial(_write_kernel, n),
            out_shape=(jax.ShapeDtypeStruct(right.shape, f32), jax.ShapeDtypeStruct((nl, rows), f32),
                       jax.ShapeDtypeStruct((rows, cols), f32)),
            in_specs=[VMEM] * 6 + [ANY],
            out_specs=(ANY,) * 3,
            scratch_shapes=[pltpu.VMEM((4, cols, width), f32), pltpu.VMEM((cols + nl, rows), f32),
                            pltpu.VMEM((rows, cols), f32), pltpu.VMEM((nl, rows), f32), dma((22,)), dma((1,))],
            compiler_params=pltpu.CompilerParams(vmem_limit_bytes=GRANT),
        )(*[pltpu.with_memory_space_constraint(v, pltpu.VMEM) for v in held], left)
        return l, r, d

    return jax.shard_map(local_step, mesh=mesh, in_specs=(col_spec, row_spec, row_spec, row_spec, row_spec), out_specs=(row_spec, row_spec, col_spec), check_vma=False)
```

```python
import functools

import jax
import jax.numpy as jnp
from jax import lax
from jax.experimental import pallas as pl
from jax.experimental.pallas import tpu as pltpu
from jax.sharding import PartitionSpec as P

EMA_DECAY = 0.9
SPLIT = 4
SUB = 2
AHEAD = 3
GRANT = 12 << 20

MESH = pl.DeviceIdType.MESH
ANY = pl.BlockSpec(memory_space=pl.ANY)
VMEM = pl.BlockSpec(memory_space=pltpu.VMEM)


def _nt(a, b):
    return lax.dot_general(a, b, (((1,), (1,)), ((), ())), preferred_element_type=jnp.float32)


def _slot(n, me, t, u, i):
    mate = me + 1 - 2 * (me % 2)
    base = jnp.where(u == 0, me, mate)
    s = t - 2
    far = 2 + 2 * (s // SPLIT)
    owner = jnp.where(i == 0, base - far, base + far)
    part = (s + 2 * i) % SPLIT
    owner = jnp.where(t == 0, me, jnp.where(t == 1, mate, owner))
    part = jnp.where(t < 2, 2 * u + i, part)
    return lax.rem(owner + n, n) * SPLIT + part


def _gather_kernel(n, grad, lroot, right, rroot, rbuf, xacc, lbuf, gbuf, gt, rr,
                   own_sem, r_sem, rr_sem, recv, recv_sub, send_p, send_m, send_d,
                   l_own, l_recv, l_send):
    me = lax.axis_index("tensor")
    mate = me + 1 - 2 * (me % 2)
    rows, width = gbuf.shape[1], gbuf.shape[2]
    cols = gt.shape[0]
    nl = lroot.shape[0]
    hl = nl // 2
    steps = 6
    ring = lambda d: lax.rem(d + n, n)
    plus, minus = ring(me + 2), ring(me - 2)

    slot = functools.partial(_slot, n, me)

    def span(sl):
        return pl.ds(pl.multiple_of(sl * width, width), width)

    def r_copy(sl):
        return pltpu.make_async_copy(right.at[:, span(sl)], rbuf.at[:, span(sl)], r_sem.at[sl])

    def rr_copy(sl, k):
        return pltpu.make_async_copy(rroot.at[:, span(sl)], rr.at[k, pl.ds(0, cols)], rr_sem.at[k])

    def own_copy(q):
        return pltpu.make_async_copy(grad.at[:, pl.ds(q * width, width)], gbuf.at[me * SPLIT + q], own_sem.at[q])

    def piece(sl, sem, dev):
        return pltpu.make_async_remote_copy(
            src_ref=gbuf.at[sl], dst_ref=gbuf.at[sl], send_sem=sem, recv_sem=recv.at[sl],
            device_id={"tensor": dev}, device_id_type=MESH)

    def pair(sl, sem, dev):
        at = gbuf.at[pl.ds(sl, 2)]
        return pltpu.make_async_remote_copy(
            src_ref=at, dst_ref=at, send_sem=sem, recv_sem=recv.at[sl],
            device_id={"tensor": dev}, device_id_type=MESH)

    def part(sl, r, sem, group, dev):
        first = rows * 3 // 4
        at = gbuf.at[sl, pl.ds(0, first) if r == 0 else pl.ds(first, rows - first)]
        return pltpu.make_async_remote_copy(
            src_ref=at, dst_ref=at, send_sem=sem, recv_sem=recv_sub.at[group, r],
            device_id={"tensor": dev}, device_id_type=MESH)

    def lpart(owner, first, count, s_idx, r_idx, dev):
        at = pl.ds(pl.multiple_of(owner * nl + first, hl), count)
        return pltpu.make_async_remote_copy(
            src_ref=lbuf.at[at], dst_ref=lbuf.at[at], send_sem=l_send.at[s_idx], recv_sem=l_recv.at[r_idx],
            device_id={"tensor": dev}, device_id_type=MESH)

    own = [own_copy(q) for q in range(SPLIT)]
    for c in own:
        c.start()
    lown = pltpu.make_async_copy(lroot, lbuf.at[pl.ds(pl.multiple_of(me * nl, nl), nl)], l_own)
    lown.start()

    def loads(t, k0):
        for u in range(2):
            for i in range(2):
                sl = slot(t, u, i)
                r_copy(sl).start()
                rr_copy(sl, k0 + 2 * u + i).start()

    barrier = pltpu.get_barrier_semaphore()
    for dev in (plus, minus, mate):
        pl.semaphore_signal(barrier, inc=1, device_id={"tensor": dev}, device_id_type=MESH)
    pl.semaphore_wait(barrier, 3)

    base = me * SPLIT
    for q in (0, 1):
        own[q].wait()
    pair(base, send_p.at[0], plus).start()
    for q in (2, 3):
        own[q].wait()
    pair(base + 2, send_m.at[0], minus).start()
    lown.wait()
    lpart(me, 0, nl, 0, 0, plus).start()
    lpart(me, 0, nl, 1, 1, minus).start()
    pair(base + 2, send_p.at[1], plus).start()
    pair(base, send_m.at[1], minus).start()
    pair(base, send_d.at[0], mate).start()
    pair(base + 2, send_d.at[1], mate).start()
    lpart(me, 0, nl, 2, 4, mate).start()
    for t in range(AHEAD):
        loads(t, 4 * t)
    for q in range(SPLIT):
        gt[pl.ds(q * width, width), :] = gbuf[me * SPLIT + q].T
    xacc[...] = jnp.zeros_like(xacc)

    lrow = pl.ds(pl.multiple_of(me * nl, nl), nl)

    def ready(t, u, k0):
        for i in range(2):
            sl = slot(t, u, i)
            r_copy(sl).wait()
            rr_copy(sl, k0 + i).wait()
            rr[k0 + i, pl.ds(cols, nl), :] = gbuf[sl, lrow, :]

    def unit(t, u, k0):
        ready(t, u, k0)
        sls = [slot(t, u, i) for i in range(2)]
        for sl in sls:
            rbuf[:, span(sl)] = EMA_DECAY * rbuf[:, span(sl)] + (1.0 - EMA_DECAY) * jnp.dot(
                gt[...], gbuf[sl], preferred_element_type=jnp.float32)
        xacc[...] += _nt(rr[k0], gbuf[sls[0]]) + _nt(rr[k0 + 1], gbuf[sls[1]])

    def arrived(sl):
        piece(sl, send_d.at[0], mate).wait_recv()

    def pair_arrived(sl):
        pair(sl, send_d.at[0], mate).wait_recv()

    def take(t):
        s = t - 2

        @pl.when(t == 1)
        def _():
            for q in (0, 2):
                pair_arrived(mate * SPLIT + q)

        @pl.when(t >= 2)
        def _():
            a, b = slot(t, 0, 0), slot(t, 0, 1)

            @pl.when((s == 0) | (s == 2))
            def _():
                pair_arrived(a)
                pair(a, send_d.at[2 + s], mate).start()
                pair_arrived(b)
                pair(b, send_d.at[3 + s], mate).start()

            @pl.when(s == 4)
            def _():
                arrived(a)
                piece(a, send_d.at[6], mate).start()
                arrived(b)
                piece(b, send_d.at[7], mate).start()

            @pl.when(s == 1)
            def _():
                lpart(minus, 0, nl, 0, 0, plus).wait_recv()
                lpart(plus, 0, nl, 1, 1, minus).wait_recv()
                lpart(minus, 0, hl, 3, 2, plus).start()
                lpart(plus, hl, hl, 4, 3, minus).start()
                piece(a - 1, send_p.at[2], plus).start()
                piece(b - 1, send_m.at[2], minus).start()
                for r in range(SUB):
                    part(a, r, send_p.at[3 + r], 0, plus).start()
                    part(b, r, send_m.at[3 + r], 1, minus).start()
                lpart(minus, 0, nl, 5, 5, mate).start()
                lpart(plus, 0, nl, 6, 6, mate).start()

    def take_last(t):
        far = ring(me + 4)
        lpart(far, 0, hl, 3, 2, plus).wait_recv()
        lpart(far, hl, hl, 4, 3, minus).wait_recv()
        lpart(far, 0, nl, 7, 7, mate).start()
        for r in range(SUB):
            for i in range(2):
                sl = slot(t, 0, i)
                part(sl, r, send_d.at[0], i, mate).wait_recv()
                part(sl, r, send_d.at[8 + i * SUB + r], 2 + i, mate).start()

    def take_mate(t):
        s = t - 2

        @pl.when((s == 0) | (s == 2))
        def _():
            pair_arrived(slot(t, 1, 0))
            pair_arrived(slot(t, 1, 1))

        @pl.when(s == 4)
        def _():
            arrived(slot(t, 1, 0))
            arrived(slot(t, 1, 1))

    def step(t, carry):
        k0 = 4 * lax.rem(t, AHEAD)
        take(t)
        unit(t, 0, k0)
        take_mate(t)
        unit(t, 1, k0 + 2)

        @pl.when(t + AHEAD < steps + 2)
        def _():
            loads(t + AHEAD, k0)
        return carry

    lax.fori_loop(0, steps + 1, step, 0)
    last = steps + 1
    k0 = 4 * (last % AHEAD)
    take_last(last)
    ready(last, 0, k0)
    for r in range(SUB):
        for i in range(2):
            part(slot(last, 1, i), r, send_d.at[0], 2 + i, mate).wait_recv()
    ready(last, 1, k0 + 2)

    for r_idx in (4, 5, 6, 7):
        lpart(me, 0, nl, 2, r_idx, mate).wait_recv()
    for s in range(2):
        pair(base, send_p.at[s], plus).wait_send()
        pair(base, send_m.at[s], minus).wait_send()
    piece(base, send_p.at[2], plus).wait_send()
    piece(base, send_m.at[2], minus).wait_send()
    for r in range(SUB):
        part(base, r, send_p.at[3 + r], 0, plus).wait_send()
        part(base, r, send_m.at[3 + r], 1, minus).wait_send()
    for s in range(6):
        pair(base, send_d.at[s], mate).wait_send()
    for s in (6, 7):
        piece(base, send_d.at[s], mate).wait_send()
    for i in range(2):
        for r in range(SUB):
            part(base, r, send_d.at[8 + i * SUB + r], 2, mate).wait_send()
    for k in range(8):
        lpart(me, 0, hl if k in (3, 4) else nl, k, 0, mate).wait_send()


def _write_kernel(n, rbuf, xacc, lbuf, gbuf, gt, rr, left, r_out, l_out, d_out,
                  tail, xs, d_buf, l_buf, r_sem, sem):
    me = lax.axis_index("tensor")
    width = gbuf.shape[2]
    cols, nl = d_buf.shape[1], left.shape[0]
    last = 7
    k0 = 4 * (last % AHEAD)

    def span(sl):
        return pl.ds(pl.multiple_of(sl * width, width), width)

    left_copy = pltpu.make_async_copy(left, l_buf, sem.at[0])
    left_copy.start()
    copies = []

    def write(src, dst):
        copies.append(pltpu.make_async_copy(src, dst, r_sem.at[len(copies)]))
        copies[-1].start(priority=len(copies) % 2)

    chips = n // 2
    far = me // 2 + chips // 2
    tall, wide = cols // 4, 2 * cols
    for c in range(1, chips):
        at = pl.ds(pl.multiple_of(lax.rem(far + c, chips) * wide, wide), wide)
        for p in range(4):
            block = (pl.ds(p * tall, tall), at)
            write(rbuf.at[block], r_out.at[block])
    for u in range(2):
        for i in range(2):
            at = span(_slot(n, me, last - 1, u, i))
            write(rbuf.at[:, at], r_out.at[:, at])
    tails = [_slot(n, me, last, u, i) for u in range(2) for i in range(2)]
    for k, sl in enumerate(tails):
        tail[k] = EMA_DECAY * rbuf[:, span(sl)] + (1.0 - EMA_DECAY) * jnp.dot(
            gt[...], gbuf[sl], preferred_element_type=jnp.float32)
        write(tail.at[k], r_out.at[:, span(sl)])
    xs[...] = xacc[...] + _nt(rr[k0], gbuf[tails[0]]) + _nt(rr[k0 + 1], gbuf[tails[1]])
    xs[...] += _nt(rr[k0 + 2], gbuf[tails[2]]) + _nt(rr[k0 + 3], gbuf[tails[3]])
    d_buf[...] = _nt(lbuf[...], xs[pl.ds(0, cols), :].astype(jnp.bfloat16))
    write(d_buf, d_out)
    left_copy.wait()
    l_buf[...] = EMA_DECAY * l_buf[...] + (1.0 - EMA_DECAY) * xs[pl.ds(cols, nl), :]
    write(l_buf, l_out)
    for c in copies:
        c.wait()


def solution(mesh):
    row_spec = P(("layer", "tensor"), None)
    col_spec = P("layer", "tensor")
    n = mesh.shape["tensor"]

    def local_step(grad, left, right, lroot, rroot):
        rows, cols = grad.shape
        nl = lroot.shape[0]
        width = cols // SPLIT
        f32, bf16 = jnp.float32, jnp.bfloat16
        dma = pltpu.SemaphoreType.DMA
        held = pl.pallas_call(
            functools.partial(_gather_kernel, n),
            out_shape=(pltpu.VMEM(right.shape, f32), pltpu.VMEM((cols + nl, rows), f32), pltpu.VMEM((rows, rows), bf16),
                       pltpu.VMEM((n * SPLIT, rows, width), bf16), pltpu.VMEM((cols, rows), bf16),
                       pltpu.VMEM((4 * AHEAD, cols + nl, width), bf16)),
            in_specs=[ANY] * 4,
            out_specs=(VMEM,) * 6,
            scratch_shapes=[
                dma((SPLIT,)), dma((n * SPLIT,)), dma((4 * AHEAD,)), dma((n * SPLIT,)),
                dma((4, SUB)), dma((3 + SUB,)), dma((3 + SUB,)), dma((8 + 2 * SUB,)),
                dma(()), dma((8,)), dma((8,)),
            ],
            compiler_params=pltpu.CompilerParams(collective_id=0, has_side_effects=True, vmem_limit_bytes=GRANT),
        )(grad, lroot, right, rroot)
        r, l, d = pl.pallas_call(
            functools.partial(_write_kernel, n),
            out_shape=(jax.ShapeDtypeStruct(right.shape, f32), jax.ShapeDtypeStruct((nl, rows), f32),
                       jax.ShapeDtypeStruct((rows, cols), f32)),
            in_specs=[VMEM] * 6 + [ANY],
            out_specs=(ANY,) * 3,
            scratch_shapes=[pltpu.VMEM((4, cols, width), f32), pltpu.VMEM((cols + nl, rows), f32),
                            pltpu.VMEM((rows, cols), f32), pltpu.VMEM((nl, rows), f32), dma((22,)), dma((1,))],
            compiler_params=pltpu.CompilerParams(vmem_limit_bytes=GRANT),
        )(*[pltpu.with_memory_space_constraint(v, pltpu.VMEM) for v in held], left)
        return l, r, d

    return jax.shard_map(local_step, mesh=mesh, in_specs=(col_spec, row_spec, row_spec, row_spec, row_spec), out_specs=(row_spec, row_spec, col_spec), check_vma=False)
```

```python
import functools

import jax
import jax.numpy as jnp
from jax import lax
from jax.experimental import pallas as pl
from jax.experimental.pallas import tpu as pltpu
from jax.sharding import PartitionSpec as P

EMA_DECAY = 0.9
SPLIT = 4
SUB = 2
AHEAD = 3
GRANT = 12 << 20

MESH = pl.DeviceIdType.MESH
ANY = pl.BlockSpec(memory_space=pl.ANY)
VMEM = pl.BlockSpec(memory_space=pltpu.VMEM)


def _nt(a, b):
    return lax.dot_general(a, b, (((1,), (1,)), ((), ())), preferred_element_type=jnp.float32)


def _slot(n, me, t, u, i):
    mate = me + 1 - 2 * (me % 2)
    base = jnp.where(u == 0, me, mate)
    s = t - 2
    far = 2 + 2 * (s // SPLIT)
    owner = jnp.where(i == 0, base - far, base + far)
    part = (s + 2 * i) % SPLIT
    owner = jnp.where(t == 0, me, jnp.where(t == 1, mate, owner))
    part = jnp.where(t < 2, 2 * u + i, part)
    return lax.rem(owner + n, n) * SPLIT + part


def _gather_kernel(n, grad, lroot, right, rroot, rbuf, xacc, gbuf, gt, rr,
                   own_sem, l_sem, r_sem, rr_sem, recv, recv_sub, send_p, send_m, send_d):
    me = lax.axis_index("tensor")
    mate = me + 1 - 2 * (me % 2)
    width = gbuf.shape[2]
    cols, rows = gt.shape
    nl = lroot.shape[0]
    body, whole = pl.ds(0, rows), pl.ds(0, rows + nl)
    steps = 6
    ring = lambda d: lax.rem(d + n, n)
    plus, minus = ring(me + 2), ring(me - 2)

    slot = functools.partial(_slot, n, me)

    def span(sl):
        return pl.ds(pl.multiple_of(sl * width, width), width)

    def r_copy(sl):
        return pltpu.make_async_copy(right.at[:, span(sl)], rbuf.at[:, span(sl)], r_sem.at[sl])

    def rr_copy(sl, k):
        return pltpu.make_async_copy(rroot.at[:, span(sl)], rr.at[k, pl.ds(0, cols)], rr_sem.at[k])

    def own_copy(q):
        return pltpu.make_async_copy(grad.at[:, pl.ds(q * width, width)], gbuf.at[me * SPLIT + q, body], own_sem.at[q])

    def left_copy(q):
        half = (q + q // 2) % 2
        return pltpu.make_async_copy(
            lroot.at[:, pl.ds(half * width, width)], gbuf.at[me * SPLIT + q, pl.ds(rows, nl)], l_sem.at[q])

    def send(at, sem, recv_sem, dev):
        return pltpu.make_async_remote_copy(
            src_ref=at, dst_ref=at, send_sem=sem, recv_sem=recv_sem,
            device_id={"tensor": dev}, device_id_type=MESH)

    def piece(sl, sem, dev):
        return send(gbuf.at[sl, whole], sem, recv.at[sl], dev)

    def pair(sl, span_rows, sem, dev):
        return send(gbuf.at[pl.ds(sl, 2), span_rows], sem, recv.at[sl], dev)

    def part(sl, r, sem, group, dev):
        first = rows * 3 // 4
        at = gbuf.at[sl, pl.ds(0, first) if r == 0 else pl.ds(first, rows - first)]
        return send(at, sem, recv_sub.at[group, r], dev)

    own = [[own_copy(q), left_copy(q)] for q in range(SPLIT)]
    for q in (0, 1, 2, 3):
        for c in own[q]:
            c.start()

    def loads(t, k0):
        for u in range(2):
            for i in range(2):
                sl = slot(t, u, i)
                r_copy(sl).start()
                rr_copy(sl, k0 + 2 * u + i).start()

    barrier = pltpu.get_barrier_semaphore()
    for dev in (plus, minus, mate):
        pl.semaphore_signal(barrier, inc=1, device_id={"tensor": dev}, device_id_type=MESH)
    pl.semaphore_wait(barrier, 3)

    base = me * SPLIT
    for q in (0, 1):
        for c in own[q]:
            c.wait()
    pair(base, whole, send_p.at[0], plus).start()
    for q in (2, 3):
        for c in own[q]:
            c.wait()
    pair(base + 2, whole, send_m.at[0], minus).start()
    pair(base + 2, body, send_p.at[1], plus).start()
    pair(base, body, send_m.at[1], minus).start()
    pair(base, whole, send_d.at[0], mate).start()
    pair(base + 2, body, send_d.at[1], mate).start()
    for t in range(AHEAD):
        loads(t, 4 * t)
    for q in range(SPLIT):
        gt[pl.ds(q * width, width), :] = gbuf[me * SPLIT + q, body, :].T
    xacc[...] = jnp.zeros_like(xacc)

    lrow = pl.ds(pl.multiple_of(me * nl, nl), nl)

    def ready(t, u, k0):
        for i in range(2):
            sl = slot(t, u, i)
            r_copy(sl).wait()
            rr_copy(sl, k0 + i).wait()
            rr[k0 + i, pl.ds(cols, nl), :] = gbuf[sl, lrow, :]

    def unit(t, u, k0):
        ready(t, u, k0)
        sls = [slot(t, u, i) for i in range(2)]
        for sl in sls:
            rbuf[:, span(sl)] = EMA_DECAY * rbuf[:, span(sl)] + (1.0 - EMA_DECAY) * jnp.dot(
                gt[...], gbuf[sl, body, :], preferred_element_type=jnp.float32)
        xacc[...] += _nt(rr[k0], gbuf[sls[0], body, :]) + _nt(rr[k0 + 1], gbuf[sls[1], body, :])

    def arrived(sl):
        piece(sl, send_d.at[0], mate).wait_recv()

    def pair_arrived(sl, span_rows):
        pair(sl, span_rows, send_d.at[0], mate).wait_recv()

    def take(t):
        s = t - 2

        @pl.when(t == 1)
        def _():
            pair_arrived(mate * SPLIT, whole)
            pair_arrived(mate * SPLIT + 2, body)

        @pl.when(t >= 2)
        def _():
            a, b = slot(t, 0, 0), slot(t, 0, 1)

            for at, span_rows in ((0, whole), (2, body)):
                @pl.when(s == at)
                def _(span_rows=span_rows):
                    pair_arrived(a, span_rows)
                    pair(a, span_rows, send_d.at[2 + s], mate).start()
                    pair_arrived(b, span_rows)
                    pair(b, span_rows, send_d.at[3 + s], mate).start()

            @pl.when(s == 4)
            def _():
                arrived(a)
                piece(a, send_d.at[6], mate).start()
                arrived(b)
                piece(b, send_d.at[7], mate).start()

            @pl.when(s == 1)
            def _():
                piece(a - 1, send_p.at[2], plus).start()
                piece(b - 1, send_m.at[2], minus).start()
                for r in range(SUB):
                    part(a, r, send_p.at[3 + r], 0, plus).start()
                    part(b, r, send_m.at[3 + r], 1, minus).start()

    def take_last(t):
        for r in range(SUB):
            for i in range(2):
                sl = slot(t, 0, i)
                part(sl, r, send_d.at[0], i, mate).wait_recv()
                part(sl, r, send_d.at[8 + i * SUB + r], 2 + i, mate).start()

    def take_mate(t):
        s = t - 2

        for at, span_rows in ((0, whole), (2, body)):
            @pl.when(s == at)
            def _(span_rows=span_rows):
                pair_arrived(slot(t, 1, 0), span_rows)
                pair_arrived(slot(t, 1, 1), span_rows)

        @pl.when(s == 4)
        def _():
            arrived(slot(t, 1, 0))
            arrived(slot(t, 1, 1))

    def step(t, carry):
        k0 = 4 * lax.rem(t, AHEAD)
        take(t)
        unit(t, 0, k0)
        take_mate(t)
        unit(t, 1, k0 + 2)

        @pl.when(t + AHEAD < steps + 2)
        def _():
            loads(t + AHEAD, k0)
        return carry

    lax.fori_loop(0, steps + 1, step, 0)
    last = steps + 1
    k0 = 4 * (last % AHEAD)
    take_last(last)
    ready(last, 0, k0)
    for r in range(SUB):
        for i in range(2):
            part(slot(last, 1, i), r, send_d.at[0], 2 + i, mate).wait_recv()
    ready(last, 1, k0 + 2)

    for s, span_rows in enumerate((whole, body)):
        pair(base, span_rows, send_p.at[s], plus).wait_send()
        pair(base, span_rows, send_m.at[s], minus).wait_send()
    piece(base, send_p.at[2], plus).wait_send()
    piece(base, send_m.at[2], minus).wait_send()
    for r in range(SUB):
        part(base, r, send_p.at[3 + r], 0, plus).wait_send()
        part(base, r, send_m.at[3 + r], 1, minus).wait_send()
    for s, span_rows in enumerate((whole, body, whole, whole, body, body)):
        pair(base, span_rows, send_d.at[s], mate).wait_send()
    for s in (6, 7):
        piece(base, send_d.at[s], mate).wait_send()
    for i in range(2):
        for r in range(SUB):
            part(base, r, send_d.at[8 + i * SUB + r], 2, mate).wait_send()


def _write_kernel(n, rbuf, xacc, gbuf, gt, rr, left, r_out, l_out, d_out,
                  tail, xs, d_buf, l_buf, lbuf, r_sem, sem):
    me = lax.axis_index("tensor")
    width = gbuf.shape[2]
    cols, nl = d_buf.shape[1], left.shape[0]
    rows = d_buf.shape[0]
    body = pl.ds(0, rows)
    last = 7
    k0 = 4 * (last % AHEAD)

    def span(sl):
        return pl.ds(pl.multiple_of(sl * width, width), width)

    left_copy = pltpu.make_async_copy(left, l_buf, sem.at[0])
    left_copy.start()
    copies = []

    def write(src, dst):
        copies.append(pltpu.make_async_copy(src, dst, r_sem.at[len(copies)]))
        copies[-1].start()

    chips = n // 2
    far = me // 2 + chips // 2
    tall, wide = cols // 4, 2 * cols
    for c in range(1, chips):
        at = pl.ds(pl.multiple_of(lax.rem(far + c, chips) * wide, wide), wide)
        for p in range(4):
            block = (pl.ds(p * tall, tall), at)
            write(rbuf.at[block], r_out.at[block])
    for u in range(2):
        for i in range(2):
            at = span(_slot(n, me, last - 1, u, i))
            write(rbuf.at[:, at], r_out.at[:, at])
    tails = [_slot(n, me, last, u, i) for u in range(2) for i in range(2)]
    for k, sl in enumerate(tails):
        tail[k] = EMA_DECAY * rbuf[:, span(sl)] + (1.0 - EMA_DECAY) * jnp.dot(
            gt[...], gbuf[sl, body, :], preferred_element_type=jnp.float32)
        write(tail.at[k], r_out.at[:, span(sl)])
    g = [gbuf[sl, body, :] for sl in tails]
    xs[...] = xacc[...] + _nt(rr[k0], g[0]) + _nt(rr[k0 + 1], g[1])
    xs[...] += _nt(rr[k0 + 2], g[2]) + _nt(rr[k0 + 3], g[3])
    mate = me + 1 - 2 * (me % 2)
    for near in (me, mate):
        for shift, parts in ((0, (0, 1)), (-2, (0, 1)), (2, (3, 2)), (4, (0, 2))):
            owner = lax.rem(near + shift + n, n)
            at = pl.ds(pl.multiple_of(owner * nl, nl), nl)
            for h, q in enumerate(parts):
                lbuf[at, pl.ds(h * width, width)] = gbuf[owner * SPLIT + q, pl.ds(rows, nl), :]
    d_buf[...] = _nt(lbuf[...], xs[pl.ds(0, cols), :].astype(jnp.bfloat16))
    write(d_buf, d_out)
    left_copy.wait()
    l_buf[...] = EMA_DECAY * l_buf[...] + (1.0 - EMA_DECAY) * xs[pl.ds(cols, nl), :]
    write(l_buf, l_out)
    for c in copies:
        c.wait()


def solution(mesh):
    row_spec = P(("layer", "tensor"), None)
    col_spec = P("layer", "tensor")
    n = mesh.shape["tensor"]

    def local_step(grad, left, right, lroot, rroot):
        rows, cols = grad.shape
        nl = lroot.shape[0]
        width = cols // SPLIT
        f32, bf16 = jnp.float32, jnp.bfloat16
        dma = pltpu.SemaphoreType.DMA
        held = pl.pallas_call(
            functools.partial(_gather_kernel, n),
            out_shape=(pltpu.VMEM(right.shape, f32), pltpu.VMEM((cols + nl, rows), f32),
                       pltpu.VMEM((n * SPLIT, rows + nl, width), bf16), pltpu.VMEM((cols, rows), bf16),
                       pltpu.VMEM((4 * AHEAD, cols + nl, width), bf16)),
            in_specs=[ANY] * 4,
            out_specs=(VMEM,) * 5,
            scratch_shapes=[
                dma((SPLIT,)), dma((SPLIT,)), dma((n * SPLIT,)), dma((4 * AHEAD,)), dma((n * SPLIT,)),
                dma((4, SUB)), dma((3 + SUB,)), dma((3 + SUB,)), dma((8 + 2 * SUB,)),
            ],
            compiler_params=pltpu.CompilerParams(collective_id=0, has_side_effects=True, vmem_limit_bytes=GRANT),
        )(grad, lroot, right, rroot)
        r, l, d = pl.pallas_call(
            functools.partial(_write_kernel, n),
            out_shape=(jax.ShapeDtypeStruct(right.shape, f32), jax.ShapeDtypeStruct((nl, rows), f32),
                       jax.ShapeDtypeStruct((rows, cols), f32)),
            in_specs=[VMEM] * 5 + [ANY],
            out_specs=(ANY,) * 3,
            scratch_shapes=[pltpu.VMEM((4, cols, width), f32), pltpu.VMEM((cols + nl, rows), f32),
                            pltpu.VMEM((rows, cols), f32), pltpu.VMEM((nl, rows), f32), pltpu.VMEM((rows, rows), bf16), dma((22,)), dma((1,))],
            compiler_params=pltpu.CompilerParams(vmem_limit_bytes=GRANT),
        )(*[pltpu.with_memory_space_constraint(v, pltpu.VMEM) for v in held], left)
        return l, r, d

    return jax.shard_map(local_step, mesh=mesh, in_specs=(col_spec, row_spec, row_spec, row_spec, row_spec), out_specs=(row_spec, row_spec, col_spec), check_vma=False)
```

```python
import functools

import jax
import jax.numpy as jnp
from jax import lax
from jax.experimental import pallas as pl
from jax.experimental.pallas import tpu as pltpu
from jax.sharding import PartitionSpec as P

EMA_DECAY = 0.9
SPLIT = 4
CUTS = (0, 384, 464, 512)
SUB = len(CUTS) - 1
AHEAD = 3
GRANT = 12 << 20

MESH = pl.DeviceIdType.MESH
ANY = pl.BlockSpec(memory_space=pl.ANY)
VMEM = pl.BlockSpec(memory_space=pltpu.VMEM)


def _nt(a, b):
    return lax.dot_general(a, b, (((1,), (1,)), ((), ())), preferred_element_type=jnp.float32)


def _slot(n, me, t, u, i):
    mate = me + 1 - 2 * (me % 2)
    base = jnp.where(u == 0, me, mate)
    s = t - 2
    far = 2 + 2 * (s // SPLIT)
    owner = jnp.where(i == 0, base - far, base + far)
    part = (s + 2 * i) % SPLIT
    owner = jnp.where(t == 0, me, jnp.where(t == 1, mate, owner))
    part = jnp.where(t < 2, 2 * u + i, part)
    return lax.rem(owner + n, n) * SPLIT + part


def _gather_kernel(n, grad, lroot, right, rroot, rbuf, xacc, gbuf, gt, rr,
                   own_sem, l_sem, r_sem, rr_sem, recv, recv_sub, send_p, send_m, send_d):
    me = lax.axis_index("tensor")
    mate = me + 1 - 2 * (me % 2)
    width = gbuf.shape[2]
    cols, rows = gt.shape
    nl = lroot.shape[0]
    body, whole = pl.ds(0, rows), pl.ds(0, rows + nl)
    steps = 6
    ring = lambda d: lax.rem(d + n, n)
    plus, minus = ring(me + 2), ring(me - 2)
    plus_mate, minus_mate = ring(mate + 2), ring(mate - 2)

    slot = functools.partial(_slot, n, me)

    def span(sl):
        return pl.ds(pl.multiple_of(sl * width, width), width)

    def r_copy(sl):
        return pltpu.make_async_copy(right.at[:, span(sl)], rbuf.at[:, span(sl)], r_sem.at[sl])

    def rr_copy(sl, k):
        return pltpu.make_async_copy(rroot.at[:, span(sl)], rr.at[k, pl.ds(0, cols)], rr_sem.at[k])

    def own_copy(q):
        return pltpu.make_async_copy(grad.at[:, pl.ds(q * width, width)], gbuf.at[me * SPLIT + q, body], own_sem.at[q])

    def left_copy(q):
        half = (q + q // 2) % 2
        return pltpu.make_async_copy(
            lroot.at[:, pl.ds(half * width, width)], gbuf.at[me * SPLIT + q, pl.ds(rows, nl)], l_sem.at[q])

    def send(at, sem, recv_sem, dev):
        return pltpu.make_async_remote_copy(
            src_ref=at, dst_ref=at, send_sem=sem, recv_sem=recv_sem,
            device_id={"tensor": dev}, device_id_type=MESH)

    def piece(sl, sem, dev):
        return send(gbuf.at[sl, whole], sem, recv.at[sl], dev)

    def pair(sl, span_rows, sem, dev):
        return send(gbuf.at[pl.ds(sl, 2), span_rows], sem, recv.at[sl], dev)

    def part(sl, r, sem, group, dev):
        at = gbuf.at[sl, pl.ds(CUTS[r] * rows // CUTS[-1], (CUTS[r + 1] - CUTS[r]) * rows // CUTS[-1])]
        return send(at, sem, recv_sub.at[group, r], dev)

    own = [[own_copy(q), left_copy(q)] for q in range(SPLIT)]
    for q in (0, 1, 2, 3):
        for c in own[q]:
            c.start()

    def loads(t, k0):
        for u in range(2):
            for i in range(2):
                sl = slot(t, u, i)
                r_copy(sl).start()
                rr_copy(sl, k0 + 2 * u + i).start()

    barrier = pltpu.get_barrier_semaphore()
    peers = (plus, minus, mate, plus_mate, minus_mate)
    for dev in peers:
        pl.semaphore_signal(barrier, inc=1, device_id={"tensor": dev}, device_id_type=MESH)
    pl.semaphore_wait(barrier, len(peers))

    base = me * SPLIT
    for q in (0, 1):
        for c in own[q]:
            c.wait()
    pair(base, whole, send_p.at[0], plus).start()
    for q in (2, 3):
        for c in own[q]:
            c.wait()
    pair(base + 2, whole, send_m.at[0], minus).start()
    pair(base + 2, body, send_p.at[1], plus).start()
    pair(base, body, send_m.at[1], minus).start()
    pair(base, whole, send_d.at[0], mate).start()
    pair(base + 2, body, send_d.at[1], mate).start()
    for t in range(AHEAD):
        loads(t, 4 * t)
    for q in range(SPLIT):
        gt[pl.ds(q * width, width), :] = gbuf[me * SPLIT + q, body, :].T
    xacc[...] = jnp.zeros_like(xacc)

    lrow = pl.ds(pl.multiple_of(me * nl, nl), nl)

    def ready(t, u, k0):
        for i in range(2):
            sl = slot(t, u, i)
            r_copy(sl).wait()
            rr_copy(sl, k0 + i).wait()
            rr[k0 + i, pl.ds(cols, nl), :] = gbuf[sl, lrow, :]

    def unit(t, u, k0):
        ready(t, u, k0)
        sls = [slot(t, u, i) for i in range(2)]
        for sl in sls:
            rbuf[:, span(sl)] = EMA_DECAY * rbuf[:, span(sl)] + (1.0 - EMA_DECAY) * jnp.dot(
                gt[...], gbuf[sl, body, :], preferred_element_type=jnp.float32)
        xacc[...] += _nt(rr[k0], gbuf[sls[0], body, :]) + _nt(rr[k0 + 1], gbuf[sls[1], body, :])

    def arrived(sl):
        piece(sl, send_d.at[0], mate).wait_recv()

    def pair_arrived(sl, span_rows):
        pair(sl, span_rows, send_d.at[0], mate).wait_recv()

    def take(t):
        s = t - 2

        @pl.when(t == 1)
        def _():
            pair_arrived(mate * SPLIT, whole)
            pair_arrived(mate * SPLIT + 2, body)

        @pl.when(t >= 2)
        def _():
            a, b = slot(t, 0, 0), slot(t, 0, 1)

            for at, span_rows in ((0, whole), (2, body)):
                @pl.when(s == at)
                def _(span_rows=span_rows):
                    pair_arrived(a, span_rows)
                    pair(a, span_rows, send_d.at[2 + s], mate).start()
                    pair_arrived(b, span_rows)
                    pair(b, span_rows, send_d.at[3 + s], mate).start()

            @pl.when(s == 4)
            def _():
                arrived(a)
                piece(a, send_d.at[6], mate).start()
                arrived(b)
                piece(b, send_d.at[7], mate).start()

            @pl.when(s == 1)
            def _():
                piece(a - 1, send_p.at[2], plus).start()
                piece(b - 1, send_m.at[2], minus).start()
                for r in range(SUB):
                    part(a, r, send_p.at[3 + r], 0, plus).start()
                    part(b, r, send_m.at[3 + r], 1, minus).start()
                part(a, SUB - 1, send_p.at[3 + SUB], 2, plus_mate).start()
                part(b, SUB - 1, send_m.at[3 + SUB], 3, minus_mate).start()

    def take_last(t):
        for r in range(SUB):
            for i in range(2):
                sl = slot(t, 0, i)
                part(sl, r, send_d.at[0], i, mate).wait_recv()
                if r < SUB - 1:
                    part(sl, r, send_d.at[8 + i * SUB + r], 2 + i, mate).start()

    def take_mate(t):
        s = t - 2

        for at, span_rows in ((0, whole), (2, body)):
            @pl.when(s == at)
            def _(span_rows=span_rows):
                pair_arrived(slot(t, 1, 0), span_rows)
                pair_arrived(slot(t, 1, 1), span_rows)

        @pl.when(s == 4)
        def _():
            arrived(slot(t, 1, 0))
            arrived(slot(t, 1, 1))

    def step(t, carry):
        k0 = 4 * lax.rem(t, AHEAD)
        take(t)
        unit(t, 0, k0)
        take_mate(t)
        unit(t, 1, k0 + 2)

        @pl.when(t + AHEAD < steps + 2)
        def _():
            loads(t + AHEAD, k0)
        return carry

    lax.fori_loop(0, steps + 1, step, 0)
    last = steps + 1
    k0 = 4 * (last % AHEAD)
    take_last(last)
    ready(last, 0, k0)
    for r in range(SUB):
        for i in range(2):
            part(slot(last, 1, i), r, send_d.at[0], 2 + i, mate).wait_recv()
    ready(last, 1, k0 + 2)

    for s, span_rows in enumerate((whole, body)):
        pair(base, span_rows, send_p.at[s], plus).wait_send()
        pair(base, span_rows, send_m.at[s], minus).wait_send()
    piece(base, send_p.at[2], plus).wait_send()
    piece(base, send_m.at[2], minus).wait_send()
    for r in range(SUB):
        part(base, r, send_p.at[3 + r], 0, plus).wait_send()
        part(base, r, send_m.at[3 + r], 1, minus).wait_send()
    part(base, SUB - 1, send_p.at[3 + SUB], 2, plus_mate).wait_send()
    part(base, SUB - 1, send_m.at[3 + SUB], 3, minus_mate).wait_send()
    for s, span_rows in enumerate((whole, body, whole, whole, body, body)):
        pair(base, span_rows, send_d.at[s], mate).wait_send()
    for s in (6, 7):
        piece(base, send_d.at[s], mate).wait_send()
    for i in range(2):
        for r in range(SUB - 1):
            part(base, r, send_d.at[8 + i * SUB + r], 2, mate).wait_send()


def _write_kernel(n, rbuf, xacc, gbuf, gt, rr, left, r_out, l_out, d_out,
                  tail, xs, d_buf, l_buf, lbuf, r_sem, sem):
    me = lax.axis_index("tensor")
    width = gbuf.shape[2]
    cols, nl = d_buf.shape[1], left.shape[0]
    rows = d_buf.shape[0]
    body = pl.ds(0, rows)
    last = 7
    k0 = 4 * (last % AHEAD)

    def span(sl):
        return pl.ds(pl.multiple_of(sl * width, width), width)

    left_copy = pltpu.make_async_copy(left, l_buf, sem.at[0])
    left_copy.start()
    copies = []

    def write(src, dst):
        copies.append(pltpu.make_async_copy(src, dst, r_sem.at[len(copies)]))
        copies[-1].start()

    chips = n // 2
    far = me // 2 + chips // 2
    tall, wide = cols // 4, 2 * cols
    for c in range(1, chips):
        at = pl.ds(pl.multiple_of(lax.rem(far + c, chips) * wide, wide), wide)
        for p in range(4):
            block = (pl.ds(p * tall, tall), at)
            write(rbuf.at[block], r_out.at[block])
    for u in range(2):
        for i in range(2):
            at = span(_slot(n, me, last - 1, u, i))
            write(rbuf.at[:, at], r_out.at[:, at])
    tails = [_slot(n, me, last, u, i) for u in range(2) for i in range(2)]
    for k, sl in enumerate(tails):
        tail[k] = EMA_DECAY * rbuf[:, span(sl)] + (1.0 - EMA_DECAY) * jnp.dot(
            gt[...], gbuf[sl, body, :], preferred_element_type=jnp.float32)
        write(tail.at[k], r_out.at[:, span(sl)])
    g = [gbuf[sl, body, :] for sl in tails]
    xs[...] = xacc[...] + _nt(rr[k0], g[0]) + _nt(rr[k0 + 1], g[1])
    xs[...] += _nt(rr[k0 + 2], g[2]) + _nt(rr[k0 + 3], g[3])
    mate = me + 1 - 2 * (me % 2)
    for near in (me, mate):
        for shift, parts in ((0, (0, 1)), (-2, (0, 1)), (2, (3, 2)), (4, (0, 2))):
            owner = lax.rem(near + shift + n, n)
            at = pl.ds(pl.multiple_of(owner * nl, nl), nl)
            for h, q in enumerate(parts):
                lbuf[at, pl.ds(h * width, width)] = gbuf[owner * SPLIT + q, pl.ds(rows, nl), :]
    d_buf[...] = _nt(lbuf[...], xs[pl.ds(0, cols), :].astype(jnp.bfloat16))
    write(d_buf, d_out)
    left_copy.wait()
    l_buf[...] = EMA_DECAY * l_buf[...] + (1.0 - EMA_DECAY) * xs[pl.ds(cols, nl), :]
    write(l_buf, l_out)
    for c in copies:
        c.wait()


def solution(mesh):
    row_spec = P(("layer", "tensor"), None)
    col_spec = P("layer", "tensor")
    n = mesh.shape["tensor"]

    def local_step(grad, left, right, lroot, rroot):
        rows, cols = grad.shape
        nl = lroot.shape[0]
        width = cols // SPLIT
        f32, bf16 = jnp.float32, jnp.bfloat16
        dma = pltpu.SemaphoreType.DMA
        held = pl.pallas_call(
            functools.partial(_gather_kernel, n),
            out_shape=(pltpu.VMEM(right.shape, f32), pltpu.VMEM((cols + nl, rows), f32),
                       pltpu.VMEM((n * SPLIT, rows + nl, width), bf16), pltpu.VMEM((cols, rows), bf16),
                       pltpu.VMEM((4 * AHEAD, cols + nl, width), bf16)),
            in_specs=[ANY] * 4,
            out_specs=(VMEM,) * 5,
            scratch_shapes=[
                dma((SPLIT,)), dma((SPLIT,)), dma((n * SPLIT,)), dma((4 * AHEAD,)), dma((n * SPLIT,)),
                dma((4, SUB)), dma((4 + SUB,)), dma((4 + SUB,)), dma((8 + 2 * SUB,)),
            ],
            compiler_params=pltpu.CompilerParams(collective_id=0, has_side_effects=True, vmem_limit_bytes=GRANT),
        )(grad, lroot, right, rroot)
        r, l, d = pl.pallas_call(
            functools.partial(_write_kernel, n),
            out_shape=(jax.ShapeDtypeStruct(right.shape, f32), jax.ShapeDtypeStruct((nl, rows), f32),
                       jax.ShapeDtypeStruct((rows, cols), f32)),
            in_specs=[VMEM] * 5 + [ANY],
            out_specs=(ANY,) * 3,
            scratch_shapes=[pltpu.VMEM((4, cols, width), f32), pltpu.VMEM((cols + nl, rows), f32),
                            pltpu.VMEM((rows, cols), f32), pltpu.VMEM((nl, rows), f32), pltpu.VMEM((rows, rows), bf16), dma((22,)), dma((1,))],
            compiler_params=pltpu.CompilerParams(vmem_limit_bytes=GRANT),
        )(*[pltpu.with_memory_space_constraint(v, pltpu.VMEM) for v in held], left)
        return l, r, d

    return jax.shard_map(local_step, mesh=mesh, in_specs=(col_spec, row_spec, row_spec, row_spec, row_spec), out_specs=(row_spec, row_spec, col_spec), check_vma=False)
```

```python
import functools

import jax
import jax.numpy as jnp
from jax import lax
from jax.experimental import pallas as pl
from jax.experimental.pallas import tpu as pltpu
from jax.sharding import PartitionSpec as P

EMA_DECAY = 0.9
SPLIT = 4
SUB = 2
AHEAD = 3
GRANT = 12 << 20

MESH = pl.DeviceIdType.MESH
ANY = pl.BlockSpec(memory_space=pl.ANY)
VMEM = pl.BlockSpec(memory_space=pltpu.VMEM)


def _nt(a, b):
    return lax.dot_general(a, b, (((1,), (1,)), ((), ())), preferred_element_type=jnp.float32)


def _slot(n, me, t, u, i):
    mate = me + 1 - 2 * (me % 2)
    base = jnp.where(u == 0, me, mate)
    s = t - 2
    far = 2 + 2 * (s // SPLIT)
    owner = jnp.where(i == 0, base - far, base + far)
    part = (s + 2 * i) % SPLIT
    owner = jnp.where(t == 0, me, jnp.where(t == 1, mate, owner))
    part = jnp.where(t < 2, 2 * u + i, part)
    return lax.rem(owner + n, n) * SPLIT + part


def _gather_kernel(n, grad, lroot, right, rroot, rbuf, xacc, gbuf, gt, rr,
                   own_sem, l_sem, r_sem, rr_sem, recv, recv_sub, send_p, send_m, send_d):
    me = lax.axis_index("tensor")
    mate = me + 1 - 2 * (me % 2)
    width = gbuf.shape[2]
    cols, rows = gt.shape
    nl = lroot.shape[0]
    body, whole = pl.ds(0, rows), pl.ds(0, rows + nl)
    steps = 6
    ring = lambda d: lax.rem(d + n, n)
    plus, minus = ring(me + 2), ring(me - 2)
    plus_mate, minus_mate = ring(mate + 2), ring(mate - 2)
    odd = me % 2 == 1

    slot = functools.partial(_slot, n, me)

    def span(sl):
        return pl.ds(pl.multiple_of(sl * width, width), width)

    def r_copy(sl):
        return pltpu.make_async_copy(right.at[:, span(sl)], rbuf.at[:, span(sl)], r_sem.at[sl])

    def rr_copy(sl, k):
        return pltpu.make_async_copy(rroot.at[:, span(sl)], rr.at[k, pl.ds(0, cols)], rr_sem.at[k])

    def own_copy(q):
        return pltpu.make_async_copy(grad.at[:, pl.ds(q * width, width)], gbuf.at[me * SPLIT + q, body], own_sem.at[q])

    def left_copy(q):
        half = (q + q // 2) % 2
        return pltpu.make_async_copy(
            lroot.at[:, pl.ds(half * width, width)], gbuf.at[me * SPLIT + q, pl.ds(rows, nl)], l_sem.at[q])

    def send(at, sem, recv_sem, dev):
        return pltpu.make_async_remote_copy(
            src_ref=at, dst_ref=at, send_sem=sem, recv_sem=recv_sem,
            device_id={"tensor": dev}, device_id_type=MESH)

    def piece(sl, sem, dev):
        return send(gbuf.at[sl, whole], sem, recv.at[sl], dev)

    def pair(sl, span_rows, sem, dev):
        return send(gbuf.at[pl.ds(sl, 2), span_rows], sem, recv.at[sl], dev)

    def part(sl, r, sem, group, dev):
        first = rows * 3 // 4
        at = gbuf.at[sl, pl.ds(0, first) if r == 0 else pl.ds(first, rows - first)]
        return send(at, sem, recv_sub.at[group, r], dev)

    own = [[own_copy(q), left_copy(q)] for q in range(SPLIT)]
    for q in (0, 1, 2, 3):
        for c in own[q]:
            c.start()

    def loads(t, k0):
        for u in range(2):
            for i in range(2):
                sl = slot(t, u, i)
                r_copy(sl).start()
                rr_copy(sl, k0 + 2 * u + i).start()

    barrier = pltpu.get_barrier_semaphore()
    peers = (plus, minus, mate, plus_mate, minus_mate)
    for dev in peers:
        pl.semaphore_signal(barrier, inc=1, device_id={"tensor": dev}, device_id_type=MESH)
    pl.semaphore_wait(barrier, len(peers))

    base = me * SPLIT
    for q in (0, 1):
        for c in own[q]:
            c.wait()
    pair(base, whole, send_p.at[0], plus).start()
    for q in (2, 3):
        for c in own[q]:
            c.wait()
    pair(base + 2, whole, send_m.at[0], minus).start()
    pair(base + 2, body, send_p.at[1], plus).start()
    pair(base, body, send_m.at[1], minus).start()
    pair(base, whole, send_d.at[0], mate).start()
    pair(base + 2, body, send_d.at[1], mate).start()
    for t in range(AHEAD):
        loads(t, 4 * t)
    for q in range(SPLIT):
        gt[pl.ds(q * width, width), :] = gbuf[me * SPLIT + q, body, :].T
    xacc[...] = jnp.zeros_like(xacc)

    lrow = pl.ds(pl.multiple_of(me * nl, nl), nl)

    def ready(t, u, k0):
        for i in range(2):
            sl = slot(t, u, i)
            r_copy(sl).wait()
            rr_copy(sl, k0 + i).wait()
            rr[k0 + i, pl.ds(cols, nl), :] = gbuf[sl, lrow, :]

    def unit(t, u, k0):
        ready(t, u, k0)
        sls = [slot(t, u, i) for i in range(2)]
        for sl in sls:
            rbuf[:, span(sl)] = EMA_DECAY * rbuf[:, span(sl)] + (1.0 - EMA_DECAY) * jnp.dot(
                gt[...], gbuf[sl, body, :], preferred_element_type=jnp.float32)
        xacc[...] += _nt(rr[k0], gbuf[sls[0], body, :]) + _nt(rr[k0 + 1], gbuf[sls[1], body, :])

    def arrived(sl):
        piece(sl, send_d.at[0], mate).wait_recv()

    def pair_arrived(sl, span_rows):
        pair(sl, span_rows, send_d.at[0], mate).wait_recv()

    def take(t):
        s = t - 2

        @pl.when(t == 1)
        def _():
            pair_arrived(mate * SPLIT, whole)
            pair_arrived(mate * SPLIT + 2, body)

        @pl.when(t >= 2)
        def _():
            a, b = slot(t, 0, 0), slot(t, 0, 1)

            for at, span_rows in ((0, whole), (2, body)):
                @pl.when(s == at)
                def _(span_rows=span_rows):
                    pair_arrived(a, span_rows)
                    pair(a, span_rows, send_d.at[2 + s], mate).start()
                    pair_arrived(b, span_rows)
                    pair(b, span_rows, send_d.at[3 + s], mate).start()

            @pl.when(s == 4)
            def _():
                arrived(a)
                piece(a, send_d.at[6], mate).start()
                arrived(b)
                piece(b, send_d.at[7], mate).start()

            @pl.when(s == 1)
            def _():
                @pl.when(odd)
                def _():
                    part(slot(t, 1, 0), SUB - 1, send_p.at[3 + SUB], 0, plus_mate).start()
                    part(slot(t, 1, 1), SUB - 1, send_m.at[3 + SUB], 1, minus_mate).start()
                piece(a - 1, send_p.at[2], plus).start()
                piece(b - 1, send_m.at[2], minus).start()
                for r in range(SUB - 1):
                    part(a, r, send_p.at[3 + r], 0, plus).start()
                    part(b, r, send_m.at[3 + r], 1, minus).start()

                @pl.when(odd)
                def _():
                    part(a, SUB - 1, send_p.at[2 + SUB], 0, plus).start()
                    part(b, SUB - 1, send_m.at[2 + SUB], 1, minus).start()

    def take_last(t):
        for r in range(SUB):
            for i in range(2):
                sl = slot(t, 0, i)
                part(sl, r, send_d.at[0], i, mate).wait_recv()
                part(sl, r, send_d.at[8 + i * SUB + r], 2 + i, mate).start()

    def take_mate(t):
        s = t - 2

        for at, span_rows in ((0, whole), (2, body)):
            @pl.when(s == at)
            def _(span_rows=span_rows):
                pair_arrived(slot(t, 1, 0), span_rows)
                pair_arrived(slot(t, 1, 1), span_rows)

        @pl.when(s == 4)
        def _():
            arrived(slot(t, 1, 0))
            arrived(slot(t, 1, 1))

    def step(t, carry):
        k0 = 4 * lax.rem(t, AHEAD)
        take(t)
        unit(t, 0, k0)
        take_mate(t)
        unit(t, 1, k0 + 2)

        @pl.when(t + AHEAD < steps + 2)
        def _():
            loads(t + AHEAD, k0)
        return carry

    lax.fori_loop(0, steps + 1, step, 0)
    last = steps + 1
    k0 = 4 * (last % AHEAD)
    take_last(last)
    ready(last, 0, k0)
    for r in range(SUB):
        for i in range(2):
            part(slot(last, 1, i), r, send_d.at[0], 2 + i, mate).wait_recv()
    ready(last, 1, k0 + 2)

    for s, span_rows in enumerate((whole, body)):
        pair(base, span_rows, send_p.at[s], plus).wait_send()
        pair(base, span_rows, send_m.at[s], minus).wait_send()
    piece(base, send_p.at[2], plus).wait_send()
    piece(base, send_m.at[2], minus).wait_send()
    for r in range(SUB - 1):
        part(base, r, send_p.at[3 + r], 0, plus).wait_send()
        part(base, r, send_m.at[3 + r], 1, minus).wait_send()

    @pl.when(odd)
    def _():
        for k in (2 + SUB, 3 + SUB):
            part(base, SUB - 1, send_p.at[k], 0, plus).wait_send()
            part(base, SUB - 1, send_m.at[k], 1, minus).wait_send()
    for s, span_rows in enumerate((whole, body, whole, whole, body, body)):
        pair(base, span_rows, send_d.at[s], mate).wait_send()
    for s in (6, 7):
        piece(base, send_d.at[s], mate).wait_send()
    for i in range(2):
        for r in range(SUB):
            part(base, r, send_d.at[8 + i * SUB + r], 2, mate).wait_send()


def _write_kernel(n, rbuf, xacc, gbuf, gt, rr, left, r_out, l_out, d_out,
                  tail, xs, d_buf, l_buf, lbuf, r_sem, sem):
    me = lax.axis_index("tensor")
    width = gbuf.shape[2]
    cols, nl = d_buf.shape[1], left.shape[0]
    rows = d_buf.shape[0]
    body = pl.ds(0, rows)
    last = 7
    k0 = 4 * (last % AHEAD)

    def span(sl):
        return pl.ds(pl.multiple_of(sl * width, width), width)

    left_copy = pltpu.make_async_copy(left, l_buf, sem.at[0])
    left_copy.start()
    copies = []

    def write(src, dst):
        copies.append(pltpu.make_async_copy(src, dst, r_sem.at[len(copies)]))
        copies[-1].start()

    chips = n // 2
    far = me // 2 + chips // 2
    tall, wide = cols // 4, 2 * cols
    for c in range(1, chips):
        at = pl.ds(pl.multiple_of(lax.rem(far + c, chips) * wide, wide), wide)
        for p in range(4):
            block = (pl.ds(p * tall, tall), at)
            write(rbuf.at[block], r_out.at[block])
    for u in range(2):
        for i in range(2):
            at = span(_slot(n, me, last - 1, u, i))
            write(rbuf.at[:, at], r_out.at[:, at])
    tails = [_slot(n, me, last, u, i) for u in range(2) for i in range(2)]
    for k, sl in enumerate(tails):
        tail[k] = EMA_DECAY * rbuf[:, span(sl)] + (1.0 - EMA_DECAY) * jnp.dot(
            gt[...], gbuf[sl, body, :], preferred_element_type=jnp.float32)
        write(tail.at[k], r_out.at[:, span(sl)])
    g = [gbuf[sl, body, :] for sl in tails]
    xs[...] = xacc[...] + _nt(rr[k0], g[0]) + _nt(rr[k0 + 1], g[1])
    xs[...] += _nt(rr[k0 + 2], g[2]) + _nt(rr[k0 + 3], g[3])
    mate = me + 1 - 2 * (me % 2)
    for near in (me, mate):
        for shift, parts in ((0, (0, 1)), (-2, (0, 1)), (2, (3, 2)), (4, (0, 2))):
            owner = lax.rem(near + shift + n, n)
            at = pl.ds(pl.multiple_of(owner * nl, nl), nl)
            for h, q in enumerate(parts):
                lbuf[at, pl.ds(h * width, width)] = gbuf[owner * SPLIT + q, pl.ds(rows, nl), :]
    d_buf[...] = _nt(lbuf[...], xs[pl.ds(0, cols), :].astype(jnp.bfloat16))
    write(d_buf, d_out)
    left_copy.wait()
    l_buf[...] = EMA_DECAY * l_buf[...] + (1.0 - EMA_DECAY) * xs[pl.ds(cols, nl), :]
    write(l_buf, l_out)
    for c in copies:
        c.wait()


def solution(mesh):
    row_spec = P(("layer", "tensor"), None)
    col_spec = P("layer", "tensor")
    n = mesh.shape["tensor"]

    def local_step(grad, left, right, lroot, rroot):
        rows, cols = grad.shape
        nl = lroot.shape[0]
        width = cols // SPLIT
        f32, bf16 = jnp.float32, jnp.bfloat16
        dma = pltpu.SemaphoreType.DMA
        held = pl.pallas_call(
            functools.partial(_gather_kernel, n),
            out_shape=(pltpu.VMEM(right.shape, f32), pltpu.VMEM((cols + nl, rows), f32),
                       pltpu.VMEM((n * SPLIT, rows + nl, width), bf16), pltpu.VMEM((cols, rows), bf16),
                       pltpu.VMEM((4 * AHEAD, cols + nl, width), bf16)),
            in_specs=[ANY] * 4,
            out_specs=(VMEM,) * 5,
            scratch_shapes=[
                dma((SPLIT,)), dma((SPLIT,)), dma((n * SPLIT,)), dma((4 * AHEAD,)), dma((n * SPLIT,)),
                dma((4, SUB)), dma((4 + SUB,)), dma((4 + SUB,)), dma((8 + 2 * SUB,)),
            ],
            compiler_params=pltpu.CompilerParams(collective_id=0, has_side_effects=True, vmem_limit_bytes=GRANT),
        )(grad, lroot, right, rroot)
        r, l, d = pl.pallas_call(
            functools.partial(_write_kernel, n),
            out_shape=(jax.ShapeDtypeStruct(right.shape, f32), jax.ShapeDtypeStruct((nl, rows), f32),
                       jax.ShapeDtypeStruct((rows, cols), f32)),
            in_specs=[VMEM] * 5 + [ANY],
            out_specs=(ANY,) * 3,
            scratch_shapes=[pltpu.VMEM((4, cols, width), f32), pltpu.VMEM((cols + nl, rows), f32),
                            pltpu.VMEM((rows, cols), f32), pltpu.VMEM((nl, rows), f32), pltpu.VMEM((rows, rows), bf16), dma((22,)), dma((1,))],
            compiler_params=pltpu.CompilerParams(vmem_limit_bytes=GRANT),
        )(*[pltpu.with_memory_space_constraint(v, pltpu.VMEM) for v in held], left)
        return l, r, d

    return jax.shard_map(local_step, mesh=mesh, in_specs=(col_spec, row_spec, row_spec, row_spec, row_spec), out_specs=(row_spec, row_spec, col_spec), check_vma=False)
```

```python
import functools

import jax
import jax.numpy as jnp
from jax import lax
from jax.experimental import pallas as pl
from jax.experimental.pallas import tpu as pltpu
from jax.sharding import PartitionSpec as P

EMA_DECAY = 0.9
SPLIT = 4
SUB = 2
AHEAD = 3
GRANT = 12 << 20

MESH = pl.DeviceIdType.MESH
ANY = pl.BlockSpec(memory_space=pl.ANY)
VMEM = pl.BlockSpec(memory_space=pltpu.VMEM)


def _nt(a, b):
    return lax.dot_general(a, b, (((1,), (1,)), ((), ())), preferred_element_type=jnp.float32)


def _slot(n, me, t, u, i):
    mate = me + 1 - 2 * (me % 2)
    base = jnp.where(u == 0, me, mate)
    s = t - 2
    far = 2 + 2 * (s // SPLIT)
    owner = jnp.where(i == 0, base - far, base + far)
    part = (s + 2 * i) % SPLIT
    owner = jnp.where(t == 0, me, jnp.where(t == 1, mate, owner))
    part = jnp.where(t < 2, 2 * u + i, part)
    return lax.rem(owner + n, n) * SPLIT + part


def _gather_kernel(n, grad, lroot, right, rroot, rbuf, xacc, gbuf, gt, rr,
                   own_sem, l_sem, r_sem, rr_sem, recv, recv_sub, send_p, send_m, send_d):
    me = lax.axis_index("tensor")
    mate = me + 1 - 2 * (me % 2)
    width = gbuf.shape[2]
    cols, rows = gt.shape
    nl = lroot.shape[0]
    body, whole = pl.ds(0, rows), pl.ds(0, rows + nl)
    steps = 6
    ring = lambda d: lax.rem(d + n, n)
    plus, minus = ring(me + 2), ring(me - 2)
    plus_mate, minus_mate = ring(mate + 2), ring(mate - 2)
    odd = me % 2 == 1

    slot = functools.partial(_slot, n, me)

    def span(sl):
        return pl.ds(pl.multiple_of(sl * width, width), width)

    def r_copy(sl):
        return pltpu.make_async_copy(right.at[:, span(sl)], rbuf.at[:, span(sl)], r_sem.at[sl])

    def rr_copy(sl, k):
        return pltpu.make_async_copy(rroot.at[:, span(sl)], rr.at[k, pl.ds(0, cols)], rr_sem.at[k])

    def own_copy(q):
        return pltpu.make_async_copy(grad.at[:, pl.ds(q * width, width)], gbuf.at[me * SPLIT + q, body], own_sem.at[q])

    def left_copy(q):
        half = (q + q // 2) % 2
        return pltpu.make_async_copy(
            lroot.at[:, pl.ds(half * width, width)], gbuf.at[me * SPLIT + q, pl.ds(rows, nl)], l_sem.at[q])

    def send(at, sem, recv_sem, dev):
        return pltpu.make_async_remote_copy(
            src_ref=at, dst_ref=at, send_sem=sem, recv_sem=recv_sem,
            device_id={"tensor": dev}, device_id_type=MESH)

    def piece(sl, sem, dev):
        return send(gbuf.at[sl, whole], sem, recv.at[sl], dev)

    def pair(sl, span_rows, sem, dev):
        return send(gbuf.at[pl.ds(sl, 2), span_rows], sem, recv.at[sl], dev)

    def part(sl, r, sem, group, dev):
        first = rows * 7 // 8
        at = gbuf.at[sl, pl.ds(0, first) if r == 0 else pl.ds(first, rows - first)]
        return send(at, sem, recv_sub.at[group, r], dev)

    own = [[own_copy(q), left_copy(q)] for q in range(SPLIT)]
    for q in (0, 1, 2, 3):
        for c in own[q]:
            c.start()

    def loads(t, k0):
        for u in range(2):
            for i in range(2):
                sl = slot(t, u, i)
                r_copy(sl).start()
                rr_copy(sl, k0 + 2 * u + i).start()

    barrier = pltpu.get_barrier_semaphore()
    peers = (plus, minus, mate, plus_mate, minus_mate)
    for dev in peers:
        pl.semaphore_signal(barrier, inc=1, device_id={"tensor": dev}, device_id_type=MESH)
    pl.semaphore_wait(barrier, len(peers))

    base = me * SPLIT
    for q in (0, 1):
        for c in own[q]:
            c.wait()
    pair(base, whole, send_p.at[0], plus).start()
    for q in (2, 3):
        for c in own[q]:
            c.wait()
    pair(base + 2, whole, send_m.at[0], minus).start()
    pair(base + 2, body, send_p.at[1], plus).start()
    pair(base, body, send_m.at[1], minus).start()
    pair(base, whole, send_d.at[0], mate).start()
    pair(base + 2, body, send_d.at[1], mate).start()
    for t in range(AHEAD):
        loads(t, 4 * t)
    for q in range(SPLIT):
        gt[pl.ds(q * width, width), :] = gbuf[me * SPLIT + q, body, :].T
    xacc[...] = jnp.zeros_like(xacc)

    lrow = pl.ds(pl.multiple_of(me * nl, nl), nl)

    def ready(t, u, k0):
        for i in range(2):
            sl = slot(t, u, i)
            r_copy(sl).wait()
            rr_copy(sl, k0 + i).wait()
            rr[k0 + i, pl.ds(cols, nl), :] = gbuf[sl, lrow, :]

    def unit(t, u, k0):
        ready(t, u, k0)
        sls = [slot(t, u, i) for i in range(2)]
        for sl in sls:
            rbuf[:, span(sl)] = EMA_DECAY * rbuf[:, span(sl)] + (1.0 - EMA_DECAY) * jnp.dot(
                gt[...], gbuf[sl, body, :], preferred_element_type=jnp.float32)
        xacc[...] += _nt(rr[k0], gbuf[sls[0], body, :]) + _nt(rr[k0 + 1], gbuf[sls[1], body, :])

    def arrived(sl):
        piece(sl, send_d.at[0], mate).wait_recv()

    def pair_arrived(sl, span_rows):
        pair(sl, span_rows, send_d.at[0], mate).wait_recv()

    def take(t):
        s = t - 2

        @pl.when(t == 1)
        def _():
            pair_arrived(mate * SPLIT, whole)
            pair_arrived(mate * SPLIT + 2, body)

        @pl.when(t >= 2)
        def _():
            a, b = slot(t, 0, 0), slot(t, 0, 1)

            for at, span_rows in ((0, whole), (2, body)):
                @pl.when(s == at)
                def _(span_rows=span_rows):
                    pair_arrived(a, span_rows)
                    pair(a, span_rows, send_d.at[2 + s], mate).start()
                    pair_arrived(b, span_rows)
                    pair(b, span_rows, send_d.at[3 + s], mate).start()

            @pl.when(s == 4)
            def _():
                arrived(a)
                piece(a, send_d.at[6], mate).start()
                arrived(b)
                piece(b, send_d.at[7], mate).start()

            @pl.when(s == 1)
            def _():
                @pl.when(odd)
                def _():
                    part(slot(t, 1, 0), SUB - 1, send_p.at[3 + SUB], 0, plus_mate).start()
                    part(slot(t, 1, 1), SUB - 1, send_m.at[3 + SUB], 1, minus_mate).start()
                piece(a - 1, send_p.at[2], plus).start()
                piece(b - 1, send_m.at[2], minus).start()
                for r in range(SUB - 1):
                    part(a, r, send_p.at[3 + r], 0, plus).start()
                    part(b, r, send_m.at[3 + r], 1, minus).start()

                @pl.when(odd)
                def _():
                    part(a, SUB - 1, send_p.at[2 + SUB], 0, plus).start()
                    part(b, SUB - 1, send_m.at[2 + SUB], 1, minus).start()

    def take_last(t):
        for r in range(SUB):
            for i in range(2):
                sl = slot(t, 0, i)
                part(sl, r, send_d.at[0], i, mate).wait_recv()
                part(sl, r, send_d.at[8 + i * SUB + r], 2 + i, mate).start()

    def take_mate(t):
        s = t - 2

        for at, span_rows in ((0, whole), (2, body)):
            @pl.when(s == at)
            def _(span_rows=span_rows):
                pair_arrived(slot(t, 1, 0), span_rows)
                pair_arrived(slot(t, 1, 1), span_rows)

        @pl.when(s == 4)
        def _():
            arrived(slot(t, 1, 0))
            arrived(slot(t, 1, 1))

    def step(t, carry):
        k0 = 4 * lax.rem(t, AHEAD)
        take(t)
        unit(t, 0, k0)
        take_mate(t)
        unit(t, 1, k0 + 2)

        @pl.when(t + AHEAD < steps + 2)
        def _():
            loads(t + AHEAD, k0)
        return carry

    lax.fori_loop(0, steps + 1, step, 0)
    last = steps + 1
    k0 = 4 * (last % AHEAD)
    take_last(last)
    ready(last, 0, k0)
    for r in range(SUB):
        for i in range(2):
            part(slot(last, 1, i), r, send_d.at[0], 2 + i, mate).wait_recv()
    ready(last, 1, k0 + 2)

    for s, span_rows in enumerate((whole, body)):
        pair(base, span_rows, send_p.at[s], plus).wait_send()
        pair(base, span_rows, send_m.at[s], minus).wait_send()
    piece(base, send_p.at[2], plus).wait_send()
    piece(base, send_m.at[2], minus).wait_send()
    for r in range(SUB - 1):
        part(base, r, send_p.at[3 + r], 0, plus).wait_send()
        part(base, r, send_m.at[3 + r], 1, minus).wait_send()

    @pl.when(odd)
    def _():
        for k in (2 + SUB, 3 + SUB):
            part(base, SUB - 1, send_p.at[k], 0, plus).wait_send()
            part(base, SUB - 1, send_m.at[k], 1, minus).wait_send()
    for s, span_rows in enumerate((whole, body, whole, whole, body, body)):
        pair(base, span_rows, send_d.at[s], mate).wait_send()
    for s in (6, 7):
        piece(base, send_d.at[s], mate).wait_send()
    for i in range(2):
        for r in range(SUB):
            part(base, r, send_d.at[8 + i * SUB + r], 2, mate).wait_send()


def _write_kernel(n, rbuf, xacc, gbuf, gt, rr, left, r_out, l_out, d_out,
                  tail, xs, d_buf, l_buf, lbuf, r_sem, sem):
    me = lax.axis_index("tensor")
    width = gbuf.shape[2]
    cols, nl = d_buf.shape[1], left.shape[0]
    rows = d_buf.shape[0]
    body = pl.ds(0, rows)
    last = 7
    k0 = 4 * (last % AHEAD)

    def span(sl):
        return pl.ds(pl.multiple_of(sl * width, width), width)

    left_copy = pltpu.make_async_copy(left, l_buf, sem.at[0])
    left_copy.start()
    copies = []

    def write(src, dst):
        copies.append(pltpu.make_async_copy(src, dst, r_sem.at[len(copies)]))
        copies[-1].start()

    chips = n // 2
    far = me // 2 + chips // 2
    tall, wide = cols // 4, 2 * cols
    for c in range(1, chips):
        at = pl.ds(pl.multiple_of(lax.rem(far + c, chips) * wide, wide), wide)
        for p in range(4):
            block = (pl.ds(p * tall, tall), at)
            write(rbuf.at[block], r_out.at[block])
    for u in range(2):
        for i in range(2):
            at = span(_slot(n, me, last - 1, u, i))
            write(rbuf.at[:, at], r_out.at[:, at])
    tails = [_slot(n, me, last, u, i) for u in range(2) for i in range(2)]
    for k, sl in enumerate(tails):
        tail[k] = EMA_DECAY * rbuf[:, span(sl)] + (1.0 - EMA_DECAY) * jnp.dot(
            gt[...], gbuf[sl, body, :], preferred_element_type=jnp.float32)
        write(tail.at[k], r_out.at[:, span(sl)])
    g = [gbuf[sl, body, :] for sl in tails]
    xs[...] = xacc[...] + _nt(rr[k0], g[0]) + _nt(rr[k0 + 1], g[1])
    xs[...] += _nt(rr[k0 + 2], g[2]) + _nt(rr[k0 + 3], g[3])
    mate = me + 1 - 2 * (me % 2)
    for near in (me, mate):
        for shift, parts in ((0, (0, 1)), (-2, (0, 1)), (2, (3, 2)), (4, (0, 2))):
            owner = lax.rem(near + shift + n, n)
            at = pl.ds(pl.multiple_of(owner * nl, nl), nl)
            for h, q in enumerate(parts):
                lbuf[at, pl.ds(h * width, width)] = gbuf[owner * SPLIT + q, pl.ds(rows, nl), :]
    d_buf[...] = _nt(lbuf[...], xs[pl.ds(0, cols), :].astype(jnp.bfloat16))
    write(d_buf, d_out)
    left_copy.wait()
    l_buf[...] = EMA_DECAY * l_buf[...] + (1.0 - EMA_DECAY) * xs[pl.ds(cols, nl), :]
    write(l_buf, l_out)
    for c in copies:
        c.wait()


def solution(mesh):
    row_spec = P(("layer", "tensor"), None)
    col_spec = P("layer", "tensor")
    n = mesh.shape["tensor"]

    def local_step(grad, left, right, lroot, rroot):
        rows, cols = grad.shape
        nl = lroot.shape[0]
        width = cols // SPLIT
        f32, bf16 = jnp.float32, jnp.bfloat16
        dma = pltpu.SemaphoreType.DMA
        held = pl.pallas_call(
            functools.partial(_gather_kernel, n),
            out_shape=(pltpu.VMEM(right.shape, f32), pltpu.VMEM((cols + nl, rows), f32),
                       pltpu.VMEM((n * SPLIT, rows + nl, width), bf16), pltpu.VMEM((cols, rows), bf16),
                       pltpu.VMEM((4 * AHEAD, cols + nl, width), bf16)),
            in_specs=[ANY] * 4,
            out_specs=(VMEM,) * 5,
            scratch_shapes=[
                dma((SPLIT,)), dma((SPLIT,)), dma((n * SPLIT,)), dma((4 * AHEAD,)), dma((n * SPLIT,)),
                dma((4, SUB)), dma((4 + SUB,)), dma((4 + SUB,)), dma((8 + 2 * SUB,)),
            ],
            compiler_params=pltpu.CompilerParams(collective_id=0, has_side_effects=True, vmem_limit_bytes=GRANT),
        )(grad, lroot, right, rroot)
        r, l, d = pl.pallas_call(
            functools.partial(_write_kernel, n),
            out_shape=(jax.ShapeDtypeStruct(right.shape, f32), jax.ShapeDtypeStruct((nl, rows), f32),
                       jax.ShapeDtypeStruct((rows, cols), f32)),
            in_specs=[VMEM] * 5 + [ANY],
            out_specs=(ANY,) * 3,
            scratch_shapes=[pltpu.VMEM((4, cols, width), f32), pltpu.VMEM((cols + nl, rows), f32),
                            pltpu.VMEM((rows, cols), f32), pltpu.VMEM((nl, rows), f32), pltpu.VMEM((rows, rows), bf16), dma((22,)), dma((1,))],
            compiler_params=pltpu.CompilerParams(vmem_limit_bytes=GRANT),
        )(*[pltpu.with_memory_space_constraint(v, pltpu.VMEM) for v in held], left)
        return l, r, d

    return jax.shard_map(local_step, mesh=mesh, in_specs=(col_spec, row_spec, row_spec, row_spec, row_spec), out_specs=(row_spec, row_spec, col_spec), check_vma=False)
```

```python
import functools

import jax
import jax.numpy as jnp
from jax import lax
from jax.experimental import pallas as pl
from jax.experimental.pallas import tpu as pltpu
from jax.sharding import PartitionSpec as P

EMA_DECAY = 0.9
SPLIT = 4
CUTS = (0, 256, 416, 512)
SUB = len(CUTS) - 1
AHEAD = 3
GRANT = 12 << 20

MESH = pl.DeviceIdType.MESH
ANY = pl.BlockSpec(memory_space=pl.ANY)
VMEM = pl.BlockSpec(memory_space=pltpu.VMEM)


def _nt(a, b):
    return lax.dot_general(a, b, (((1,), (1,)), ((), ())), preferred_element_type=jnp.float32)


def _slot(n, me, t, u, i):
    mate = me + 1 - 2 * (me % 2)
    base = jnp.where(u == 0, me, mate)
    s = t - 2
    far = 2 + 2 * (s // SPLIT)
    owner = jnp.where(i == 0, base - far, base + far)
    part = (s + 2 * i) % SPLIT
    owner = jnp.where(t == 0, me, jnp.where(t == 1, mate, owner))
    part = jnp.where(t < 2, 2 * u + i, part)
    return lax.rem(owner + n, n) * SPLIT + part


def _gather_kernel(n, grad, lroot, right, rroot, rbuf, xacc, gbuf, gt, rr,
                   own_sem, l_sem, r_sem, rr_sem, recv, recv_sub, send_p, send_m, send_d):
    me = lax.axis_index("tensor")
    mate = me + 1 - 2 * (me % 2)
    width = gbuf.shape[2]
    cols, rows = gt.shape
    nl = lroot.shape[0]
    body, whole = pl.ds(0, rows), pl.ds(0, rows + nl)
    steps = 6
    ring = lambda d: lax.rem(d + n, n)
    plus, minus = ring(me + 2), ring(me - 2)
    plus_mate, minus_mate = ring(mate + 2), ring(mate - 2)
    odd = me % 2 == 1

    slot = functools.partial(_slot, n, me)

    def span(sl):
        return pl.ds(pl.multiple_of(sl * width, width), width)

    def r_copy(sl):
        return pltpu.make_async_copy(right.at[:, span(sl)], rbuf.at[:, span(sl)], r_sem.at[sl])

    def rr_copy(sl, k):
        return pltpu.make_async_copy(rroot.at[:, span(sl)], rr.at[k, pl.ds(0, cols)], rr_sem.at[k])

    def own_copy(q):
        return pltpu.make_async_copy(grad.at[:, pl.ds(q * width, width)], gbuf.at[me * SPLIT + q, body], own_sem.at[q])

    def left_copy(q):
        half = (q + q // 2) % 2
        return pltpu.make_async_copy(
            lroot.at[:, pl.ds(half * width, width)], gbuf.at[me * SPLIT + q, pl.ds(rows, nl)], l_sem.at[q])

    def send(at, sem, recv_sem, dev):
        return pltpu.make_async_remote_copy(
            src_ref=at, dst_ref=at, send_sem=sem, recv_sem=recv_sem,
            device_id={"tensor": dev}, device_id_type=MESH)

    def piece(sl, sem, dev):
        return send(gbuf.at[sl, whole], sem, recv.at[sl], dev)

    def pair(sl, span_rows, sem, dev):
        return send(gbuf.at[pl.ds(sl, 2), span_rows], sem, recv.at[sl], dev)

    def part(sl, r, sem, group, dev):
        first, end = (CUTS[r + k] * rows // CUTS[-1] for k in range(2))
        at = gbuf.at[sl, pl.ds(first, end - first)]
        return send(at, sem, recv_sub.at[group, r], dev)

    own = [[own_copy(q), left_copy(q)] for q in range(SPLIT)]
    for q in (0, 1, 2, 3):
        for c in own[q]:
            c.start()

    def loads(t, k0):
        for u in range(2):
            for i in range(2):
                sl = slot(t, u, i)
                r_copy(sl).start()
                rr_copy(sl, k0 + 2 * u + i).start()

    barrier = pltpu.get_barrier_semaphore()
    peers = (plus, minus, mate, plus_mate, minus_mate)
    for dev in peers:
        pl.semaphore_signal(barrier, inc=1, device_id={"tensor": dev}, device_id_type=MESH)
    pl.semaphore_wait(barrier, len(peers))

    base = me * SPLIT
    for q in (0, 1):
        for c in own[q]:
            c.wait()
    pair(base, whole, send_p.at[0], plus).start()
    for q in (2, 3):
        for c in own[q]:
            c.wait()
    pair(base + 2, whole, send_m.at[0], minus).start()
    pair(base + 2, body, send_p.at[1], plus).start()
    pair(base, body, send_m.at[1], minus).start()
    pair(base, whole, send_d.at[0], mate).start()
    pair(base + 2, body, send_d.at[1], mate).start()
    for t in range(AHEAD):
        loads(t, 4 * t)
    for q in range(SPLIT):
        gt[pl.ds(q * width, width), :] = gbuf[me * SPLIT + q, body, :].T
    xacc[...] = jnp.zeros_like(xacc)

    lrow = pl.ds(pl.multiple_of(me * nl, nl), nl)

    def ready(t, u, k0):
        for i in range(2):
            sl = slot(t, u, i)
            r_copy(sl).wait()
            rr_copy(sl, k0 + i).wait()
            rr[k0 + i, pl.ds(cols, nl), :] = gbuf[sl, lrow, :]

    def unit(t, u, k0):
        ready(t, u, k0)
        sls = [slot(t, u, i) for i in range(2)]
        for sl in sls:
            rbuf[:, span(sl)] = EMA_DECAY * rbuf[:, span(sl)] + (1.0 - EMA_DECAY) * jnp.dot(
                gt[...], gbuf[sl, body, :], preferred_element_type=jnp.float32)
        xacc[...] += _nt(rr[k0], gbuf[sls[0], body, :]) + _nt(rr[k0 + 1], gbuf[sls[1], body, :])

    def arrived(sl):
        piece(sl, send_d.at[0], mate).wait_recv()

    def pair_arrived(sl, span_rows):
        pair(sl, span_rows, send_d.at[0], mate).wait_recv()

    def take(t):
        s = t - 2

        @pl.when(t == 1)
        def _():
            pair_arrived(mate * SPLIT, whole)
            pair_arrived(mate * SPLIT + 2, body)

        @pl.when(t >= 2)
        def _():
            a, b = slot(t, 0, 0), slot(t, 0, 1)

            for at, span_rows in ((0, whole), (2, body)):
                @pl.when(s == at)
                def _(span_rows=span_rows):
                    pair_arrived(a, span_rows)
                    pair(a, span_rows, send_d.at[2 + s], mate).start()
                    pair_arrived(b, span_rows)
                    pair(b, span_rows, send_d.at[3 + s], mate).start()

            @pl.when(s == 4)
            def _():
                arrived(a)
                piece(a, send_d.at[6], mate).start()
                arrived(b)
                piece(b, send_d.at[7], mate).start()

            @pl.when(s == 1)
            def _():
                @pl.when(odd)
                def _():
                    part(slot(t, 1, 0), SUB - 1, send_p.at[3 + SUB], 0, plus_mate).start()
                    part(slot(t, 1, 1), SUB - 1, send_m.at[3 + SUB], 1, minus_mate).start()
                piece(a - 1, send_p.at[2], plus).start()
                piece(b - 1, send_m.at[2], minus).start()
                for r in range(SUB - 1):
                    part(a, r, send_p.at[3 + r], 0, plus).start()
                    part(b, r, send_m.at[3 + r], 1, minus).start()

                @pl.when(odd)
                def _():
                    part(a, SUB - 1, send_p.at[2 + SUB], 0, plus).start()
                    part(b, SUB - 1, send_m.at[2 + SUB], 1, minus).start()

    def take_last(t):
        for r in range(SUB):
            for i in range(2):
                sl = slot(t, 0, i)
                part(sl, r, send_d.at[0], i, mate).wait_recv()
                part(sl, r, send_d.at[8 + i * SUB + r], 2 + i, mate).start()

    def take_mate(t):
        s = t - 2

        for at, span_rows in ((0, whole), (2, body)):
            @pl.when(s == at)
            def _(span_rows=span_rows):
                pair_arrived(slot(t, 1, 0), span_rows)
                pair_arrived(slot(t, 1, 1), span_rows)

        @pl.when(s == 4)
        def _():
            arrived(slot(t, 1, 0))
            arrived(slot(t, 1, 1))

    def step(t, carry):
        k0 = 4 * lax.rem(t, AHEAD)
        take(t)
        unit(t, 0, k0)
        take_mate(t)
        unit(t, 1, k0 + 2)

        @pl.when(t + AHEAD < steps + 2)
        def _():
            loads(t + AHEAD, k0)
        return carry

    lax.fori_loop(0, steps + 1, step, 0)
    last = steps + 1
    k0 = 4 * (last % AHEAD)
    take_last(last)
    ready(last, 0, k0)
    for r in range(SUB):
        for i in range(2):
            part(slot(last, 1, i), r, send_d.at[0], 2 + i, mate).wait_recv()
    ready(last, 1, k0 + 2)

    for s, span_rows in enumerate((whole, body)):
        pair(base, span_rows, send_p.at[s], plus).wait_send()
        pair(base, span_rows, send_m.at[s], minus).wait_send()
    piece(base, send_p.at[2], plus).wait_send()
    piece(base, send_m.at[2], minus).wait_send()
    for r in range(SUB - 1):
        part(base, r, send_p.at[3 + r], 0, plus).wait_send()
        part(base, r, send_m.at[3 + r], 1, minus).wait_send()

    @pl.when(odd)
    def _():
        for k in (2 + SUB, 3 + SUB):
            part(base, SUB - 1, send_p.at[k], 0, plus).wait_send()
            part(base, SUB - 1, send_m.at[k], 1, minus).wait_send()
    for s, span_rows in enumerate((whole, body, whole, whole, body, body)):
        pair(base, span_rows, send_d.at[s], mate).wait_send()
    for s in (6, 7):
        piece(base, send_d.at[s], mate).wait_send()
    for i in range(2):
        for r in range(SUB):
            part(base, r, send_d.at[8 + i * SUB + r], 2, mate).wait_send()


def _write_kernel(n, rbuf, xacc, gbuf, gt, rr, left, r_out, l_out, d_out,
                  tail, xs, d_buf, l_buf, lbuf, r_sem, sem):
    me = lax.axis_index("tensor")
    width = gbuf.shape[2]
    cols, nl = d_buf.shape[1], left.shape[0]
    rows = d_buf.shape[0]
    body = pl.ds(0, rows)
    last = 7
    k0 = 4 * (last % AHEAD)

    def span(sl):
        return pl.ds(pl.multiple_of(sl * width, width), width)

    left_copy = pltpu.make_async_copy(left, l_buf, sem.at[0])
    left_copy.start()
    copies = []

    def write(src, dst):
        copies.append(pltpu.make_async_copy(src, dst, r_sem.at[len(copies)]))
        copies[-1].start()

    chips = n // 2
    far = me // 2 + chips // 2
    tall, wide = cols // 4, 2 * cols
    for c in range(1, chips):
        at = pl.ds(pl.multiple_of(lax.rem(far + c, chips) * wide, wide), wide)
        for p in range(4):
            block = (pl.ds(p * tall, tall), at)
            write(rbuf.at[block], r_out.at[block])
    for u in range(2):
        for i in range(2):
            at = span(_slot(n, me, last - 1, u, i))
            write(rbuf.at[:, at], r_out.at[:, at])
    tails = [_slot(n, me, last, u, i) for u in range(2) for i in range(2)]
    for k, sl in enumerate(tails):
        tail[k] = EMA_DECAY * rbuf[:, span(sl)] + (1.0 - EMA_DECAY) * jnp.dot(
            gt[...], gbuf[sl, body, :], preferred_element_type=jnp.float32)
        write(tail.at[k], r_out.at[:, span(sl)])
    g = [gbuf[sl, body, :] for sl in tails]
    xs[...] = xacc[...] + _nt(rr[k0], g[0]) + _nt(rr[k0 + 1], g[1])
    xs[...] += _nt(rr[k0 + 2], g[2]) + _nt(rr[k0 + 3], g[3])
    mate = me + 1 - 2 * (me % 2)
    for near in (me, mate):
        for shift, parts in ((0, (0, 1)), (-2, (0, 1)), (2, (3, 2)), (4, (0, 2))):
            owner = lax.rem(near + shift + n, n)
            at = pl.ds(pl.multiple_of(owner * nl, nl), nl)
            for h, q in enumerate(parts):
                lbuf[at, pl.ds(h * width, width)] = gbuf[owner * SPLIT + q, pl.ds(rows, nl), :]
    d_buf[...] = _nt(lbuf[...], xs[pl.ds(0, cols), :].astype(jnp.bfloat16))
    write(d_buf, d_out)
    left_copy.wait()
    l_buf[...] = EMA_DECAY * l_buf[...] + (1.0 - EMA_DECAY) * xs[pl.ds(cols, nl), :]
    write(l_buf, l_out)
    for c in copies:
        c.wait()


def solution(mesh):
    row_spec = P(("layer", "tensor"), None)
    col_spec = P("layer", "tensor")
    n = mesh.shape["tensor"]

    def local_step(grad, left, right, lroot, rroot):
        rows, cols = grad.shape
        nl = lroot.shape[0]
        width = cols // SPLIT
        f32, bf16 = jnp.float32, jnp.bfloat16
        dma = pltpu.SemaphoreType.DMA
        held = pl.pallas_call(
            functools.partial(_gather_kernel, n),
            out_shape=(pltpu.VMEM(right.shape, f32), pltpu.VMEM((cols + nl, rows), f32),
                       pltpu.VMEM((n * SPLIT, rows + nl, width), bf16), pltpu.VMEM((cols, rows), bf16),
                       pltpu.VMEM((4 * AHEAD, cols + nl, width), bf16)),
            in_specs=[ANY] * 4,
            out_specs=(VMEM,) * 5,
            scratch_shapes=[
                dma((SPLIT,)), dma((SPLIT,)), dma((n * SPLIT,)), dma((4 * AHEAD,)), dma((n * SPLIT,)),
                dma((4, SUB)), dma((4 + SUB,)), dma((4 + SUB,)), dma((8 + 2 * SUB,)),
            ],
            compiler_params=pltpu.CompilerParams(collective_id=0, has_side_effects=True, vmem_limit_bytes=GRANT),
        )(grad, lroot, right, rroot)
        r, l, d = pl.pallas_call(
            functools.partial(_write_kernel, n),
            out_shape=(jax.ShapeDtypeStruct(right.shape, f32), jax.ShapeDtypeStruct((nl, rows), f32),
                       jax.ShapeDtypeStruct((rows, cols), f32)),
            in_specs=[VMEM] * 5 + [ANY],
            out_specs=(ANY,) * 3,
            scratch_shapes=[pltpu.VMEM((4, cols, width), f32), pltpu.VMEM((cols + nl, rows), f32),
                            pltpu.VMEM((rows, cols), f32), pltpu.VMEM((nl, rows), f32), pltpu.VMEM((rows, rows), bf16), dma((22,)), dma((1,))],
            compiler_params=pltpu.CompilerParams(vmem_limit_bytes=GRANT),
        )(*[pltpu.with_memory_space_constraint(v, pltpu.VMEM) for v in held], left)
        return l, r, d

    return jax.shard_map(local_step, mesh=mesh, in_specs=(col_spec, row_spec, row_spec, row_spec, row_spec), out_specs=(row_spec, row_spec, col_spec), check_vma=False)
```

```python
import functools

import jax
import jax.numpy as jnp
from jax import lax
from jax.experimental import pallas as pl
from jax.experimental.pallas import tpu as pltpu
from jax.sharding import PartitionSpec as P

EMA_DECAY = 0.9
SPLIT = 4
CUTS = (0, 352, 464, 512)
SUB = len(CUTS) - 1
AHEAD = 3
GRANT = 12 << 20

MESH = pl.DeviceIdType.MESH
ANY = pl.BlockSpec(memory_space=pl.ANY)
VMEM = pl.BlockSpec(memory_space=pltpu.VMEM)


def _nt(a, b):
    return lax.dot_general(a, b, (((1,), (1,)), ((), ())), preferred_element_type=jnp.float32)


def _slot(n, me, t, u, i):
    mate = me + 1 - 2 * (me % 2)
    base = jnp.where(u == 0, me, mate)
    s = t - 2
    far = 2 + 2 * (s // SPLIT)
    owner = jnp.where(i == 0, base - far, base + far)
    part = (s + 2 * i) % SPLIT
    owner = jnp.where(t == 0, me, jnp.where(t == 1, mate, owner))
    part = jnp.where(t < 2, 2 * u + i, part)
    return lax.rem(owner + n, n) * SPLIT + part


def _gather_kernel(n, grad, lroot, right, rroot, rbuf, xacc, gbuf, gt, rr,
                   own_sem, l_sem, r_sem, rr_sem, recv, recv_sub, send_p, send_m, send_d):
    me = lax.axis_index("tensor")
    mate = me + 1 - 2 * (me % 2)
    width = gbuf.shape[2]
    cols, rows = gt.shape
    nl = lroot.shape[0]
    body, whole = pl.ds(0, rows), pl.ds(0, rows + nl)
    steps = 6
    ring = lambda d: lax.rem(d + n, n)
    plus, minus = ring(me + 2), ring(me - 2)
    plus_mate, minus_mate = ring(mate + 2), ring(mate - 2)
    odd = me % 2 == 1

    slot = functools.partial(_slot, n, me)

    def span(sl):
        return pl.ds(pl.multiple_of(sl * width, width), width)

    def r_copy(sl):
        return pltpu.make_async_copy(right.at[:, span(sl)], rbuf.at[:, span(sl)], r_sem.at[sl])

    def rr_copy(sl, k):
        return pltpu.make_async_copy(rroot.at[:, span(sl)], rr.at[k, pl.ds(0, cols)], rr_sem.at[k])

    def own_copy(q):
        return pltpu.make_async_copy(grad.at[:, pl.ds(q * width, width)], gbuf.at[me * SPLIT + q, body], own_sem.at[q])

    def left_copy(q):
        half = (q + q // 2) % 2
        return pltpu.make_async_copy(
            lroot.at[:, pl.ds(half * width, width)], gbuf.at[me * SPLIT + q, pl.ds(rows, nl)], l_sem.at[q])

    def send(at, sem, recv_sem, dev):
        return pltpu.make_async_remote_copy(
            src_ref=at, dst_ref=at, send_sem=sem, recv_sem=recv_sem,
            device_id={"tensor": dev}, device_id_type=MESH)

    def piece(sl, sem, dev):
        return send(gbuf.at[sl, whole], sem, recv.at[sl], dev)

    def pair(sl, span_rows, sem, dev):
        return send(gbuf.at[pl.ds(sl, 2), span_rows], sem, recv.at[sl], dev)

    def part(sl, r, sem, group, dev):
        first, end = (CUTS[r + k] * rows // CUTS[-1] for k in range(2))
        at = gbuf.at[sl, pl.ds(first, end - first)]
        return send(at, sem, recv_sub.at[group, r], dev)

    own = [[own_copy(q), left_copy(q)] for q in range(SPLIT)]
    for q in (0, 1, 2, 3):
        for c in own[q]:
            c.start()

    def loads(t, k0):
        for u in range(2):
            for i in range(2):
                sl = slot(t, u, i)
                r_copy(sl).start()
                rr_copy(sl, k0 + 2 * u + i).start()

    barrier = pltpu.get_barrier_semaphore()
    peers = (plus, minus, mate, plus_mate, minus_mate)
    for dev in peers:
        pl.semaphore_signal(barrier, inc=1, device_id={"tensor": dev}, device_id_type=MESH)
    pl.semaphore_wait(barrier, len(peers))

    base = me * SPLIT
    for q in (0, 1):
        for c in own[q]:
            c.wait()
    pair(base, whole, send_p.at[0], plus).start()
    for q in (2, 3):
        for c in own[q]:
            c.wait()
    pair(base + 2, whole, send_m.at[0], minus).start()
    pair(base + 2, body, send_p.at[1], plus).start()
    pair(base, body, send_m.at[1], minus).start()
    pair(base, whole, send_d.at[0], mate).start()
    pair(base + 2, body, send_d.at[1], mate).start()
    for t in range(AHEAD):
        loads(t, 4 * t)
    for q in range(SPLIT):
        gt[pl.ds(q * width, width), :] = gbuf[me * SPLIT + q, body, :].T
    xacc[...] = jnp.zeros_like(xacc)

    lrow = pl.ds(pl.multiple_of(me * nl, nl), nl)

    def ready(t, u, k0):
        for i in range(2):
            sl = slot(t, u, i)
            r_copy(sl).wait()
            rr_copy(sl, k0 + i).wait()
            rr[k0 + i, pl.ds(cols, nl), :] = gbuf[sl, lrow, :]

    def unit(t, u, k0):
        ready(t, u, k0)
        sls = [slot(t, u, i) for i in range(2)]
        for sl in sls:
            rbuf[:, span(sl)] = EMA_DECAY * rbuf[:, span(sl)] + (1.0 - EMA_DECAY) * jnp.dot(
                gt[...], gbuf[sl, body, :], preferred_element_type=jnp.float32)
        xacc[...] += _nt(rr[k0], gbuf[sls[0], body, :]) + _nt(rr[k0 + 1], gbuf[sls[1], body, :])

    def arrived(sl):
        piece(sl, send_d.at[0], mate).wait_recv()

    def pair_arrived(sl, span_rows):
        pair(sl, span_rows, send_d.at[0], mate).wait_recv()

    def take(t):
        s = t - 2

        @pl.when(t == 1)
        def _():
            pair_arrived(mate * SPLIT, whole)
            pair_arrived(mate * SPLIT + 2, body)

        @pl.when(t >= 2)
        def _():
            a, b = slot(t, 0, 0), slot(t, 0, 1)

            for at, span_rows in ((0, whole), (2, body)):
                @pl.when(s == at)
                def _(span_rows=span_rows):
                    pair_arrived(a, span_rows)
                    pair(a, span_rows, send_d.at[2 + s], mate).start()
                    pair_arrived(b, span_rows)
                    pair(b, span_rows, send_d.at[3 + s], mate).start()

            @pl.when(s == 4)
            def _():
                arrived(a)
                piece(a, send_d.at[6], mate).start()
                arrived(b)
                piece(b, send_d.at[7], mate).start()

            @pl.when(s == 1)
            def _():
                @pl.when(odd)
                def _():
                    part(slot(t, 1, 0), SUB - 1, send_p.at[3 + SUB], 0, plus_mate).start()
                    part(slot(t, 1, 1), SUB - 1, send_m.at[3 + SUB], 1, minus_mate).start()
                piece(a - 1, send_p.at[2], plus).start()
                piece(b - 1, send_m.at[2], minus).start()
                for r in range(SUB - 1):
                    part(a, r, send_p.at[3 + r], 0, plus).start()
                    part(b, r, send_m.at[3 + r], 1, minus).start()

                @pl.when(odd)
                def _():
                    part(a, SUB - 1, send_p.at[2 + SUB], 0, plus).start()
                    part(b, SUB - 1, send_m.at[2 + SUB], 1, minus).start()

    def take_last(t):
        for r in range(SUB):
            for i in range(2):
                sl = slot(t, 0, i)
                part(sl, r, send_d.at[0], i, mate).wait_recv()
                part(sl, r, send_d.at[8 + i * SUB + r], 2 + i, mate).start()

    def take_mate(t):
        s = t - 2

        for at, span_rows in ((0, whole), (2, body)):
            @pl.when(s == at)
            def _(span_rows=span_rows):
                pair_arrived(slot(t, 1, 0), span_rows)
                pair_arrived(slot(t, 1, 1), span_rows)

        @pl.when(s == 4)
        def _():
            arrived(slot(t, 1, 0))
            arrived(slot(t, 1, 1))

    def step(t, carry):
        k0 = 4 * lax.rem(t, AHEAD)
        take(t)
        unit(t, 0, k0)
        take_mate(t)
        unit(t, 1, k0 + 2)

        @pl.when(t + AHEAD < steps + 2)
        def _():
            loads(t + AHEAD, k0)
        return carry

    lax.fori_loop(0, steps + 1, step, 0)
    last = steps + 1
    k0 = 4 * (last % AHEAD)
    take_last(last)
    ready(last, 0, k0)
    for r in range(SUB):
        for i in range(2):
            part(slot(last, 1, i), r, send_d.at[0], 2 + i, mate).wait_recv()
    ready(last, 1, k0 + 2)

    for s, span_rows in enumerate((whole, body)):
        pair(base, span_rows, send_p.at[s], plus).wait_send()
        pair(base, span_rows, send_m.at[s], minus).wait_send()
    piece(base, send_p.at[2], plus).wait_send()
    piece(base, send_m.at[2], minus).wait_send()
    for r in range(SUB - 1):
        part(base, r, send_p.at[3 + r], 0, plus).wait_send()
        part(base, r, send_m.at[3 + r], 1, minus).wait_send()

    @pl.when(odd)
    def _():
        for k in (2 + SUB, 3 + SUB):
            part(base, SUB - 1, send_p.at[k], 0, plus).wait_send()
            part(base, SUB - 1, send_m.at[k], 1, minus).wait_send()
    for s, span_rows in enumerate((whole, body, whole, whole, body, body)):
        pair(base, span_rows, send_d.at[s], mate).wait_send()
    for s in (6, 7):
        piece(base, send_d.at[s], mate).wait_send()
    for i in range(2):
        for r in range(SUB):
            part(base, r, send_d.at[8 + i * SUB + r], 2, mate).wait_send()


def _write_kernel(n, rbuf, xacc, gbuf, gt, rr, left, r_out, l_out, d_out,
                  tail, xs, d_buf, l_buf, lbuf, r_sem, sem):
    me = lax.axis_index("tensor")
    width = gbuf.shape[2]
    cols, nl = d_buf.shape[1], left.shape[0]
    rows = d_buf.shape[0]
    body = pl.ds(0, rows)
    last = 7
    k0 = 4 * (last % AHEAD)

    def span(sl):
        return pl.ds(pl.multiple_of(sl * width, width), width)

    left_copy = pltpu.make_async_copy(left, l_buf, sem.at[0])
    left_copy.start()
    copies = []

    def write(src, dst):
        copies.append(pltpu.make_async_copy(src, dst, r_sem.at[len(copies)]))
        copies[-1].start()

    chips = n // 2
    far = me // 2 + chips // 2
    tall, wide = cols // 4, 2 * cols
    for c in range(1, chips):
        at = pl.ds(pl.multiple_of(lax.rem(far + c, chips) * wide, wide), wide)
        for p in range(4):
            block = (pl.ds(p * tall, tall), at)
            write(rbuf.at[block], r_out.at[block])
    for u in range(2):
        for i in range(2):
            at = span(_slot(n, me, last - 1, u, i))
            write(rbuf.at[:, at], r_out.at[:, at])
    tails = [_slot(n, me, last, u, i) for u in range(2) for i in range(2)]
    for k, sl in enumerate(tails):
        tail[k] = EMA_DECAY * rbuf[:, span(sl)] + (1.0 - EMA_DECAY) * jnp.dot(
            gt[...], gbuf[sl, body, :], preferred_element_type=jnp.float32)
        write(tail.at[k], r_out.at[:, span(sl)])
    g = [gbuf[sl, body, :] for sl in tails]
    xs[...] = xacc[...] + _nt(rr[k0], g[0]) + _nt(rr[k0 + 1], g[1])
    xs[...] += _nt(rr[k0 + 2], g[2]) + _nt(rr[k0 + 3], g[3])
    mate = me + 1 - 2 * (me % 2)
    for near in (me, mate):
        for shift, parts in ((0, (0, 1)), (-2, (0, 1)), (2, (3, 2)), (4, (0, 2))):
            owner = lax.rem(near + shift + n, n)
            at = pl.ds(pl.multiple_of(owner * nl, nl), nl)
            for h, q in enumerate(parts):
                lbuf[at, pl.ds(h * width, width)] = gbuf[owner * SPLIT + q, pl.ds(rows, nl), :]
    d_buf[...] = _nt(lbuf[...], xs[pl.ds(0, cols), :].astype(jnp.bfloat16))
    write(d_buf, d_out)
    left_copy.wait()
    l_buf[...] = EMA_DECAY * l_buf[...] + (1.0 - EMA_DECAY) * xs[pl.ds(cols, nl), :]
    write(l_buf, l_out)
    for c in copies:
        c.wait()


def solution(mesh):
    row_spec = P(("layer", "tensor"), None)
    col_spec = P("layer", "tensor")
    n = mesh.shape["tensor"]

    def local_step(grad, left, right, lroot, rroot):
        rows, cols = grad.shape
        nl = lroot.shape[0]
        width = cols // SPLIT
        f32, bf16 = jnp.float32, jnp.bfloat16
        dma = pltpu.SemaphoreType.DMA
        held = pl.pallas_call(
            functools.partial(_gather_kernel, n),
            out_shape=(pltpu.VMEM(right.shape, f32), pltpu.VMEM((cols + nl, rows), f32),
                       pltpu.VMEM((n * SPLIT, rows + nl, width), bf16), pltpu.VMEM((cols, rows), bf16),
                       pltpu.VMEM((4 * AHEAD, cols + nl, width), bf16)),
            in_specs=[ANY] * 4,
            out_specs=(VMEM,) * 5,
            scratch_shapes=[
                dma((SPLIT,)), dma((SPLIT,)), dma((n * SPLIT,)), dma((4 * AHEAD,)), dma((n * SPLIT,)),
                dma((4, SUB)), dma((4 + SUB,)), dma((4 + SUB,)), dma((8 + 2 * SUB,)),
            ],
            compiler_params=pltpu.CompilerParams(collective_id=0, has_side_effects=True, vmem_limit_bytes=GRANT),
        )(grad, lroot, right, rroot)
        r, l, d = pl.pallas_call(
            functools.partial(_write_kernel, n),
            out_shape=(jax.ShapeDtypeStruct(right.shape, f32), jax.ShapeDtypeStruct((nl, rows), f32),
                       jax.ShapeDtypeStruct((rows, cols), f32)),
            in_specs=[VMEM] * 5 + [ANY],
            out_specs=(ANY,) * 3,
            scratch_shapes=[pltpu.VMEM((4, cols, width), f32), pltpu.VMEM((cols + nl, rows), f32),
                            pltpu.VMEM((rows, cols), f32), pltpu.VMEM((nl, rows), f32), pltpu.VMEM((rows, rows), bf16), dma((22,)), dma((1,))],
            compiler_params=pltpu.CompilerParams(vmem_limit_bytes=GRANT),
        )(*[pltpu.with_memory_space_constraint(v, pltpu.VMEM) for v in held], left)
        return l, r, d

    return jax.shard_map(local_step, mesh=mesh, in_specs=(col_spec, row_spec, row_spec, row_spec, row_spec), out_specs=(row_spec, row_spec, col_spec), check_vma=False)
```

```python
import functools

import jax
import jax.numpy as jnp
from jax import lax
from jax.experimental import pallas as pl
from jax.experimental.pallas import tpu as pltpu
from jax.sharding import PartitionSpec as P

EMA_DECAY = 0.9
SPLIT = 4
SUB = 2
AHEAD = 3
GRANT = 12 << 20

MESH = pl.DeviceIdType.MESH
ANY = pl.BlockSpec(memory_space=pl.ANY)
VMEM = pl.BlockSpec(memory_space=pltpu.VMEM)


def _nt(a, b):
    return lax.dot_general(a, b, (((1,), (1,)), ((), ())), preferred_element_type=jnp.float32)


def _slot(n, me, t, u, i):
    mate = me + 1 - 2 * (me % 2)
    base = jnp.where(u == 0, me, mate)
    s = t - 2
    far = 2 + 2 * (s // SPLIT)
    owner = jnp.where(i == 0, base - far, base + far)
    part = (s + 2 * i) % SPLIT
    owner = jnp.where(t == 0, me, jnp.where(t == 1, mate, owner))
    part = jnp.where(t < 2, 2 * u + i, part)
    return lax.rem(owner + n, n) * SPLIT + part


def _gather_kernel(n, grad, lroot, right, rroot, rbuf, xacc, gbuf, gt, rr,
                   own_sem, l_sem, r_sem, rr_sem, recv, recv_sub, send_p, send_m, send_d):
    me = lax.axis_index("tensor")
    mate = me + 1 - 2 * (me % 2)
    width = gbuf.shape[2]
    cols, rows = gt.shape
    nl = lroot.shape[0]
    body, whole = pl.ds(0, rows), pl.ds(0, rows + nl)
    steps = 6
    ring = lambda d: lax.rem(d + n, n)
    plus, minus = ring(me + 2), ring(me - 2)
    plus_mate, minus_mate = ring(mate + 2), ring(mate - 2)
    odd = me % 2 == 1

    slot = functools.partial(_slot, n, me)

    def span(sl):
        return pl.ds(pl.multiple_of(sl * width, width), width)

    def r_copy(sl):
        return pltpu.make_async_copy(right.at[:, span(sl)], rbuf.at[:, span(sl)], r_sem.at[sl])

    def rr_copy(sl, k):
        return pltpu.make_async_copy(rroot.at[:, span(sl)], rr.at[k, pl.ds(0, cols)], rr_sem.at[k])

    def own_copy(q):
        return pltpu.make_async_copy(grad.at[:, pl.ds(q * width, width)], gbuf.at[me * SPLIT + q, body], own_sem.at[q])

    def left_copy(q):
        half = (q + q // 2) % 2
        return pltpu.make_async_copy(
            lroot.at[:, pl.ds(half * width, width)], gbuf.at[me * SPLIT + q, pl.ds(rows, nl)], l_sem.at[q])

    def send(at, sem, recv_sem, dev):
        return pltpu.make_async_remote_copy(
            src_ref=at, dst_ref=at, send_sem=sem, recv_sem=recv_sem,
            device_id={"tensor": dev}, device_id_type=MESH)

    def piece(sl, sem, dev):
        return send(gbuf.at[sl, whole], sem, recv.at[sl], dev)

    def pair(sl, span_rows, sem, dev):
        return send(gbuf.at[pl.ds(sl, 2), span_rows], sem, recv.at[sl], dev)

    def part(sl, r, sem, group, dev):
        first = rows * 5 // 8
        at = gbuf.at[sl, pl.ds(0, first) if r == 0 else pl.ds(first, rows - first)]
        return send(at, sem, recv_sub.at[group, r], dev)

    own = [[own_copy(q), left_copy(q)] for q in range(SPLIT)]
    for q in (0, 1, 2, 3):
        for c in own[q]:
            c.start()

    def loads(t, k0):
        for u in range(2):
            for i in range(2):
                sl = slot(t, u, i)
                r_copy(sl).start()
                rr_copy(sl, k0 + 2 * u + i).start()

    barrier = pltpu.get_barrier_semaphore()
    peers = (plus, minus, mate, plus_mate, minus_mate)
    for dev in peers:
        pl.semaphore_signal(barrier, inc=1, device_id={"tensor": dev}, device_id_type=MESH)
    pl.semaphore_wait(barrier, len(peers))

    base = me * SPLIT
    for q in (0, 1):
        for c in own[q]:
            c.wait()
    pair(base, whole, send_p.at[0], plus).start()
    for q in (2, 3):
        for c in own[q]:
            c.wait()
    pair(base + 2, whole, send_m.at[0], minus).start()
    pair(base + 2, body, send_p.at[1], plus).start()
    pair(base, body, send_m.at[1], minus).start()
    pair(base, whole, send_d.at[0], mate).start()
    pair(base + 2, body, send_d.at[1], mate).start()
    for t in range(AHEAD):
        loads(t, 4 * t)
    for q in range(SPLIT):
        gt[pl.ds(q * width, width), :] = gbuf[me * SPLIT + q, body, :].T
    xacc[...] = jnp.zeros_like(xacc)

    lrow = pl.ds(pl.multiple_of(me * nl, nl), nl)

    def ready(t, u, k0):
        for i in range(2):
            sl = slot(t, u, i)
            r_copy(sl).wait()
            rr_copy(sl, k0 + i).wait()
            rr[k0 + i, pl.ds(cols, nl), :] = gbuf[sl, lrow, :]

    def unit(t, u, k0):
        ready(t, u, k0)
        sls = [slot(t, u, i) for i in range(2)]
        for sl in sls:
            rbuf[:, span(sl)] = EMA_DECAY * rbuf[:, span(sl)] + (1.0 - EMA_DECAY) * jnp.dot(
                gt[...], gbuf[sl, body, :], preferred_element_type=jnp.float32)
        xacc[...] += _nt(rr[k0], gbuf[sls[0], body, :]) + _nt(rr[k0 + 1], gbuf[sls[1], body, :])

    def arrived(sl):
        piece(sl, send_d.at[0], mate).wait_recv()

    def pair_arrived(sl, span_rows):
        pair(sl, span_rows, send_d.at[0], mate).wait_recv()

    def take(t):
        s = t - 2

        @pl.when(t == 1)
        def _():
            pair_arrived(mate * SPLIT, whole)
            pair_arrived(mate * SPLIT + 2, body)

        @pl.when(t >= 2)
        def _():
            a, b = slot(t, 0, 0), slot(t, 0, 1)

            for at, span_rows in ((0, whole), (2, body)):
                @pl.when(s == at)
                def _(span_rows=span_rows):
                    pair_arrived(a, span_rows)
                    pair(a, span_rows, send_d.at[2 + s], mate).start()
                    pair_arrived(b, span_rows)
                    pair(b, span_rows, send_d.at[3 + s], mate).start()

            @pl.when(s == 4)
            def _():
                arrived(a)
                piece(a, send_d.at[6], mate).start()
                arrived(b)
                piece(b, send_d.at[7], mate).start()

            @pl.when(s == 1)
            def _():
                @pl.when(odd)
                def _():
                    part(slot(t, 1, 0), SUB - 1, send_p.at[3 + SUB], 0, plus_mate).start()
                    part(slot(t, 1, 1), SUB - 1, send_m.at[3 + SUB], 1, minus_mate).start()
                piece(a - 1, send_p.at[2], plus).start()
                piece(b - 1, send_m.at[2], minus).start()
                for r in range(SUB - 1):
                    part(a, r, send_p.at[3 + r], 0, plus).start()
                    part(b, r, send_m.at[3 + r], 1, minus).start()

                @pl.when(odd)
                def _():
                    part(a, SUB - 1, send_p.at[2 + SUB], 0, plus).start()
                    part(b, SUB - 1, send_m.at[2 + SUB], 1, minus).start()

    def take_last(t):
        for r in range(SUB):
            for i in range(2):
                sl = slot(t, 0, i)
                part(sl, r, send_d.at[0], i, mate).wait_recv()
                part(sl, r, send_d.at[8 + i * SUB + r], 2 + i, mate).start()

    def take_mate(t):
        s = t - 2

        for at, span_rows in ((0, whole), (2, body)):
            @pl.when(s == at)
            def _(span_rows=span_rows):
                pair_arrived(slot(t, 1, 0), span_rows)
                pair_arrived(slot(t, 1, 1), span_rows)

        @pl.when(s == 4)
        def _():
            arrived(slot(t, 1, 0))
            arrived(slot(t, 1, 1))

    def step(t, carry):
        k0 = 4 * lax.rem(t, AHEAD)
        take(t)
        unit(t, 0, k0)
        take_mate(t)
        unit(t, 1, k0 + 2)

        @pl.when(t + AHEAD < steps + 2)
        def _():
            loads(t + AHEAD, k0)
        return carry

    lax.fori_loop(0, steps + 1, step, 0)
    last = steps + 1
    k0 = 4 * (last % AHEAD)
    take_last(last)
    ready(last, 0, k0)
    for r in range(SUB):
        for i in range(2):
            part(slot(last, 1, i), r, send_d.at[0], 2 + i, mate).wait_recv()
    ready(last, 1, k0 + 2)

    for s, span_rows in enumerate((whole, body)):
        pair(base, span_rows, send_p.at[s], plus).wait_send()
        pair(base, span_rows, send_m.at[s], minus).wait_send()
    piece(base, send_p.at[2], plus).wait_send()
    piece(base, send_m.at[2], minus).wait_send()
    for r in range(SUB - 1):
        part(base, r, send_p.at[3 + r], 0, plus).wait_send()
        part(base, r, send_m.at[3 + r], 1, minus).wait_send()

    @pl.when(odd)
    def _():
        for k in (2 + SUB, 3 + SUB):
            part(base, SUB - 1, send_p.at[k], 0, plus).wait_send()
            part(base, SUB - 1, send_m.at[k], 1, minus).wait_send()
    for s, span_rows in enumerate((whole, body, whole, whole, body, body)):
        pair(base, span_rows, send_d.at[s], mate).wait_send()
    for s in (6, 7):
        piece(base, send_d.at[s], mate).wait_send()
    for i in range(2):
        for r in range(SUB):
            part(base, r, send_d.at[8 + i * SUB + r], 2, mate).wait_send()


def _write_kernel(n, rbuf, xacc, gbuf, gt, rr, left, r_out, l_out, d_out,
                  tail, xs, d_buf, l_buf, lbuf, r_sem, sem):
    me = lax.axis_index("tensor")
    width = gbuf.shape[2]
    cols, nl = d_buf.shape[1], left.shape[0]
    rows = d_buf.shape[0]
    body = pl.ds(0, rows)
    last = 7
    k0 = 4 * (last % AHEAD)

    def span(sl):
        return pl.ds(pl.multiple_of(sl * width, width), width)

    left_copy = pltpu.make_async_copy(left, l_buf, sem.at[0])
    left_copy.start()
    copies = []

    def write(src, dst):
        copies.append(pltpu.make_async_copy(src, dst, r_sem.at[len(copies)]))
        copies[-1].start()

    chips = n // 2
    far = me // 2 + chips // 2
    tall, wide = cols // 4, 2 * cols
    for c in range(1, chips):
        at = pl.ds(pl.multiple_of(lax.rem(far + c, chips) * wide, wide), wide)
        for p in range(4):
            block = (pl.ds(p * tall, tall), at)
            write(rbuf.at[block], r_out.at[block])
    for u in range(2):
        for i in range(2):
            at = span(_slot(n, me, last - 1, u, i))
            write(rbuf.at[:, at], r_out.at[:, at])
    tails = [_slot(n, me, last, u, i) for u in range(2) for i in range(2)]
    for k, sl in enumerate(tails):
        tail[k] = EMA_DECAY * rbuf[:, span(sl)] + (1.0 - EMA_DECAY) * jnp.dot(
            gt[...], gbuf[sl, body, :], preferred_element_type=jnp.float32)
        write(tail.at[k], r_out.at[:, span(sl)])
    g = [gbuf[sl, body, :] for sl in tails]
    xs[...] = xacc[...] + _nt(rr[k0], g[0]) + _nt(rr[k0 + 1], g[1])
    xs[...] += _nt(rr[k0 + 2], g[2]) + _nt(rr[k0 + 3], g[3])
    mate = me + 1 - 2 * (me % 2)
    for near in (me, mate):
        for shift, parts in ((0, (0, 1)), (-2, (0, 1)), (2, (3, 2)), (4, (0, 2))):
            owner = lax.rem(near + shift + n, n)
            at = pl.ds(pl.multiple_of(owner * nl, nl), nl)
            for h, q in enumerate(parts):
                lbuf[at, pl.ds(h * width, width)] = gbuf[owner * SPLIT + q, pl.ds(rows, nl), :]
    d_buf[...] = _nt(lbuf[...], xs[pl.ds(0, cols), :].astype(jnp.bfloat16))
    write(d_buf, d_out)
    left_copy.wait()
    l_buf[...] = EMA_DECAY * l_buf[...] + (1.0 - EMA_DECAY) * xs[pl.ds(cols, nl), :]
    write(l_buf, l_out)
    for c in copies:
        c.wait()


def solution(mesh):
    row_spec = P(("layer", "tensor"), None)
    col_spec = P("layer", "tensor")
    n = mesh.shape["tensor"]

    def local_step(grad, left, right, lroot, rroot):
        rows, cols = grad.shape
        nl = lroot.shape[0]
        width = cols // SPLIT
        f32, bf16 = jnp.float32, jnp.bfloat16
        dma = pltpu.SemaphoreType.DMA
        held = pl.pallas_call(
            functools.partial(_gather_kernel, n),
            out_shape=(pltpu.VMEM(right.shape, f32), pltpu.VMEM((cols + nl, rows), f32),
                       pltpu.VMEM((n * SPLIT, rows + nl, width), bf16), pltpu.VMEM((cols, rows), bf16),
                       pltpu.VMEM((4 * AHEAD, cols + nl, width), bf16)),
            in_specs=[ANY] * 4,
            out_specs=(VMEM,) * 5,
            scratch_shapes=[
                dma((SPLIT,)), dma((SPLIT,)), dma((n * SPLIT,)), dma((4 * AHEAD,)), dma((n * SPLIT,)),
                dma((4, SUB)), dma((4 + SUB,)), dma((4 + SUB,)), dma((8 + 2 * SUB,)),
            ],
            compiler_params=pltpu.CompilerParams(collective_id=0, has_side_effects=True, vmem_limit_bytes=GRANT),
        )(grad, lroot, right, rroot)
        r, l, d = pl.pallas_call(
            functools.partial(_write_kernel, n),
            out_shape=(jax.ShapeDtypeStruct(right.shape, f32), jax.ShapeDtypeStruct((nl, rows), f32),
                       jax.ShapeDtypeStruct((rows, cols), f32)),
            in_specs=[VMEM] * 5 + [ANY],
            out_specs=(ANY,) * 3,
            scratch_shapes=[pltpu.VMEM((4, cols, width), f32), pltpu.VMEM((cols + nl, rows), f32),
                            pltpu.VMEM((rows, cols), f32), pltpu.VMEM((nl, rows), f32), pltpu.VMEM((rows, rows), bf16), dma((22,)), dma((1,))],
            compiler_params=pltpu.CompilerParams(vmem_limit_bytes=GRANT),
        )(*[pltpu.with_memory_space_constraint(v, pltpu.VMEM) for v in held], left)
        return l, r, d

    return jax.shard_map(local_step, mesh=mesh, in_specs=(col_spec, row_spec, row_spec, row_spec, row_spec), out_specs=(row_spec, row_spec, col_spec), check_vma=False)
```

```python
import functools

import jax
import jax.numpy as jnp
from jax import lax
from jax.experimental import pallas as pl
from jax.experimental.pallas import tpu as pltpu
from jax.sharding import PartitionSpec as P

EMA_DECAY = 0.9
SPLIT = 4
SUB = 2
AHEAD = 3
GRANT = 12 << 20

MESH = pl.DeviceIdType.MESH
ANY = pl.BlockSpec(memory_space=pl.ANY)
VMEM = pl.BlockSpec(memory_space=pltpu.VMEM)


def _nt(a, b):
    return lax.dot_general(a, b, (((1,), (1,)), ((), ())), preferred_element_type=jnp.float32)


def _slot(n, me, t, u, i):
    mate = me + 1 - 2 * (me % 2)
    base = jnp.where(u == 0, me, mate)
    s = t - 2
    far = 2 + 2 * (s // SPLIT)
    owner = jnp.where(i == 0, base - far, base + far)
    part = (s + 2 * i) % SPLIT
    owner = jnp.where(t == 0, me, jnp.where(t == 1, mate, owner))
    part = jnp.where(t < 2, 2 * u + i, part)
    return lax.rem(owner + n, n) * SPLIT + part


def _gather_kernel(n, grad, lroot, right, rroot, rbuf, xacc, gbuf, gt, rr,
                   own_sem, l_sem, r_sem, rr_sem, recv, recv_sub, send_p, send_m, send_d):
    me = lax.axis_index("tensor")
    mate = me + 1 - 2 * (me % 2)
    width = gbuf.shape[2]
    cols, rows = gt.shape
    nl = lroot.shape[0]
    body, whole = pl.ds(0, rows), pl.ds(0, rows + nl)
    steps = 6
    ring = lambda d: lax.rem(d + n, n)
    plus, minus = ring(me + 2), ring(me - 2)
    plus_mate, minus_mate = ring(mate + 2), ring(mate - 2)
    odd = me % 2 == 1

    slot = functools.partial(_slot, n, me)

    def span(sl):
        return pl.ds(pl.multiple_of(sl * width, width), width)

    def r_copy(sl):
        return pltpu.make_async_copy(right.at[:, span(sl)], rbuf.at[:, span(sl)], r_sem.at[sl])

    def rr_copy(sl, k):
        return pltpu.make_async_copy(rroot.at[:, span(sl)], rr.at[k, pl.ds(0, cols)], rr_sem.at[k])

    def own_copy(q):
        return pltpu.make_async_copy(grad.at[:, pl.ds(q * width, width)], gbuf.at[me * SPLIT + q, body], own_sem.at[q])

    def left_copy(q):
        half = (q + q // 2) % 2
        return pltpu.make_async_copy(
            lroot.at[:, pl.ds(half * width, width)], gbuf.at[me * SPLIT + q, pl.ds(rows, nl)], l_sem.at[q])

    def send(at, sem, recv_sem, dev):
        return pltpu.make_async_remote_copy(
            src_ref=at, dst_ref=at, send_sem=sem, recv_sem=recv_sem,
            device_id={"tensor": dev}, device_id_type=MESH)

    def piece(sl, sem, dev):
        return send(gbuf.at[sl, whole], sem, recv.at[sl], dev)

    def pair(sl, span_rows, sem, dev):
        return send(gbuf.at[pl.ds(sl, 2), span_rows], sem, recv.at[sl], dev)

    def part(sl, r, sem, group, dev):
        first = rows // 2
        at = gbuf.at[sl, pl.ds(0, first) if r == 0 else pl.ds(first, rows - first)]
        return send(at, sem, recv_sub.at[group, r], dev)

    own = [[own_copy(q), left_copy(q)] for q in range(SPLIT)]
    for q in (0, 1, 2, 3):
        for c in own[q]:
            c.start()

    def loads(t, k0):
        for u in range(2):
            for i in range(2):
                sl = slot(t, u, i)
                r_copy(sl).start()
                rr_copy(sl, k0 + 2 * u + i).start()

    barrier = pltpu.get_barrier_semaphore()
    peers = (plus, minus, mate, plus_mate, minus_mate)
    for dev in peers:
        pl.semaphore_signal(barrier, inc=1, device_id={"tensor": dev}, device_id_type=MESH)
    pl.semaphore_wait(barrier, len(peers))

    base = me * SPLIT
    for q in (0, 1):
        for c in own[q]:
            c.wait()
    pair(base, whole, send_p.at[0], plus).start()
    for q in (2, 3):
        for c in own[q]:
            c.wait()
    pair(base + 2, whole, send_m.at[0], minus).start()
    pair(base + 2, body, send_p.at[1], plus).start()
    pair(base, body, send_m.at[1], minus).start()
    pair(base, whole, send_d.at[0], mate).start()
    pair(base + 2, body, send_d.at[1], mate).start()
    for t in range(AHEAD):
        loads(t, 4 * t)
    for q in range(SPLIT):
        gt[pl.ds(q * width, width), :] = gbuf[me * SPLIT + q, body, :].T
    xacc[...] = jnp.zeros_like(xacc)

    lrow = pl.ds(pl.multiple_of(me * nl, nl), nl)

    def ready(t, u, k0):
        for i in range(2):
            sl = slot(t, u, i)
            r_copy(sl).wait()
            rr_copy(sl, k0 + i).wait()
            rr[k0 + i, pl.ds(cols, nl), :] = gbuf[sl, lrow, :]

    def unit(t, u, k0):
        ready(t, u, k0)
        sls = [slot(t, u, i) for i in range(2)]
        for sl in sls:
            rbuf[:, span(sl)] = EMA_DECAY * rbuf[:, span(sl)] + (1.0 - EMA_DECAY) * jnp.dot(
                gt[...], gbuf[sl, body, :], preferred_element_type=jnp.float32)
        xacc[...] += _nt(rr[k0], gbuf[sls[0], body, :]) + _nt(rr[k0 + 1], gbuf[sls[1], body, :])

    def arrived(sl):
        piece(sl, send_d.at[0], mate).wait_recv()

    def pair_arrived(sl, span_rows):
        pair(sl, span_rows, send_d.at[0], mate).wait_recv()

    def take(t):
        s = t - 2

        @pl.when(t == 1)
        def _():
            pair_arrived(mate * SPLIT, whole)
            pair_arrived(mate * SPLIT + 2, body)

        @pl.when(t >= 2)
        def _():
            a, b = slot(t, 0, 0), slot(t, 0, 1)

            for at, span_rows in ((0, whole), (2, body)):
                @pl.when(s == at)
                def _(span_rows=span_rows):
                    pair_arrived(a, span_rows)
                    pair(a, span_rows, send_d.at[2 + s], mate).start()
                    pair_arrived(b, span_rows)
                    pair(b, span_rows, send_d.at[3 + s], mate).start()

            @pl.when(s == 4)
            def _():
                arrived(a)
                piece(a, send_d.at[6], mate).start()
                arrived(b)
                piece(b, send_d.at[7], mate).start()

            @pl.when(s == 1)
            def _():
                @pl.when(odd)
                def _():
                    part(slot(t, 1, 0), SUB - 1, send_p.at[3 + SUB], 0, plus_mate).start()
                    part(slot(t, 1, 1), SUB - 1, send_m.at[3 + SUB], 1, minus_mate).start()
                piece(a - 1, send_p.at[2], plus).start()
                piece(b - 1, send_m.at[2], minus).start()
                for r in range(SUB - 1):
                    part(a, r, send_p.at[3 + r], 0, plus).start()
                    part(b, r, send_m.at[3 + r], 1, minus).start()

                @pl.when(odd)
                def _():
                    part(a, SUB - 1, send_p.at[2 + SUB], 0, plus).start()
                    part(b, SUB - 1, send_m.at[2 + SUB], 1, minus).start()

    def take_last(t):
        for r in range(SUB):
            for i in range(2):
                sl = slot(t, 0, i)
                part(sl, r, send_d.at[0], i, mate).wait_recv()
                part(sl, r, send_d.at[8 + i * SUB + r], 2 + i, mate).start()

    def take_mate(t):
        s = t - 2

        for at, span_rows in ((0, whole), (2, body)):
            @pl.when(s == at)
            def _(span_rows=span_rows):
                pair_arrived(slot(t, 1, 0), span_rows)
                pair_arrived(slot(t, 1, 1), span_rows)

        @pl.when(s == 4)
        def _():
            arrived(slot(t, 1, 0))
            arrived(slot(t, 1, 1))

    def step(t, carry):
        k0 = 4 * lax.rem(t, AHEAD)
        take(t)
        unit(t, 0, k0)
        take_mate(t)
        unit(t, 1, k0 + 2)

        @pl.when(t + AHEAD < steps + 2)
        def _():
            loads(t + AHEAD, k0)
        return carry

    lax.fori_loop(0, steps + 1, step, 0)
    last = steps + 1
    k0 = 4 * (last % AHEAD)
    take_last(last)
    ready(last, 0, k0)
    for r in range(SUB):
        for i in range(2):
            part(slot(last, 1, i), r, send_d.at[0], 2 + i, mate).wait_recv()
    ready(last, 1, k0 + 2)

    for s, span_rows in enumerate((whole, body)):
        pair(base, span_rows, send_p.at[s], plus).wait_send()
        pair(base, span_rows, send_m.at[s], minus).wait_send()
    piece(base, send_p.at[2], plus).wait_send()
    piece(base, send_m.at[2], minus).wait_send()
    for r in range(SUB - 1):
        part(base, r, send_p.at[3 + r], 0, plus).wait_send()
        part(base, r, send_m.at[3 + r], 1, minus).wait_send()

    @pl.when(odd)
    def _():
        for k in (2 + SUB, 3 + SUB):
            part(base, SUB - 1, send_p.at[k], 0, plus).wait_send()
            part(base, SUB - 1, send_m.at[k], 1, minus).wait_send()
    for s, span_rows in enumerate((whole, body, whole, whole, body, body)):
        pair(base, span_rows, send_d.at[s], mate).wait_send()
    for s in (6, 7):
        piece(base, send_d.at[s], mate).wait_send()
    for i in range(2):
        for r in range(SUB):
            part(base, r, send_d.at[8 + i * SUB + r], 2, mate).wait_send()


def _write_kernel(n, rbuf, xacc, gbuf, gt, rr, left, r_out, l_out, d_out,
                  tail, xs, d_buf, l_buf, lbuf, r_sem, sem):
    me = lax.axis_index("tensor")
    width = gbuf.shape[2]
    cols, nl = d_buf.shape[1], left.shape[0]
    rows = d_buf.shape[0]
    body = pl.ds(0, rows)
    last = 7
    k0 = 4 * (last % AHEAD)

    def span(sl):
        return pl.ds(pl.multiple_of(sl * width, width), width)

    left_copy = pltpu.make_async_copy(left, l_buf, sem.at[0])
    left_copy.start()
    copies = []

    def write(src, dst):
        copies.append(pltpu.make_async_copy(src, dst, r_sem.at[len(copies)]))
        copies[-1].start()

    chips = n // 2
    far = me // 2 + chips // 2
    tall, wide = cols // 4, 2 * cols
    for c in range(1, chips):
        at = pl.ds(pl.multiple_of(lax.rem(far + c, chips) * wide, wide), wide)
        for p in range(4):
            block = (pl.ds(p * tall, tall), at)
            write(rbuf.at[block], r_out.at[block])
    for u in range(2):
        for i in range(2):
            at = span(_slot(n, me, last - 1, u, i))
            write(rbuf.at[:, at], r_out.at[:, at])
    tails = [_slot(n, me, last, u, i) for u in range(2) for i in range(2)]
    for k, sl in enumerate(tails):
        tail[k] = EMA_DECAY * rbuf[:, span(sl)] + (1.0 - EMA_DECAY) * jnp.dot(
            gt[...], gbuf[sl, body, :], preferred_element_type=jnp.float32)
        write(tail.at[k], r_out.at[:, span(sl)])
    g = [gbuf[sl, body, :] for sl in tails]
    xs[...] = xacc[...] + _nt(rr[k0], g[0]) + _nt(rr[k0 + 1], g[1])
    xs[...] += _nt(rr[k0 + 2], g[2]) + _nt(rr[k0 + 3], g[3])
    mate = me + 1 - 2 * (me % 2)
    for near in (me, mate):
        for shift, parts in ((0, (0, 1)), (-2, (0, 1)), (2, (3, 2)), (4, (0, 2))):
            owner = lax.rem(near + shift + n, n)
            at = pl.ds(pl.multiple_of(owner * nl, nl), nl)
            for h, q in enumerate(parts):
                lbuf[at, pl.ds(h * width, width)] = gbuf[owner * SPLIT + q, pl.ds(rows, nl), :]
    d_buf[...] = _nt(lbuf[...], xs[pl.ds(0, cols), :].astype(jnp.bfloat16))
    write(d_buf, d_out)
    left_copy.wait()
    l_buf[...] = EMA_DECAY * l_buf[...] + (1.0 - EMA_DECAY) * xs[pl.ds(cols, nl), :]
    write(l_buf, l_out)
    for c in copies:
        c.wait()


def solution(mesh):
    row_spec = P(("layer", "tensor"), None)
    col_spec = P("layer", "tensor")
    n = mesh.shape["tensor"]

    def local_step(grad, left, right, lroot, rroot):
        rows, cols = grad.shape
        nl = lroot.shape[0]
        width = cols // SPLIT
        f32, bf16 = jnp.float32, jnp.bfloat16
        dma = pltpu.SemaphoreType.DMA
        held = pl.pallas_call(
            functools.partial(_gather_kernel, n),
            out_shape=(pltpu.VMEM(right.shape, f32), pltpu.VMEM((cols + nl, rows), f32),
                       pltpu.VMEM((n * SPLIT, rows + nl, width), bf16), pltpu.VMEM((cols, rows), bf16),
                       pltpu.VMEM((4 * AHEAD, cols + nl, width), bf16)),
            in_specs=[ANY] * 4,
            out_specs=(VMEM,) * 5,
            scratch_shapes=[
                dma((SPLIT,)), dma((SPLIT,)), dma((n * SPLIT,)), dma((4 * AHEAD,)), dma((n * SPLIT,)),
                dma((4, SUB)), dma((4 + SUB,)), dma((4 + SUB,)), dma((8 + 2 * SUB,)),
            ],
            compiler_params=pltpu.CompilerParams(collective_id=0, has_side_effects=True, vmem_limit_bytes=GRANT),
        )(grad, lroot, right, rroot)
        r, l, d = pl.pallas_call(
            functools.partial(_write_kernel, n),
            out_shape=(jax.ShapeDtypeStruct(right.shape, f32), jax.ShapeDtypeStruct((nl, rows), f32),
                       jax.ShapeDtypeStruct((rows, cols), f32)),
            in_specs=[VMEM] * 5 + [ANY],
            out_specs=(ANY,) * 3,
            scratch_shapes=[pltpu.VMEM((4, cols, width), f32), pltpu.VMEM((cols + nl, rows), f32),
                            pltpu.VMEM((rows, cols), f32), pltpu.VMEM((nl, rows), f32), pltpu.VMEM((rows, rows), bf16), dma((22,)), dma((1,))],
            compiler_params=pltpu.CompilerParams(vmem_limit_bytes=GRANT),
        )(*[pltpu.with_memory_space_constraint(v, pltpu.VMEM) for v in held], left)
        return l, r, d

    return jax.shard_map(local_step, mesh=mesh, in_specs=(col_spec, row_spec, row_spec, row_spec, row_spec), out_specs=(row_spec, row_spec, col_spec), check_vma=False)
```

```python
import functools

import jax
import jax.numpy as jnp
from jax import lax
from jax.experimental import pallas as pl
from jax.experimental.pallas import tpu as pltpu
from jax.sharding import PartitionSpec as P

EMA_DECAY = 0.9
SPLIT = 4
SUB = 2
AHEAD = 3
GRANT = 12 << 20

MESH = pl.DeviceIdType.MESH
ANY = pl.BlockSpec(memory_space=pl.ANY)
VMEM = pl.BlockSpec(memory_space=pltpu.VMEM)


def _nt(a, b):
    return lax.dot_general(a, b, (((1,), (1,)), ((), ())), preferred_element_type=jnp.float32)


def _slot(n, me, t, u, i):
    mate = me + 1 - 2 * (me % 2)
    base = jnp.where(u == 0, me, mate)
    s = t - 2
    far = 2 + 2 * (s // SPLIT)
    owner = jnp.where(i == 0, base - far, base + far)
    part = (s + 2 * i) % SPLIT
    owner = jnp.where(t == 0, me, jnp.where(t == 1, mate, owner))
    part = jnp.where(t < 2, 2 * u + i, part)
    return lax.rem(owner + n, n) * SPLIT + part


def _gather_kernel(n, grad, lroot, right, rroot, rbuf, xacc, gbuf, gt, rr,
                   own_sem, l_sem, r_sem, rr_sem, recv, recv_sub, send_p, send_m, send_d):
    me = lax.axis_index("tensor")
    mate = me + 1 - 2 * (me % 2)
    width = gbuf.shape[2]
    cols, rows = gt.shape
    nl = lroot.shape[0]
    body, whole = pl.ds(0, rows), pl.ds(0, rows + nl)
    steps = 6
    ring = lambda d: lax.rem(d + n, n)
    plus, minus = ring(me + 2), ring(me - 2)
    plus_mate, minus_mate = ring(mate + 2), ring(mate - 2)
    odd = me % 2 == 1

    slot = functools.partial(_slot, n, me)

    def span(sl):
        return pl.ds(pl.multiple_of(sl * width, width), width)

    def r_copy(sl):
        return pltpu.make_async_copy(right.at[:, span(sl)], rbuf.at[:, span(sl)], r_sem.at[sl])

    def rr_copy(sl, k):
        return pltpu.make_async_copy(rroot.at[:, span(sl)], rr.at[k, pl.ds(0, cols)], rr_sem.at[k])

    def own_copy(q):
        return pltpu.make_async_copy(grad.at[:, pl.ds(q * width, width)], gbuf.at[me * SPLIT + q, body], own_sem.at[q])

    def left_copy(q):
        half = (q + q // 2) % 2
        return pltpu.make_async_copy(
            lroot.at[:, pl.ds(half * width, width)], gbuf.at[me * SPLIT + q, pl.ds(rows, nl)], l_sem.at[q])

    def send(at, sem, recv_sem, dev):
        return pltpu.make_async_remote_copy(
            src_ref=at, dst_ref=at, send_sem=sem, recv_sem=recv_sem,
            device_id={"tensor": dev}, device_id_type=MESH)

    def piece(sl, sem, dev):
        return send(gbuf.at[sl, whole], sem, recv.at[sl], dev)

    def pair(sl, span_rows, sem, dev):
        return send(gbuf.at[pl.ds(sl, 2), span_rows], sem, recv.at[sl], dev)

    def part(sl, r, sem, group, dev):
        first = rows * 11 // 16
        at = gbuf.at[sl, pl.ds(0, first) if r == 0 else pl.ds(first, rows - first)]
        return send(at, sem, recv_sub.at[group, r], dev)

    own = [[own_copy(q), left_copy(q)] for q in range(SPLIT)]
    for q in (0, 1, 2, 3):
        for c in own[q]:
            c.start()

    def loads(t, k0):
        for u in range(2):
            for i in range(2):
                sl = slot(t, u, i)
                r_copy(sl).start()
                rr_copy(sl, k0 + 2 * u + i).start()

    barrier = pltpu.get_barrier_semaphore()
    peers = (plus, minus, mate, plus_mate, minus_mate)
    for dev in peers:
        pl.semaphore_signal(barrier, inc=1, device_id={"tensor": dev}, device_id_type=MESH)
    pl.semaphore_wait(barrier, len(peers))

    base = me * SPLIT
    for q in (0, 1):
        for c in own[q]:
            c.wait()
    pair(base, whole, send_p.at[0], plus).start()
    for q in (2, 3):
        for c in own[q]:
            c.wait()
    pair(base + 2, whole, send_m.at[0], minus).start()
    pair(base + 2, body, send_p.at[1], plus).start()
    pair(base, body, send_m.at[1], minus).start()
    pair(base, whole, send_d.at[0], mate).start()
    pair(base + 2, body, send_d.at[1], mate).start()
    for t in range(AHEAD):
        loads(t, 4 * t)
    for q in range(SPLIT):
        gt[pl.ds(q * width, width), :] = gbuf[me * SPLIT + q, body, :].T
    xacc[...] = jnp.zeros_like(xacc)

    lrow = pl.ds(pl.multiple_of(me * nl, nl), nl)

    def ready(t, u, k0):
        for i in range(2):
            sl = slot(t, u, i)
            r_copy(sl).wait()
            rr_copy(sl, k0 + i).wait()
            rr[k0 + i, pl.ds(cols, nl), :] = gbuf[sl, lrow, :]

    def unit(t, u, k0):
        ready(t, u, k0)
        sls = [slot(t, u, i) for i in range(2)]
        for sl in sls:
            rbuf[:, span(sl)] = EMA_DECAY * rbuf[:, span(sl)] + (1.0 - EMA_DECAY) * jnp.dot(
                gt[...], gbuf[sl, body, :], preferred_element_type=jnp.float32)
        xacc[...] += _nt(rr[k0], gbuf[sls[0], body, :]) + _nt(rr[k0 + 1], gbuf[sls[1], body, :])

    def arrived(sl):
        piece(sl, send_d.at[0], mate).wait_recv()

    def pair_arrived(sl, span_rows):
        pair(sl, span_rows, send_d.at[0], mate).wait_recv()

    def take(t):
        s = t - 2

        @pl.when(t == 1)
        def _():
            pair_arrived(mate * SPLIT, whole)
            pair_arrived(mate * SPLIT + 2, body)

        @pl.when(t >= 2)
        def _():
            a, b = slot(t, 0, 0), slot(t, 0, 1)

            for at, span_rows in ((0, whole), (2, body)):
                @pl.when(s == at)
                def _(span_rows=span_rows):
                    pair_arrived(a, span_rows)
                    pair(a, span_rows, send_d.at[2 + s], mate).start()
                    pair_arrived(b, span_rows)
                    pair(b, span_rows, send_d.at[3 + s], mate).start()

            @pl.when(s == 4)
            def _():
                arrived(a)
                piece(a, send_d.at[6], mate).start()
                arrived(b)
                piece(b, send_d.at[7], mate).start()

            @pl.when(s == 1)
            def _():
                @pl.when(odd)
                def _():
                    part(slot(t, 1, 0), SUB - 1, send_p.at[3 + SUB], 0, plus_mate).start()
                    part(slot(t, 1, 1), SUB - 1, send_m.at[3 + SUB], 1, minus_mate).start()
                piece(a - 1, send_p.at[2], plus).start()
                piece(b - 1, send_m.at[2], minus).start()
                for r in range(SUB - 1):
                    part(a, r, send_p.at[3 + r], 0, plus).start()
                    part(b, r, send_m.at[3 + r], 1, minus).start()

                @pl.when(odd)
                def _():
                    part(a, SUB - 1, send_p.at[2 + SUB], 0, plus).start()
                    part(b, SUB - 1, send_m.at[2 + SUB], 1, minus).start()

    def take_last(t):
        for r in range(SUB):
            for i in range(2):
                sl = slot(t, 0, i)
                part(sl, r, send_d.at[0], i, mate).wait_recv()
                part(sl, r, send_d.at[8 + i * SUB + r], 2 + i, mate).start()

    def take_mate(t):
        s = t - 2

        for at, span_rows in ((0, whole), (2, body)):
            @pl.when(s == at)
            def _(span_rows=span_rows):
                pair_arrived(slot(t, 1, 0), span_rows)
                pair_arrived(slot(t, 1, 1), span_rows)

        @pl.when(s == 4)
        def _():
            arrived(slot(t, 1, 0))
            arrived(slot(t, 1, 1))

    def step(t, carry):
        k0 = 4 * lax.rem(t, AHEAD)
        take(t)
        unit(t, 0, k0)
        take_mate(t)
        unit(t, 1, k0 + 2)

        @pl.when(t + AHEAD < steps + 2)
        def _():
            loads(t + AHEAD, k0)
        return carry

    lax.fori_loop(0, steps + 1, step, 0)
    last = steps + 1
    k0 = 4 * (last % AHEAD)
    take_last(last)
    ready(last, 0, k0)
    for r in range(SUB):
        for i in range(2):
            part(slot(last, 1, i), r, send_d.at[0], 2 + i, mate).wait_recv()
    ready(last, 1, k0 + 2)

    for s, span_rows in enumerate((whole, body)):
        pair(base, span_rows, send_p.at[s], plus).wait_send()
        pair(base, span_rows, send_m.at[s], minus).wait_send()
    piece(base, send_p.at[2], plus).wait_send()
    piece(base, send_m.at[2], minus).wait_send()
    for r in range(SUB - 1):
        part(base, r, send_p.at[3 + r], 0, plus).wait_send()
        part(base, r, send_m.at[3 + r], 1, minus).wait_send()

    @pl.when(odd)
    def _():
        for k in (2 + SUB, 3 + SUB):
            part(base, SUB - 1, send_p.at[k], 0, plus).wait_send()
            part(base, SUB - 1, send_m.at[k], 1, minus).wait_send()
    for s, span_rows in enumerate((whole, body, whole, whole, body, body)):
        pair(base, span_rows, send_d.at[s], mate).wait_send()
    for s in (6, 7):
        piece(base, send_d.at[s], mate).wait_send()
    for i in range(2):
        for r in range(SUB):
            part(base, r, send_d.at[8 + i * SUB + r], 2, mate).wait_send()


def _write_kernel(n, rbuf, xacc, gbuf, gt, rr, left, r_out, l_out, d_out,
                  tail, xs, d_buf, l_buf, lbuf, r_sem, sem):
    me = lax.axis_index("tensor")
    width = gbuf.shape[2]
    cols, nl = d_buf.shape[1], left.shape[0]
    rows = d_buf.shape[0]
    body = pl.ds(0, rows)
    last = 7
    k0 = 4 * (last % AHEAD)

    def span(sl):
        return pl.ds(pl.multiple_of(sl * width, width), width)

    left_copy = pltpu.make_async_copy(left, l_buf, sem.at[0])
    left_copy.start()
    copies = []

    def write(src, dst):
        copies.append(pltpu.make_async_copy(src, dst, r_sem.at[len(copies)]))
        copies[-1].start()

    chips = n // 2
    far = me // 2 + chips // 2
    tall, wide = cols // 4, 2 * cols
    for c in range(1, chips):
        at = pl.ds(pl.multiple_of(lax.rem(far + c, chips) * wide, wide), wide)
        for p in range(4):
            block = (pl.ds(p * tall, tall), at)
            write(rbuf.at[block], r_out.at[block])
    for u in range(2):
        for i in range(2):
            at = span(_slot(n, me, last - 1, u, i))
            write(rbuf.at[:, at], r_out.at[:, at])
    tails = [_slot(n, me, last, u, i) for u in range(2) for i in range(2)]
    for k, sl in enumerate(tails):
        tail[k] = EMA_DECAY * rbuf[:, span(sl)] + (1.0 - EMA_DECAY) * jnp.dot(
            gt[...], gbuf[sl, body, :], preferred_element_type=jnp.float32)
        write(tail.at[k], r_out.at[:, span(sl)])
    g = [gbuf[sl, body, :] for sl in tails]
    xs[...] = xacc[...] + _nt(rr[k0], g[0]) + _nt(rr[k0 + 1], g[1])
    xs[...] += _nt(rr[k0 + 2], g[2]) + _nt(rr[k0 + 3], g[3])
    mate = me + 1 - 2 * (me % 2)
    for near in (me, mate):
        for shift, parts in ((0, (0, 1)), (-2, (0, 1)), (2, (3, 2)), (4, (0, 2))):
            owner = lax.rem(near + shift + n, n)
            at = pl.ds(pl.multiple_of(owner * nl, nl), nl)
            for h, q in enumerate(parts):
                lbuf[at, pl.ds(h * width, width)] = gbuf[owner * SPLIT + q, pl.ds(rows, nl), :]
    d_buf[...] = _nt(lbuf[...], xs[pl.ds(0, cols), :].astype(jnp.bfloat16))
    write(d_buf, d_out)
    left_copy.wait()
    l_buf[...] = EMA_DECAY * l_buf[...] + (1.0 - EMA_DECAY) * xs[pl.ds(cols, nl), :]
    write(l_buf, l_out)
    for c in copies:
        c.wait()


def solution(mesh):
    row_spec = P(("layer", "tensor"), None)
    col_spec = P("layer", "tensor")
    n = mesh.shape["tensor"]

    def local_step(grad, left, right, lroot, rroot):
        rows, cols = grad.shape
        nl = lroot.shape[0]
        width = cols // SPLIT
        f32, bf16 = jnp.float32, jnp.bfloat16
        dma = pltpu.SemaphoreType.DMA
        held = pl.pallas_call(
            functools.partial(_gather_kernel, n),
            out_shape=(pltpu.VMEM(right.shape, f32), pltpu.VMEM((cols + nl, rows), f32),
                       pltpu.VMEM((n * SPLIT, rows + nl, width), bf16), pltpu.VMEM((cols, rows), bf16),
                       pltpu.VMEM((4 * AHEAD, cols + nl, width), bf16)),
            in_specs=[ANY] * 4,
            out_specs=(VMEM,) * 5,
            scratch_shapes=[
                dma((SPLIT,)), dma((SPLIT,)), dma((n * SPLIT,)), dma((4 * AHEAD,)), dma((n * SPLIT,)),
                dma((4, SUB)), dma((4 + SUB,)), dma((4 + SUB,)), dma((8 + 2 * SUB,)),
            ],
            compiler_params=pltpu.CompilerParams(collective_id=0, has_side_effects=True, vmem_limit_bytes=GRANT),
        )(grad, lroot, right, rroot)
        r, l, d = pl.pallas_call(
            functools.partial(_write_kernel, n),
            out_shape=(jax.ShapeDtypeStruct(right.shape, f32), jax.ShapeDtypeStruct((nl, rows), f32),
                       jax.ShapeDtypeStruct((rows, cols), f32)),
            in_specs=[VMEM] * 5 + [ANY],
            out_specs=(ANY,) * 3,
            scratch_shapes=[pltpu.VMEM((4, cols, width), f32), pltpu.VMEM((cols + nl, rows), f32),
                            pltpu.VMEM((rows, cols), f32), pltpu.VMEM((nl, rows), f32), pltpu.VMEM((rows, rows), bf16), dma((22,)), dma((1,))],
            compiler_params=pltpu.CompilerParams(vmem_limit_bytes=GRANT),
        )(*[pltpu.with_memory_space_constraint(v, pltpu.VMEM) for v in held], left)
        return l, r, d

    return jax.shard_map(local_step, mesh=mesh, in_specs=(col_spec, row_spec, row_spec, row_spec, row_spec), out_specs=(row_spec, row_spec, col_spec), check_vma=False)
```
